256 devices in a mesh: tm: 8 (over x, core), space: 32 (over z, y).
Axes of the slice: x: 4, y: 4, z: 8, core: 2. Of those that a mesh axis runs over, the one named last changes fastest.
Arguments:
- span_opening: float32 [8, 128, 64, 128], P('tm', 'space'), may hold values from -8 to 8
- source_power: float32 [8, 2, 128, 64, 128], P('tm', None, 'space'), may hold values from -24 to 24
- warmth_retention: float32 [128, 64, 128], P('space'), may hold values from 0.02 to 0.4
Outputs:
- fpoint: float32 [8, 128, 64, 128], P('tm', 'space')
- updated: float32 [8, 128, 64, 128], P('tm', 'space')
The draws below stay inside these ranges and needn't reach their ends.
All inputs are finite; a program needn't handle non-finite values.
Results may differ from the reference program's by a relative error of at most 0.0001.
Values sent between devices are 32-bit elements; how exact they have to be, the bound alone decides.
No kernel may reach another device: no remote copies, remote signals or barrier semaphores. Data moves between devices by JAX's collectives and lax.ppermute only.
A program may use at most 64 MiB of HBM per device.

```python
import math
import jax
import jax.numpy as jnp

NY = 64
NX = 128
STEPS = 2
COARSE_SWEEPS = 24
GROUPS = 8
NZ = 128


def draw_source_power(key, part):
    rough = 4.0 * jax.random.normal(key, (GROUPS, STEPS, NZ, NY, NX), jnp.float32)
    return jnp.clip(rough, -24.0, 24.0)


def shard_levels(rng, extent, pieces, smallest, largest):
    level, own = 1.0, jax.random.fold_in(rng, 6)
    for axis_at, blocks in pieces:
        steps = jnp.exp(jax.random.uniform(jax.random.fold_in(own, axis_at), (blocks,), jnp.float32, smallest / len(pieces), largest / len(pieces)))
        level = level * jnp.repeat(steps, extent[axis_at] // blocks).reshape([-1 if axis == axis_at else 1 for axis in range(len(extent))])
    return level


def scatter_about(own_key, shape, scale, reach, cuts=(), held_as=jnp.bfloat16):
    loudness = shard_levels(own_key, shape, cuts, -0.22, 0.18) if cuts else 1.0
    result = jax.random.normal(own_key, shape, jnp.float32) * scale * loudness
    return jnp.minimum(jnp.maximum(result, -reach), reach).astype(held_as)


def setup_inputs(seed: int = 0) -> dict:
    arg_keys = jax.random.split(jax.random.key(seed), 4)
    span_opening = scatter_about(arg_keys[0], (GROUPS, NZ, NY, NX), 2.0, 8.0, ((0, 8), (1, 32)), jnp.float32)
    source_power = draw_source_power(jax.random.fold_in(arg_keys[3], 71), 0)
    warmth_retention = jnp.clip(jnp.exp(math.log(0.4) - 2.9957323 * jax.random.uniform(arg_keys[2], (NZ, NY, NX), jnp.float32) ** shard_levels(arg_keys[2], (NZ, NY, NX), ((0, 32),), -0.2, 0.2)), 0.02, 0.4)
    return {"span_opening": span_opening, "source_power": source_power, "warmth_retention": warmth_retention}


relax_weight = 0.8


def mean_to_rougher(field):
    extent_layout = field.shape
    blocks = field.reshape(extent_layout[0] // 2, 2, extent_layout[1] // 2, 2, extent_layout[2] // 2, 2)
    return blocks.mean(axis=(1, 3, 5))


def lift_to_finer(field):
    extent_layout = field.shape
    grown = jnp.broadcast_to(field[:, None, :, None, :, None], (extent_layout[0], 2, extent_layout[1], 2, extent_layout[2], 2))
    return grown.reshape(2 * extent_layout[0], 2 * extent_layout[1], 2 * extent_layout[2])


def neighbour_sum(field, padded):
    flat = jnp.pad(field, ((0, 0), (1, 1), (1, 1)))
    total = padded[2:] + padded[:-2]
    total = total + flat[:, 2:, 1:-1] + flat[:, :-2, 1:-1]
    return total + flat[:, 1:-1, 2:] + flat[:, 1:-1, :-2]


def apply_nearby_part(field, retention_quantities, conductance):
    padded = jnp.pad(field, ((1, 1), (0, 0), (0, 0)))
    return (retention_quantities + 6.0 * conductance) * field - conductance * neighbour_sum(field, padded)


def bottom_grid_inversion(load_components, retention_quantities):
    conductance = 0.125
    diagonal = retention_quantities + 6.0 * conductance
    first_approximation = relax_weight * load_components / diagonal
    for sweep_index in range(COARSE_SWEEPS - 1):
        first_approximation = first_approximation + relax_weight * (load_components - apply_nearby_part(first_approximation, retention_quantities, conductance)) / diagonal
    return first_approximation


def personal_hierarchy_cycle(load_components, volume_holdings, hierarchy_layers):
    if hierarchy_layers == 3:
        return bottom_grid_inversion(load_components, volume_holdings[3])
    conductance = 0.5 ** hierarchy_layers
    retention_quantities = volume_holdings[hierarchy_layers]
    diagonal = retention_quantities + 6.0 * conductance
    first_approximation = relax_weight * load_components / diagonal
    first_approximation = first_approximation + relax_weight * (load_components - apply_nearby_part(first_approximation, retention_quantities, conductance)) / diagonal
    further_moments = load_components - apply_nearby_part(first_approximation, retention_quantities, conductance)
    first_approximation = first_approximation + lift_to_finer(personal_hierarchy_cycle(mean_to_rougher(further_moments), volume_holdings, hierarchy_layers + 1))
    for sweep_index in range(2):
        first_approximation = first_approximation + relax_weight * (load_components - apply_nearby_part(first_approximation, retention_quantities, conductance)) / diagonal
    return first_approximation


def reference(span_opening, source_power, warmth_retention):
    volume_holdings = [warmth_retention]
    for level_index in range(3):
        volume_holdings.append(mean_to_rougher(volume_holdings[-1]))
    fpoints = []
    closing_results = []
    for moment_packet in range(GROUPS):
        warmth_distribution = span_opening[moment_packet]
        opening_condition = warmth_distribution
        for moment_count in range(STEPS):
            warmth_distribution = personal_hierarchy_cycle(warmth_retention * warmth_distribution + source_power[moment_packet, moment_count], volume_holdings, 0)
            if moment_count == 0:
                opening_condition = warmth_distribution
        fpoints.append(opening_condition)
        closing_results.append(warmth_distribution)
    updated = jnp.stack([span_opening[0]] + closing_results[:-1])
    return jnp.stack(fpoints), updated
```

```python
import jax
import jax.numpy as jnp
from jax import lax
from jax.experimental import pallas as pl
from jax.experimental.pallas import tpu as pltpu
from jax.sharding import PartitionSpec as P

COARSE_SWEEPS = 24
NY, NX = 64, 128
SLABS = 32
SPANS = 8
DEPTH = 4
OMEGA = 0.8
F32 = jnp.float32
VMEM = pl.BlockSpec(memory_space=pltpu.VMEM)


def f32(*shape):
    return jax.ShapeDtypeStruct(shape, F32)


def call(body, outs, scratch, *args):
    return pl.pallas_call(
        body,
        out_shape=outs,
        in_specs=[VMEM] * len(args),
        out_specs=tuple(VMEM for _ in outs),
        scratch_shapes=[pltpu.VMEM(s, F32) for s in scratch],
    )(*args)


def dot(a, b):
    return jnp.dot(a, b, precision=lax.Precision.HIGHEST, preferred_element_type=F32)


def iota(shape, axis):
    return lax.broadcasted_iota(jnp.int32, shape, axis)


def picks(test, scale):
    i, j = iota((128, 128), 0), iota((128, 128), 1)
    return jnp.where(test(i, j), jnp.float32(scale), jnp.float32(0.0))


def around_plane(c, below, above):
    row, lane = iota(c.shape, 0), iota(c.shape, 1)
    total = below + above
    total = total + jnp.where(lane > 0, pltpu.roll(c, 1, 1), 0.0)
    total = total + jnp.where(lane < NX - 1, pltpu.roll(c, NX - 1, 1), 0.0)
    total = total + jnp.where(row > 0, pltpu.roll(c, 1, 0), 0.0)
    return total + jnp.where(row < NY - 1, pltpu.roll(c, NY - 1, 0), 0.0)


def around_block(c, below, above):
    row, lane = iota(c.shape, 0), iota(c.shape, 1)
    col = lane & 63
    total = pltpu.roll(c + jnp.where(lane < 64, above, below), 64, 1)
    total = total + jnp.where(col > 0, pltpu.roll(c, 1, 1), 0.0)
    total = total + jnp.where(col < 63, pltpu.roll(c, 127, 1), 0.0)
    total = total + jnp.where(row > 0, pltpu.roll(c, 1, 0), 0.0)
    return total + jnp.where(row < 31, pltpu.roll(c, 31, 0), 0.0)


def around_low(v):
    row, lane = iota(v.shape, 0), iota(v.shape, 1)
    y, x = row & 15, lane & 31
    ends = iota((16, 128), 1)
    below = jnp.where(ends >= 32, pltpu.roll(v[112:], 32, 1), 0.0)
    above = jnp.where(ends < 96, pltpu.roll(v[:16], 96, 1), 0.0)
    total = jnp.concatenate([below, v[:112]], 0) + jnp.concatenate([v[16:], above], 0)
    total = total + jnp.where(x > 0, pltpu.roll(v, 1, 1), 0.0)
    total = total + jnp.where(x < 31, pltpu.roll(v, 127, 1), 0.0)
    total = total + jnp.where(y > 0, pltpu.roll(v, 1, 0), 0.0)
    return total + jnp.where(y < 15, pltpu.roll(v, 127, 0), 0.0)


def coarsest(b3, w3):
    lane, row = iota((8, 128), 1), iota((8, 128), 0)
    x = lane & 15
    steps = []
    for k in range(4):
        w = w3[8 * k : 8 * k + 8]
        wh = 0.125 * w
        steps.append(
            (
                w * b3[8 * k : 8 * k + 8],
                wh,
                jnp.where(x > 0, wh, 0.0),
                jnp.where(x < 15, wh, 0.0),
                jnp.where(row > 0, wh, 0.0),
                jnp.where(row < 7, wh, 0.0),
            )
        )
    inside = lane < 64

    def sweep(_, v):
        below = jnp.where(inside, pltpu.roll(v[3], 16, 1), 0.0)
        above = jnp.where(inside, pltpu.roll(v[0], 112, 1), 0.0)
        line = (below, *v, above)
        new = []
        for k in range(4):
            wb, wh, left, right, up, down = steps[k]
            c = v[k]
            t = (0.2 * c + wb) + wh * (line[k] + line[k + 2])
            s = up * pltpu.roll(c, 1, 0) + down * pltpu.roll(c, 7, 0)
            e = left * pltpu.roll(c, 1, 1) + right * pltpu.roll(c, 127, 1)
            new.append((t + s) + e)
        return tuple(new)

    v = lax.fori_loop(0, COARSE_SWEEPS - 1, sweep, tuple(s[0] for s in steps), unroll=True)
    return jnp.concatenate(v, 0)


def pack_body(u, src, cap, b_out, up, dn):
    for p in range(DEPTH):
        c = cap[p]
        b = c * u[0, p] + src[0, 0, p]
        b_out[p] = b
        if p > 0:
            up[p - 1] = b
            up[p + 2] = c
        if p < 3:
            dn[p] = b
            dn[p + 3] = c


def row_pairs(ref, start, count):
    return ref[pl.ds(start, count, stride=2), :] + ref[pl.ds(start + 1, count, stride=2), :]


def fine_down(first, b_own, cap, lo, hi, w, xs, send, ys, rs):
    lo_pick = picks(lambda i, j: (i >> 1) == j, 0.125)
    hi_pick = picks(lambda i, j: (i >> 1) + 64 == j, 0.125)

    def b(p):
        return lo[p + 3] if p < 0 else (b_own[p] if p < DEPTH else hi[p - DEPTH])

    if first:
        s = lax.axis_index("space")
        for p in range(-3, 7):
            c = lo[p + 6] if p < 0 else (cap[p] if p < DEPTH else hi[p - 1])
            v = OMEGA / (c + 6.0)
            if p < 0:
                v = jnp.where(s > 0, v, 0.0)
            if p >= DEPTH:
                v = jnp.where(s < SLABS - 1, v, 0.0)
            w[p + 3] = v
    for p in range(-3, 7):
        ys[p + 3] = w[p + 3] * b(p)
    for p in range(-2, 6):
        i = p + 3
        xs[p + 2] = 1.2 * ys[i] + w[i] * around_plane(ys[i], ys[i - 1], ys[i + 1])
    for half in range(2):
        total = None
        for p in (2 * half, 2 * half + 1):
            i = p + 2
            r = b(p) - (cap[p] + 6.0) * xs[i] + around_plane(xs[i], xs[i - 1], xs[i + 1])
            total = r if total is None else total + r
        rs[pl.ds(64 * half, 64), :] = total
        if first:
            rs[pl.ds(128 + 64 * half, 64), :] = cap[2 * half] + cap[2 * half + 1]
    parts = [(row_pairs(rs, 0, 32), row_pairs(rs, 64, 32))]
    if first:
        parts.append((row_pairs(rs, 128, 32), row_pairs(rs, 192, 32)))
    low = jnp.concatenate([a for a, _ in parts], 0)
    high = jnp.concatenate([a for _, a in parts], 0)
    block = dot(low, lo_pick) + dot(high, hi_pick)
    for peer in range(SLABS):
        send[peer] = block


def first_down_body(b_own, cap, lo, hi, w, xs, send, ys, rs):
    fine_down(True, b_own, cap, lo, hi, w, xs, send, ys, rs)


def next_down_body(b_own, cap, lo, hi, w, xs, send, ys, rs):
    fine_down(False, b_own, cap, lo, hi, w, xs, send, ys, rs)


CHUNK = 8


def over_blocks(body):
    @pl.loop(0, SLABS // CHUNK)
    def _(c):
        for k in range(CHUNK):
            body(c * CHUNK + k)


def to_low(rows):
    total = None
    for q in range(4):
        pick = picks(lambda i, j: ((j >> 5) == q) & (((i & 63) >> 1) == (j & 31)), 0.125)
        part = dot(row_pairs(rows, 256 * q, 128), pick)
        total = part if total is None else total + part
    return total


def to_coarsest(v, t3):
    for k in range(4):
        t3[pl.ds(16 * k, 16), :] = v[32 * k : 32 * k + 16] + v[32 * k + 16 : 32 * k + 32]
    pick = picks(lambda i, j: (j < 64) & ((i >> 5) == (j >> 4)) & (((i & 31) >> 1) == (j & 15)), 0.125)
    return dot(row_pairs(t3, 0, 32), pick)


def from_coarsest(v, t3):
    pick = picks(lambda i, j: (i < 64) & ((j >> 5) == (i >> 4)) & (((j & 31) >> 1) == (i & 15)), 1.0)
    v = dot(v, pick)
    t3[pl.ds(0, 32, stride=2), :] = v
    t3[pl.ds(1, 32, stride=2), :] = v
    parts = []
    for k in range(4):
        block = t3[pl.ds(16 * k, 16), :]
        parts += [block, block]
    return jnp.concatenate(parts, 0)


def coarse_levels(got, caps, first, w1, w2, d2, w3, y1, x1, r1, f1, t3):
    zero = jnp.zeros((32, 128), F32)
    for i in (0, 1, 34, 35):
        y1[i] = zero
        x1[i] = zero
        f1[pl.ds(32 * i, 32), :] = zero
        if first:
            w1[i] = zero

    if first:

        def caps_in(s):
            c = caps[s, pl.ds(32, 32), :]
            w = OMEGA / (c + 3.0)
            w1[s + 2] = w
            y1[s + 2] = w * got[s, pl.ds(0, 32), :]
            r1[pl.ds(pl.multiple_of(s * 32, 32), 32), :] = c

        over_blocks(caps_in)
        c2 = to_low(r1)
        d2[...] = c2 + 1.5
        w2[...] = OMEGA / (c2 + 1.5)
        w3[...] = OMEGA / (to_coarsest(c2, t3) + 0.75)
    else:

        def right_side(s):
            y1[s + 2] = w1[s + 2] * got[s, pl.ds(0, 32), :]

        over_blocks(right_side)

    def sweep(s):
        y = y1[s + 2]
        x1[s + 2] = 1.2 * y + 0.5 * w1[s + 2] * around_block(y, y1[s + 1], y1[s + 3])

    over_blocks(sweep)

    def residual(s):
        x = x1[s + 2]
        r = got[s, pl.ds(0, 32), :] - (caps[s, pl.ds(32, 32), :] + 3.0) * x
        r = r + 0.5 * around_block(x, x1[s + 1], x1[s + 3])
        r1[pl.ds(pl.multiple_of(s * 32, 32), 32), :] = r

    over_blocks(residual)
    b = to_low(r1)
    w, d = w2[...], d2[...]
    y = w * b
    x = 1.2 * y + 0.25 * w * around_low(y)
    r = b - d * x + 0.25 * around_low(x)
    x = x + from_coarsest(coarsest(to_coarsest(r, t3), w3[...]), t3)
    for _ in range(2):
        x = 0.2 * x + y + 0.25 * w * around_low(x)
    for q in range(4):
        pick = picks(lambda i, j: ((i >> 5) == q) & ((i & 31) == ((j & 63) >> 1)), 1.0)
        v = dot(x, pick)
        f1[pl.ds(64 + 256 * q, 128, stride=2), :] = v
        f1[pl.ds(65 + 256 * q, 128, stride=2), :] = v


def fine_up(b_own, lo, hi, w, xs, w1, y1, x1, f1, xa, xb, f0, x0, x9, out):
    s = lax.axis_index("space")
    for j in range(5):
        rows = pl.ds(pl.multiple_of((s + j) * 32, 32), 32)
        xa[j] = x1[s + j] + f1[rows, :]
    xb[0] = jnp.zeros((32, 128), F32)
    xb[4] = jnp.zeros((32, 128), F32)
    for old, new in ((xa, xb), (xb, xa)):
        for j in (1, 2, 3):
            c = old[j]
            t = around_block(c, old[j - 1], old[j + 1])
            new[j] = 0.2 * c + y1[s + j] + 0.5 * w1[s + j] * t
    one, two, three = xa[1], xa[2], xa[3]
    low = dot(jnp.concatenate([two, three], 0), picks(lambda i, j: i == (j >> 1), 1.0))
    high = dot(jnp.concatenate([one, two], 0), picks(lambda i, j: i == (j >> 1) + 64, 1.0))
    for q, v in enumerate((high[:32], low[:32], high[32:], low[32:])):
        f0[pl.ds(64 * q, 32, stride=2), :] = v
        f0[pl.ds(64 * q + 1, 32, stride=2), :] = v
    for i in range(8):
        x0[i] = xs[i] + f0[pl.ds(64 * (i // 2), 64), :]
    for p in range(-1, 5):
        i = p + 2
        b = lo[2] if p < 0 else (b_own[p] if p < DEPTH else hi[0])
        c = x0[i]
        x9[p + 1] = 0.2 * c + w[p + 3] * (b + around_plane(c, x0[i - 1], x0[i + 1]))
    for p in range(DEPTH):
        c = x9[p + 1]
        u = 0.2 * c + w[p + 3] * (b_own[p] + around_plane(c, x9[p], x9[p + 2]))
        out(p, u)


def first_up_body(
    got, b_own, lo, hi, w, xs, cap, src, u_out, b_out, up, dn, w1, w2, d2, w3, *work
):
    y1, x1, r1, f1, t3, xa, xb, f0, x0, x9 = work
    coarse_levels(got, got, True, w1, w2, d2, w3, y1, x1, r1, f1, t3)

    def out(p, u):
        u_out[0, p] = u
        b = cap[p] * u + src[0, 1, p]
        b_out[p] = b
        if p > 0:
            up[p - 1] = b
        if p < 3:
            dn[p] = b

    fine_up(b_own, lo, hi, w, xs, w1, y1, x1, f1, xa, xb, f0, x0, x9, out)


def next_up_body(got, caps, b_own, lo, hi, w, xs, w1, w2, d2, w3, start, u_out, *work):
    y1, x1, r1, f1, t3, xa, xb, f0, x0, x9 = work
    coarse_levels(got, caps, False, w1, w2, d2, w3, y1, x1, r1, f1, t3)
    keep = lax.axis_index("tm") == 0

    def out(p, u):
        u_out[0, p] = jnp.where(keep, start[0, p], u)

    fine_up(b_own, lo, hi, w, xs, w1, y1, x1, f1, xa, xb, f0, x0, x9, out)


WORK = [
    (36, 32, 128),
    (36, 32, 128),
    (1024, 128),
    (36 * 32, 128),
    (64, 128),
    (5, 32, 128),
    (5, 32, 128),
    (256, 128),
    (8, NY, NX),
    (6, NY, NX),
]


def moved(x, spans, slabs):
    pairs = []
    for t in range(SPANS):
        for s in range(SLABS):
            pairs.append((t * SLABS + s, (t + spans) % SPANS * SLABS + (s + slabs) % SLABS))
    return lax.ppermute(x, ("tm", "space"), pairs)


def shards(u0, src, cap):
    plane = (NY, NX)
    b, up, dn = call(
        pack_body, (f32(4, *plane), f32(6, *plane), f32(6, *plane)), [], u0, src, cap
    )
    lo, hi = moved(up, 0, 1), moved(dn, 0, -1)
    w, xs, send = call(
        first_down_body,
        (f32(10, *plane), f32(8, *plane), f32(SLABS, 64, 128)),
        [(10, *plane), (256, 128)],
        b,
        cap,
        lo,
        hi,
    )
    got = lax.all_to_all(send, "space", 0, 0, tiled=True)
    fpoint, b, up, dn, w1, w2, d2, w3 = call(
        first_up_body,
        (
            f32(1, 4, *plane),
            f32(4, *plane),
            f32(3, *plane),
            f32(3, *plane),
            f32(36, 32, 128),
            f32(128, 128),
            f32(128, 128),
            f32(32, 128),
        ),
        WORK,
        got,
        b,
        lo,
        hi,
        w,
        xs,
        cap,
        src,
    )
    b, lo, hi = moved(b, 1, 0), moved(up, 1, 1), moved(dn, 1, -1)
    xs, send = call(
        lambda b, cap, lo, hi, w, xs, send, ys, rs: next_down_body(
            b, cap, lo, hi, w, xs, send, ys, rs
        ),
        (f32(8, *plane), f32(SLABS, 32, 128)),
        [(10, *plane), (256, 128)],
        b,
        cap,
        lo,
        hi,
        w,
    )
    caps = got
    got = lax.all_to_all(send, "space", 0, 0, tiled=True)
    (updated,) = call(
        next_up_body,
        (f32(1, 4, *plane),),
        WORK,
        got,
        caps,
        b,
        lo,
        hi,
        w,
        xs,
        w1,
        w2,
        d2,
        w3,
        u0,
    )
    return fpoint, updated


def solution(mesh):
    in_specs = (
        P("tm", "space", None, None),
        P("tm", None, "space", None, None),
        P("space", None, None),
    )
    out_specs = (P("tm", "space", None, None), P("tm", "space", None, None))
    return jax.shard_map(shards, mesh=mesh, in_specs=in_specs, out_specs=out_specs, check_vma=False)
```

```python
import jax
import jax.numpy as jnp
from jax import lax
from jax.experimental import pallas as pl
from jax.experimental.pallas import tpu as pltpu
from jax.sharding import PartitionSpec as P

COARSE_SWEEPS = 24
NY, NX = 64, 128
SLABS = 32
SPANS = 8
DEPTH = 4
OMEGA = 0.8
F32 = jnp.float32
VMEM = pl.BlockSpec(memory_space=pltpu.VMEM)


def f32(*shape):
    return jax.ShapeDtypeStruct(shape, F32)


def call(body, outs, scratch, *args):
    return pl.pallas_call(
        body,
        out_shape=outs,
        in_specs=[VMEM] * len(args),
        out_specs=tuple(VMEM for _ in outs),
        scratch_shapes=[pltpu.VMEM(s, F32) for s in scratch],
        compiler_params=pltpu.CompilerParams(vmem_limit_bytes=16 << 20),
    )(*args)


def dot(a, b):
    return jnp.dot(a, b, precision=lax.Precision.HIGHEST, preferred_element_type=F32)


def iota(shape, axis):
    return lax.broadcasted_iota(jnp.int32, shape, axis)


def picks(test, scale):
    i, j = iota((128, 128), 0), iota((128, 128), 1)
    return jnp.where(test(i, j), jnp.float32(scale), jnp.float32(0.0))


def around_plane(c, below, above):
    row, lane = iota(c.shape, 0), iota(c.shape, 1)
    total = below + above
    total = total + jnp.where(lane > 0, pltpu.roll(c, 1, 1), 0.0)
    total = total + jnp.where(lane < NX - 1, pltpu.roll(c, NX - 1, 1), 0.0)
    total = total + jnp.where(row > 0, pltpu.roll(c, 1, 0), 0.0)
    return total + jnp.where(row < NY - 1, pltpu.roll(c, NY - 1, 0), 0.0)


def around_block(c, below, above):
    row, lane = iota(c.shape, 0), iota(c.shape, 1)
    col = lane & 63
    total = pltpu.roll(c + jnp.where(lane < 64, above, below), 64, 1)
    total = total + jnp.where(col > 0, pltpu.roll(c, 1, 1), 0.0)
    total = total + jnp.where(col < 63, pltpu.roll(c, 127, 1), 0.0)
    total = total + jnp.where(row > 0, pltpu.roll(c, 1, 0), 0.0)
    return total + jnp.where(row < 31, pltpu.roll(c, 31, 0), 0.0)


def around_low(v):
    row, lane = iota(v.shape, 0), iota(v.shape, 1)
    y, x = row & 15, lane & 31
    ends = iota((16, 128), 1)
    below = jnp.where(ends >= 32, pltpu.roll(v[112:], 32, 1), 0.0)
    above = jnp.where(ends < 96, pltpu.roll(v[:16], 96, 1), 0.0)
    total = jnp.concatenate([below, v[:112]], 0) + jnp.concatenate([v[16:], above], 0)
    total = total + jnp.where(x > 0, pltpu.roll(v, 1, 1), 0.0)
    total = total + jnp.where(x < 31, pltpu.roll(v, 127, 1), 0.0)
    total = total + jnp.where(y > 0, pltpu.roll(v, 1, 0), 0.0)
    return total + jnp.where(y < 15, pltpu.roll(v, 127, 0), 0.0)


def coarsest(b3, w3):
    lane, row = iota((8, 128), 1), iota((8, 128), 0)
    x = lane & 15
    steps = []
    for k in range(4):
        w = w3[8 * k : 8 * k + 8]
        wh = 0.125 * w
        steps.append(
            (
                w * b3[8 * k : 8 * k + 8],
                wh,
                jnp.where(x > 0, wh, 0.0),
                jnp.where(x < 15, wh, 0.0),
                jnp.where(row > 0, wh, 0.0),
                jnp.where(row < 7, wh, 0.0),
            )
        )
    inside = lane < 64

    def sweep(_, v):
        below = jnp.where(inside, pltpu.roll(v[3], 16, 1), 0.0)
        above = jnp.where(inside, pltpu.roll(v[0], 112, 1), 0.0)
        line = (below, *v, above)
        new = []
        for k in range(4):
            wb, wh, left, right, up, down = steps[k]
            c = v[k]
            t = (0.2 * c + wb) + wh * (line[k] + line[k + 2])
            s = up * pltpu.roll(c, 1, 0) + down * pltpu.roll(c, 7, 0)
            e = left * pltpu.roll(c, 1, 1) + right * pltpu.roll(c, 127, 1)
            new.append((t + s) + e)
        return tuple(new)

    v = lax.fori_loop(0, COARSE_SWEEPS - 1, sweep, tuple(s[0] for s in steps), unroll=True)
    return jnp.concatenate(v, 0)


def pack_body(u, src, cap, b_out, up, dn):
    for p in range(DEPTH):
        c = cap[p]
        b = c * u[0, p] + src[0, 0, p]
        b_out[p] = b
        if p > 0:
            up[p - 1] = b
            up[p + 2] = c
        if p < 3:
            dn[p] = b
            dn[p + 3] = c


def row_pairs(ref, start, count):
    return ref[pl.ds(start, count, stride=2), :] + ref[pl.ds(start + 1, count, stride=2), :]


def fine_down(first, b_own, cap, lo, hi, w, xs, send, ys, rs):
    lo_pick = picks(lambda i, j: (i >> 1) == j, 0.125)
    hi_pick = picks(lambda i, j: (i >> 1) + 64 == j, 0.125)

    def b(p):
        return lo[p + 3] if p < 0 else (b_own[p] if p < DEPTH else hi[p - DEPTH])

    if first:
        s = lax.axis_index("space")
        for p in range(-3, 7):
            c = lo[p + 6] if p < 0 else (cap[p] if p < DEPTH else hi[p - 1])
            v = OMEGA / (c + 6.0)
            if p < 0:
                v = jnp.where(s > 0, v, 0.0)
            if p >= DEPTH:
                v = jnp.where(s < SLABS - 1, v, 0.0)
            w[p + 3] = v
    for p in range(-3, 7):
        ys[p + 3] = w[p + 3] * b(p)
    for p in range(-2, 6):
        i = p + 3
        xs[p + 2] = 1.2 * ys[i] + w[i] * around_plane(ys[i], ys[i - 1], ys[i + 1])
    for half in range(2):
        total = None
        for p in (2 * half, 2 * half + 1):
            i = p + 2
            r = b(p) - (cap[p] + 6.0) * xs[i] + around_plane(xs[i], xs[i - 1], xs[i + 1])
            total = r if total is None else total + r
        rs[pl.ds(64 * half, 64), :] = total
        if first:
            rs[pl.ds(128 + 64 * half, 64), :] = cap[2 * half] + cap[2 * half + 1]
    parts = [(row_pairs(rs, 0, 32), row_pairs(rs, 64, 32))]
    if first:
        parts.append((row_pairs(rs, 128, 32), row_pairs(rs, 192, 32)))
    low = jnp.concatenate([a for a, _ in parts], 0)
    high = jnp.concatenate([a for _, a in parts], 0)
    block = dot(low, lo_pick) + dot(high, hi_pick)
    for peer in range(SLABS):
        send[peer] = block


def first_down_body(b_own, cap, lo, hi, w, xs, send, ys, rs):
    fine_down(True, b_own, cap, lo, hi, w, xs, send, ys, rs)


def next_down_body(b_own, cap, lo, hi, w, xs, send, ys, rs):
    fine_down(False, b_own, cap, lo, hi, w, xs, send, ys, rs)


CHUNK = 8


def over_blocks(body):
    @pl.loop(0, SLABS // CHUNK)
    def _(c):
        for k in range(CHUNK):
            body(c * CHUNK + k)


def to_low(rows):
    total = None
    for q in range(4):
        pick = picks(lambda i, j: ((j >> 5) == q) & (((i & 63) >> 1) == (j & 31)), 0.125)
        part = dot(row_pairs(rows, 256 * q, 128), pick)
        total = part if total is None else total + part
    return total


def to_coarsest(v, t3):
    for k in range(4):
        t3[pl.ds(16 * k, 16), :] = v[32 * k : 32 * k + 16] + v[32 * k + 16 : 32 * k + 32]
    pick = picks(lambda i, j: (j < 64) & ((i >> 5) == (j >> 4)) & (((i & 31) >> 1) == (j & 15)), 0.125)
    return dot(row_pairs(t3, 0, 32), pick)


def from_coarsest(v, t3):
    pick = picks(lambda i, j: (i < 64) & ((j >> 5) == (i >> 4)) & (((j & 31) >> 1) == (i & 15)), 1.0)
    v = dot(v, pick)
    t3[pl.ds(0, 32, stride=2), :] = v
    t3[pl.ds(1, 32, stride=2), :] = v
    parts = []
    for k in range(4):
        block = t3[pl.ds(16 * k, 16), :]
        parts += [block, block]
    return jnp.concatenate(parts, 0)


def coarse_levels(got, caps, first, w1, w2, d2, w3, y1, x1, r1, f1, t3):
    zero = jnp.zeros((32, 128), F32)
    for i in (0, 1, 34, 35):
        y1[i] = zero
        x1[i] = zero
        f1[pl.ds(32 * i, 32), :] = zero
        if first:
            w1[i] = zero

    if first:

        def caps_in(s):
            c = caps[s, pl.ds(32, 32), :]
            w = OMEGA / (c + 3.0)
            w1[s + 2] = w
            y1[s + 2] = w * got[s, pl.ds(0, 32), :]
            r1[pl.ds(pl.multiple_of(s * 32, 32), 32), :] = c

        over_blocks(caps_in)
        c2 = to_low(r1)
        d2[...] = c2 + 1.5
        w2[...] = OMEGA / (c2 + 1.5)
        w3[...] = OMEGA / (to_coarsest(c2, t3) + 0.75)
    else:

        def right_side(s):
            y1[s + 2] = w1[s + 2] * got[s, pl.ds(0, 32), :]

        over_blocks(right_side)

    def sweep(s):
        y = y1[s + 2]
        x1[s + 2] = 1.2 * y + 0.5 * w1[s + 2] * around_block(y, y1[s + 1], y1[s + 3])

    over_blocks(sweep)

    def residual(s):
        x = x1[s + 2]
        r = got[s, pl.ds(0, 32), :] - (caps[s, pl.ds(32, 32), :] + 3.0) * x
        r = r + 0.5 * around_block(x, x1[s + 1], x1[s + 3])
        r1[pl.ds(pl.multiple_of(s * 32, 32), 32), :] = r

    over_blocks(residual)
    b = to_low(r1)
    w, d = w2[...], d2[...]
    y = w * b
    x = 1.2 * y + 0.25 * w * around_low(y)
    r = b - d * x + 0.25 * around_low(x)
    x = x + from_coarsest(coarsest(to_coarsest(r, t3), w3[...]), t3)
    for _ in range(2):
        x = 0.2 * x + y + 0.25 * w * around_low(x)
    for q in range(4):
        pick = picks(lambda i, j: ((i >> 5) == q) & ((i & 31) == ((j & 63) >> 1)), 1.0)
        v = dot(x, pick)
        f1[pl.ds(64 + 256 * q, 128, stride=2), :] = v
        f1[pl.ds(65 + 256 * q, 128, stride=2), :] = v


def fine_up(b_own, lo, hi, w, xs, w1, y1, x1, f1, xa, xb, f0, x0, x9, out):
    s = lax.axis_index("space")
    for j in range(5):
        rows = pl.ds(pl.multiple_of((s + j) * 32, 32), 32)
        xa[j] = x1[s + j] + f1[rows, :]
    xb[0] = jnp.zeros((32, 128), F32)
    xb[4] = jnp.zeros((32, 128), F32)
    for old, new in ((xa, xb), (xb, xa)):
        for j in (1, 2, 3):
            c = old[j]
            t = around_block(c, old[j - 1], old[j + 1])
            new[j] = 0.2 * c + y1[s + j] + 0.5 * w1[s + j] * t
    one, two, three = xa[1], xa[2], xa[3]
    low = dot(jnp.concatenate([two, three], 0), picks(lambda i, j: i == (j >> 1), 1.0))
    high = dot(jnp.concatenate([one, two], 0), picks(lambda i, j: i == (j >> 1) + 64, 1.0))
    for q, v in enumerate((high[:32], low[:32], high[32:], low[32:])):
        f0[pl.ds(64 * q, 32, stride=2), :] = v
        f0[pl.ds(64 * q + 1, 32, stride=2), :] = v
    for i in range(8):
        x0[i] = xs[i] + f0[pl.ds(64 * (i // 2), 64), :]
    for p in range(-1, 5):
        i = p + 2
        b = lo[2] if p < 0 else (b_own[p] if p < DEPTH else hi[0])
        c = x0[i]
        x9[p + 1] = 0.2 * c + w[p + 3] * (b + around_plane(c, x0[i - 1], x0[i + 1]))
    for p in range(DEPTH):
        c = x9[p + 1]
        u = 0.2 * c + w[p + 3] * (b_own[p] + around_plane(c, x9[p], x9[p + 2]))
        out(p, u)


def first_up_body(
    got, b_own, lo, hi, w, xs, cap, src, u_out, b_out, up, dn, w1, w2, d2, w3, *work
):
    y1, x1, r1, f1, t3, xa, xb, f0, x0, x9 = work
    coarse_levels(got, got, True, w1, w2, d2, w3, y1, x1, r1, f1, t3)

    def out(p, u):
        u_out[0, p] = u
        b = cap[p] * u + src[0, 1, p]
        b_out[p] = b
        if p > 0:
            up[p - 1] = b
        if p < 3:
            dn[p] = b

    fine_up(b_own, lo, hi, w, xs, w1, y1, x1, f1, xa, xb, f0, x0, x9, out)


def next_up_body(got, caps, b_own, lo, hi, w, xs, w1, w2, d2, w3, start, u_out, *work):
    y1, x1, r1, f1, t3, xa, xb, f0, x0, x9 = work
    coarse_levels(got, caps, False, w1, w2, d2, w3, y1, x1, r1, f1, t3)
    keep = lax.axis_index("tm") == 0

    def out(p, u):
        u_out[0, p] = jnp.where(keep, start[0, p], u)

    fine_up(b_own, lo, hi, w, xs, w1, y1, x1, f1, xa, xb, f0, x0, x9, out)


WORK = [
    (36, 32, 128),
    (36, 32, 128),
    (1024, 128),
    (36 * 32, 128),
    (64, 128),
    (5, 32, 128),
    (5, 32, 128),
    (256, 128),
    (8, NY, NX),
    (6, NY, NX),
]


def moved(x, spans, slabs):
    pairs = []
    for t in range(SPANS):
        for s in range(SLABS):
            pairs.append((t * SLABS + s, (t + spans) % SPANS * SLABS + (s + slabs) % SLABS))
    return lax.ppermute(x, ("tm", "space"), pairs)


def shards(u0, src, cap):
    plane = (NY, NX)
    b, up, dn = call(
        pack_body, (f32(4, *plane), f32(6, *plane), f32(6, *plane)), [], u0, src, cap
    )
    lo, hi = moved(up, 0, 1), moved(dn, 0, -1)
    w, xs, send = call(
        first_down_body,
        (f32(10, *plane), f32(8, *plane), f32(SLABS, 64, 128)),
        [(10, *plane), (256, 128)],
        b,
        cap,
        lo,
        hi,
    )
    got = lax.all_to_all(send, "space", 0, 0, tiled=True)
    fpoint, b, up, dn, w1, w2, d2, w3 = call(
        first_up_body,
        (
            f32(1, 4, *plane),
            f32(4, *plane),
            f32(3, *plane),
            f32(3, *plane),
            f32(36, 32, 128),
            f32(128, 128),
            f32(128, 128),
            f32(32, 128),
        ),
        WORK,
        got,
        b,
        lo,
        hi,
        w,
        xs,
        cap,
        src,
    )
    b, lo, hi = moved(b, 1, 0), moved(up, 1, 1), moved(dn, 1, -1)
    xs, send = call(
        lambda b, cap, lo, hi, w, xs, send, ys, rs: next_down_body(
            b, cap, lo, hi, w, xs, send, ys, rs
        ),
        (f32(8, *plane), f32(SLABS, 32, 128)),
        [(10, *plane), (256, 128)],
        b,
        cap,
        lo,
        hi,
        w,
    )
    caps = got
    got = lax.all_to_all(send, "space", 0, 0, tiled=True)
    (updated,) = call(
        next_up_body,
        (f32(1, 4, *plane),),
        WORK,
        got,
        caps,
        b,
        lo,
        hi,
        w,
        xs,
        w1,
        w2,
        d2,
        w3,
        u0,
    )
    return fpoint, updated


def solution(mesh):
    in_specs = (
        P("tm", "space", None, None),
        P("tm", None, "space", None, None),
        P("space", None, None),
    )
    out_specs = (P("tm", "space", None, None), P("tm", "space", None, None))
    return jax.shard_map(shards, mesh=mesh, in_specs=in_specs, out_specs=out_specs, check_vma=False)
```

```python
import jax
import jax.numpy as jnp
from jax import lax
from jax.experimental import pallas as pl
from jax.experimental.pallas import tpu as pltpu
from jax.sharding import PartitionSpec as P

COARSE_SWEEPS = 24
NY, NX = 64, 128
SLABS = 32
SPANS = 8
DEPTH = 4
OMEGA = 0.8
F32 = jnp.float32
VMEM = pl.BlockSpec(memory_space=pltpu.VMEM)


def f32(*shape):
    return jax.ShapeDtypeStruct(shape, F32)


def call(body, outs, scratch, *args):
    return pl.pallas_call(
        body,
        out_shape=outs,
        in_specs=[VMEM] * len(args),
        out_specs=tuple(VMEM for _ in outs),
        scratch_shapes=[pltpu.VMEM(s, F32) for s in scratch],
        compiler_params=pltpu.CompilerParams(vmem_limit_bytes=16 << 20),
    )(*args)


def dot(a, b):
    return jnp.dot(a, b, precision=lax.Precision.HIGHEST, preferred_element_type=F32)


def iota(shape, axis):
    return lax.broadcasted_iota(jnp.int32, shape, axis)


def picks(test, scale):
    i, j = iota((128, 128), 0), iota((128, 128), 1)
    return jnp.where(test(i, j), jnp.float32(scale), jnp.float32(0.0))


def around_plane(c, below, above):
    row, lane = iota(c.shape, 0), iota(c.shape, 1)
    total = below + above
    total = total + jnp.where(lane > 0, pltpu.roll(c, 1, 1), 0.0)
    total = total + jnp.where(lane < NX - 1, pltpu.roll(c, NX - 1, 1), 0.0)
    total = total + jnp.where(row > 0, pltpu.roll(c, 1, 0), 0.0)
    return total + jnp.where(row < NY - 1, pltpu.roll(c, NY - 1, 0), 0.0)


def around_block(c, below, above):
    row, lane = iota(c.shape, 0), iota(c.shape, 1)
    col = lane & 63
    total = pltpu.roll(c + jnp.where(lane < 64, above, below), 64, 1)
    total = total + jnp.where(col > 0, pltpu.roll(c, 1, 1), 0.0)
    total = total + jnp.where(col < 63, pltpu.roll(c, 127, 1), 0.0)
    total = total + jnp.where(row > 0, pltpu.roll(c, 1, 0), 0.0)
    return total + jnp.where(row < 31, pltpu.roll(c, 31, 0), 0.0)


def around_low(v):
    row, lane = iota(v.shape, 0), iota(v.shape, 1)
    y, x = row & 15, lane & 31
    ends = iota((16, 128), 1)
    below = jnp.where(ends >= 32, pltpu.roll(v[112:], 32, 1), 0.0)
    above = jnp.where(ends < 96, pltpu.roll(v[:16], 96, 1), 0.0)
    total = jnp.concatenate([below, v[:112]], 0) + jnp.concatenate([v[16:], above], 0)
    total = total + jnp.where(x > 0, pltpu.roll(v, 1, 1), 0.0)
    total = total + jnp.where(x < 31, pltpu.roll(v, 127, 1), 0.0)
    total = total + jnp.where(y > 0, pltpu.roll(v, 1, 0), 0.0)
    return total + jnp.where(y < 15, pltpu.roll(v, 127, 0), 0.0)


def coarsest(b3, w3):
    lane, row = iota((8, 128), 1), iota((8, 128), 0)
    x = lane & 15
    steps = []
    for k in range(4):
        w = w3[8 * k : 8 * k + 8]
        wh = 0.125 * w
        steps.append(
            (
                w * b3[8 * k : 8 * k + 8],
                wh,
                jnp.where(x > 0, wh, 0.0),
                jnp.where(x < 15, wh, 0.0),
                jnp.where(row > 0, wh, 0.0),
                jnp.where(row < 7, wh, 0.0),
            )
        )
    inside = lane < 64

    def sweep(_, v):
        below = jnp.where(inside, pltpu.roll(v[3], 16, 1), 0.0)
        above = jnp.where(inside, pltpu.roll(v[0], 112, 1), 0.0)
        line = (below, *v, above)
        new = []
        for k in range(4):
            wb, wh, left, right, up, down = steps[k]
            c = v[k]
            t = (0.2 * c + wb) + wh * (line[k] + line[k + 2])
            s = up * pltpu.roll(c, 1, 0) + down * pltpu.roll(c, 7, 0)
            e = left * pltpu.roll(c, 1, 1) + right * pltpu.roll(c, 127, 1)
            new.append((t + s) + e)
        return tuple(new)

    v = lax.fori_loop(0, COARSE_SWEEPS - 1, sweep, tuple(s[0] for s in steps), unroll=True)
    return jnp.concatenate(v, 0)


def pack_body(u, src, cap, b_out, up, dn):
    for p in range(DEPTH):
        c = cap[p]
        b = c * u[0, p] + src[0, 0, p]
        b_out[p] = b
        ends, i = (dn, p) if p < 2 else (up, p - 2)
        ends[i] = b
        ends[i + 2] = c


def row_pairs(ref, start, count):
    return ref[pl.ds(start, count, stride=2), :] + ref[pl.ds(start + 1, count, stride=2), :]


def block_sweep(y, w, below, above):
    return 1.2 * y + 0.5 * w * around_block(y, below, above)


def fine_down(first, b_own, cap, lo, hi, w, w1, c1, xs, send, up, dn, block, ys, rs):
    lane = iota((32, 128), 1)
    lo_pick = picks(lambda i, j: (i >> 1) == j, 0.125)
    hi_pick = picks(lambda i, j: (i >> 1) + 64 == j, 0.125)

    def b(p):
        return lo[p + 2] if p < 0 else (b_own[p] if p < DEPTH else hi[p - DEPTH])

    def c(p):
        return lo[p + 4] if p < 0 else (cap[p] if p < DEPTH else hi[p - 2])

    if first:
        s = lax.axis_index("space")
        for p in range(-2, 6):
            v = OMEGA / (c(p) + 6.0)
            if p < 0:
                v = jnp.where(s > 0, v, 0.0)
            if p >= DEPTH:
                v = jnp.where(s < SLABS - 1, v, 0.0)
            w[p + 2] = v
    for p in range(-2, 6):
        ys[p + 2] = w[p + 2] * b(p)
    for p in range(-1, 5):
        i = p + 2
        xs[p + 1] = 1.2 * ys[i] + w[i] * around_plane(ys[i], ys[i - 1], ys[i + 1])
    for half in range(2):
        total = None
        for p in (2 * half, 2 * half + 1):
            i = p + 1
            r = b(p) - (cap[p] + 6.0) * xs[i] + around_plane(xs[i], xs[i - 1], xs[i + 1])
            total = r if total is None else total + r
        rs[pl.ds(64 * half, 64), :] = total
    if first:
        for k, p in enumerate((0, 2, 4, -2)):
            rs[pl.ds(128 + 64 * k, 64), :] = c(p) + c(p + 1)
    low, high = [row_pairs(rs, 0, 32)], [row_pairs(rs, 64, 32)]
    if first:
        low += [row_pairs(rs, 128, 32), row_pairs(rs, 256, 32)]
        high += [row_pairs(rs, 192, 32), row_pairs(rs, 320, 32)]
    blocks = dot(jnp.concatenate(low, 0), lo_pick) + dot(jnp.concatenate(high, 0), hi_pick)
    b1 = blocks[:32]
    if first:
        c1[0], c1[1] = blocks[32:64], blocks[64:]
        wide = OMEGA / (blocks[64:] + 3.0)
        w1[0] = jnp.where((lane >= 64) & (s > 0), wide, 0.0)
        w1[1] = OMEGA / (blocks[32:64] + 3.0)
        w1[2] = jnp.where((lane < 64) & (s < SLABS - 1), wide, 0.0)
    rows = 64 if first else 32
    block[...] = blocks[:rows]
    up[pl.ds(0, rows), :] = blocks[:rows]
    dn[pl.ds(0, rows), :] = blocks[:rows]
    up[pl.ds(rows, 64), :] = xs[3]
    dn[pl.ds(rows, 64), :] = xs[2]

    zero = jnp.zeros((32, 128), F32)
    y = w1[1] * b1
    x = [
        block_sweep(zero, w1[0], zero, y),
        block_sweep(y, w1[1], zero, zero),
        block_sweep(zero, w1[2], y, zero),
    ]
    own, beside = c1[0] + 3.0, c1[1] + 3.0
    r = [
        0.5 * around_block(x[0], zero, x[1]) - beside * x[0],
        b1 - own * x[1] + 0.5 * around_block(x[1], x[0], x[2]),
        0.5 * around_block(x[2], x[1], zero) - beside * x[2],
        c1[0],
    ]
    for k in range(4):
        rs[pl.ds(32 * k, 32), :] = r[k]
    low = dot(row_pairs(rs, 0, 64), picks(lambda i, j: ((i & 63) >> 1) == (j & 31), 0.125))
    group = iota((16, 128), 1) >> 5
    message = low[48:]
    for k in range(3):
        message = jnp.where(group == k, low[16 * k : 16 * k + 16], message)
    for peer in range(SLABS):
        send[peer] = message


def first_down_body(b_own, cap, lo, hi, *rest):
    fine_down(True, b_own, cap, lo, hi, *rest)


def next_down_body(*refs):
    fine_down(False, *refs)


def spread(v):
    v = v + pltpu.roll(v, 64, 1)
    return v + pltpu.roll(v, 32, 1)


def to_coarsest(v, t3):
    for k in range(4):
        t3[pl.ds(16 * k, 16), :] = v[32 * k : 32 * k + 16] + v[32 * k + 16 : 32 * k + 32]
    pick = picks(lambda i, j: (j < 64) & ((i >> 5) == (j >> 4)) & (((i & 31) >> 1) == (j & 15)), 0.125)
    return dot(row_pairs(t3, 0, 32), pick)


def from_coarsest(v, t3):
    pick = picks(lambda i, j: (i < 64) & ((j >> 5) == (i >> 4)) & (((j & 31) >> 1) == (i & 15)), 1.0)
    v = dot(v, pick)
    t3[pl.ds(0, 32, stride=2), :] = v
    t3[pl.ds(1, 32, stride=2), :] = v
    parts = []
    for k in range(4):
        block = t3[pl.ds(16 * k, 16), :]
        parts += [block, block]
    return jnp.concatenate(parts, 0)


def low_levels(got, first, w2, d2, w3, x2, t3):
    group = iota((16, 128), 1) >> 5
    parts, caps = [], []
    for zl in range(8):
        total, cap = None, None
        for zh in range(4):
            z = 8 * zh + zl
            v = jnp.where(group == 1, got[z], 0.0)
            if z + 1 < SLABS:
                v = jnp.where(group == 0, got[z + 1], v)
            if z > 0:
                v = jnp.where(group == 2, got[z - 1], v)
            v = spread(v)
            total = v if total is None else jnp.where(group == zh, v, total)
            if first:
                v = spread(jnp.where(group == 3, got[z], 0.0))
                cap = v if cap is None else jnp.where(group == zh, v, cap)
        parts.append(total)
        caps.append(cap)
    b = jnp.concatenate(parts, 0)
    if first:
        c2 = jnp.concatenate(caps, 0)
        d2[...] = c2 + 1.5
        w2[...] = OMEGA / (c2 + 1.5)
        w3[...] = OMEGA / (to_coarsest(c2, t3) + 0.75)
    w, d = w2[...], d2[...]
    y = w * b
    x = 1.2 * y + 0.25 * w * around_low(y)
    r = b - d * x + 0.25 * around_low(x)
    x = x + from_coarsest(coarsest(to_coarsest(r, t3), w3[...]), t3)
    for _ in range(2):
        x = 0.2 * x + y + 0.25 * w * around_low(x)
    x2[...] = x


def fine_up(got, near, first, b_own, lo, hi, w, xs, w1, w2, d2, w3, work, out):
    x2, t3, f1, y1, xa, xb, f0, x0, x9 = work
    low_levels(got, first, w2, d2, w3, x2, t3)
    s = lax.axis_index("space")
    lo2, lo1, block, hi1, hi2 = near
    for j, ref in enumerate(near):
        if first:
            v = OMEGA / (ref[pl.ds(32, 32), :] + 3.0)
            z = s + (j - 2)
            w1[j] = jnp.where((z >= 0) & (z < SLABS), v, 0.0)
        y1[j] = w1[j] * ref[pl.ds(0, 32), :]
    zero = jnp.zeros((32, 128), F32)
    group = iota((16, 128), 1) >> 5
    parts = []
    for j in range(5):
        z = s + (j - 2)
        v = x2[pl.ds(pl.multiple_of((z & 7) * 16, 16), 16), :]
        parts.append(spread(jnp.where(group == (z >> 3), v, 0.0)))
    pick = picks(lambda i, j: i == ((j & 63) >> 1), 1.0)
    v = dot(jnp.concatenate(parts, 0), pick)
    f1[pl.ds(0, 80, stride=2), :] = v
    f1[pl.ds(1, 80, stride=2), :] = v
    for j in range(5):
        below = y1[j - 1] if j > 0 else zero
        above = y1[j + 1] if j < 4 else zero
        xa[j] = block_sweep(y1[j], w1[j], below, above) + f1[pl.ds(32 * j, 32), :]
    xb[0] = zero
    xb[4] = zero
    for old, new in ((xa, xb), (xb, xa)):
        for j in (1, 2, 3):
            c = old[j]
            t = around_block(c, old[j - 1], old[j + 1])
            new[j] = 0.2 * c + y1[j] + 0.5 * w1[j] * t
    one, two, three = xa[1], xa[2], xa[3]
    low = dot(jnp.concatenate([two, three], 0), picks(lambda i, j: i == (j >> 1), 1.0))
    high = dot(jnp.concatenate([one, two], 0), picks(lambda i, j: i == (j >> 1) + 64, 1.0))
    for q, v in enumerate((high[:32], low[:32], high[32:], low[32:])):
        f0[pl.ds(64 * q, 32, stride=2), :] = v
        f0[pl.ds(64 * q + 1, 32, stride=2), :] = v
    rows = 64 if first else 32
    far_below = jnp.where(s > 0, lo1[pl.ds(rows, 64), :], 0.0)
    far_above = jnp.where(s < SLABS - 1, hi1[pl.ds(rows, 64), :], 0.0)
    for i in range(8):
        v = far_below if i == 0 else (far_above if i == 7 else xs[i - 1])
        x0[i] = v + f0[pl.ds(64 * (i // 2), 64), :]
    for p in range(-1, 5):
        i = p + 2
        b = lo[1] if p < 0 else (b_own[p] if p < DEPTH else hi[0])
        c = x0[i]
        x9[p + 1] = 0.2 * c + w[i] * (b + around_plane(c, x0[i - 1], x0[i + 1]))
    for p in range(DEPTH):
        c = x9[p + 1]
        u = 0.2 * c + w[p + 2] * (b_own[p] + around_plane(c, x9[p], x9[p + 2]))
        out(p, u)


def first_up_body(
    got, lo2, lo1, block, hi1, hi2, b_own, lo, hi, w, xs, cap, src,
    u_out, b_out, up, dn, w1, w2, d2, w3, *work
):
    def out(p, u):
        u_out[0, p] = u
        b = cap[p] * u + src[0, 1, p]
        b_out[p] = b
        ends, i = (dn, p) if p < 2 else (up, p - 2)
        ends[i] = b

    near = (lo2, lo1, block, hi1, hi2)
    fine_up(got, near, True, b_own, lo, hi, w, xs, w1, w2, d2, w3, work, out)


def next_up_body(
    got, lo2, lo1, block, hi1, hi2, b_own, lo, hi, w, xs, w1, w2, d2, w3, start, u_out, *work
):
    keep = lax.axis_index("tm") == 0

    def out(p, u):
        u_out[0, p] = jnp.where(keep, start[0, p], u)

    near = (lo2, lo1, block, hi1, hi2)
    fine_up(got, near, False, b_own, lo, hi, w, xs, w1, w2, d2, w3, work, out)


WORK = [
    (128, 128),
    (64, 128),
    (160, 128),
    (5, 32, 128),
    (5, 32, 128),
    (5, 32, 128),
    (256, 128),
    (8, NY, NX),
    (6, NY, NX),
]
DOWN_WORK = [(8, NY, NX), (384, 128)]
PLANE = (NY, NX)
MESSAGE = f32(SLABS, 16, 128)


def moved(x, spans, slabs):
    pairs = []
    for t in range(SPANS):
        for s in range(SLABS):
            pairs.append((t * SLABS + s, (t + spans) % SPANS * SLABS + (s + slabs) % SLABS))
    return lax.ppermute(x, ("tm", "space"), pairs)


def exchanged(send, up, dn, block):
    lo1, hi1 = moved(up, 0, 1), moved(dn, 0, -1)
    lo2, hi2 = moved(block, 0, 2), moved(block, 0, -2)
    got = lax.all_to_all(send, "space", 0, 0, tiled=True)
    return got, lo2, lo1, block, hi1, hi2


def shards(u0, src, cap):
    b, up, dn = call(pack_body, (f32(4, *PLANE), f32(4, *PLANE), f32(4, *PLANE)), [], u0, src, cap)
    lo, hi = moved(up, 0, 1), moved(dn, 0, -1)
    w, w1, c1, xs, send, up, dn, block = call(
        first_down_body,
        (
            f32(8, *PLANE),
            f32(3, 32, 128),
            f32(2, 32, 128),
            f32(6, *PLANE),
            MESSAGE,
            f32(128, 128),
            f32(128, 128),
            f32(64, 128),
        ),
        DOWN_WORK,
        *(b, cap, lo, hi),
    )
    fpoint, b, up, dn, v1, w2, d2, w3 = call(
        first_up_body,
        (
            f32(1, 4, *PLANE),
            f32(4, *PLANE),
            f32(2, *PLANE),
            f32(2, *PLANE),
            f32(5, 32, 128),
            f32(128, 128),
            f32(128, 128),
            f32(32, 128),
        ),
        WORK,
        *exchanged(send, up, dn, block),
        *(b, lo, hi, w, xs, cap, src),
    )
    b, lo, hi = moved(b, 1, 0), moved(up, 1, 1), moved(dn, 1, -1)
    xs, send, up, dn, block = call(
        next_down_body,
        (f32(6, *PLANE), MESSAGE, f32(96, 128), f32(96, 128), f32(32, 128)),
        DOWN_WORK,
        *(b, cap, lo, hi, w, w1, c1),
    )
    (updated,) = call(
        next_up_body,
        (f32(1, 4, *PLANE),),
        WORK,
        *exchanged(send, up, dn, block),
        *(b, lo, hi, w, xs, v1, w2, d2, w3, u0),
    )
    return fpoint, updated


def solution(mesh):
    in_specs = (
        P("tm", "space", None, None),
        P("tm", None, "space", None, None),
        P("space", None, None),
    )
    out_specs = (P("tm", "space", None, None), P("tm", "space", None, None))
    return jax.shard_map(shards, mesh=mesh, in_specs=in_specs, out_specs=out_specs, check_vma=False)
```

```python
import jax
import jax.numpy as jnp
from jax import lax
from jax.experimental import pallas as pl
from jax.experimental.pallas import tpu as pltpu
from jax.sharding import PartitionSpec as P

COARSE_SWEEPS = 24
NY, NX = 64, 128
SLABS = 32
SPANS = 8
DEPTH = 4
OMEGA = 0.8
F32 = jnp.float32
VMEM = pl.BlockSpec(memory_space=pltpu.VMEM)


def f32(*shape):
    return jax.ShapeDtypeStruct(shape, F32)


def call(body, outs, scratch, *args, space=VMEM, flops=None, sems=()):
    return pl.pallas_call(
        body,
        out_shape=outs,
        in_specs=[space] * len(args),
        out_specs=tuple(VMEM for _ in outs),
        scratch_shapes=[pltpu.VMEM(s, F32) for s in scratch] + list(sems),
        compiler_params=pltpu.CompilerParams(vmem_limit_bytes=16 << 20),
        cost_estimate=flops and pl.CostEstimate(flops=flops, transcendentals=0, bytes_accessed=0),
    )(*args)


def dot(a, b):
    return jnp.dot(a, b, precision=lax.Precision.HIGHEST, preferred_element_type=F32)


def iota(shape, axis):
    return lax.broadcasted_iota(jnp.int32, shape, axis)


def picks(test, scale):
    i, j = iota((128, 128), 0), iota((128, 128), 1)
    return jnp.where(test(i, j), jnp.float32(scale), jnp.float32(0.0))


def around_plane(c, below, above):
    row, lane = iota(c.shape, 0), iota(c.shape, 1)
    total = below + above
    total = total + jnp.where(lane > 0, pltpu.roll(c, 1, 1), 0.0)
    total = total + jnp.where(lane < NX - 1, pltpu.roll(c, NX - 1, 1), 0.0)
    total = total + jnp.where(row > 0, pltpu.roll(c, 1, 0), 0.0)
    return total + jnp.where(row < NY - 1, pltpu.roll(c, NY - 1, 0), 0.0)


def around_block(c, below, above):
    row, lane = iota(c.shape, 0), iota(c.shape, 1)
    col = lane & 63
    total = pltpu.roll(c + jnp.where(lane < 64, above, below), 64, 1)
    total = total + jnp.where(col > 0, pltpu.roll(c, 1, 1), 0.0)
    total = total + jnp.where(col < 63, pltpu.roll(c, 127, 1), 0.0)
    total = total + jnp.where(row > 0, pltpu.roll(c, 1, 0), 0.0)
    return total + jnp.where(row < 31, pltpu.roll(c, 31, 0), 0.0)


def around_low(v):
    row, lane = iota(v.shape, 0), iota(v.shape, 1)
    y, x = row & 15, lane & 31
    ends = iota((16, 128), 1)
    below = jnp.where(ends >= 32, pltpu.roll(v[112:], 32, 1), 0.0)
    above = jnp.where(ends < 96, pltpu.roll(v[:16], 96, 1), 0.0)
    total = jnp.concatenate([below, v[:112]], 0) + jnp.concatenate([v[16:], above], 0)
    total = total + jnp.where(x > 0, pltpu.roll(v, 1, 1), 0.0)
    total = total + jnp.where(x < 31, pltpu.roll(v, 127, 1), 0.0)
    total = total + jnp.where(y > 0, pltpu.roll(v, 1, 0), 0.0)
    return total + jnp.where(y < 15, pltpu.roll(v, 127, 0), 0.0)


def coarsest(b3, w3):
    lane, row = iota((8, 128), 1), iota((8, 128), 0)
    x = lane & 15
    steps = []
    for k in range(4):
        w = w3[8 * k : 8 * k + 8]
        wh = 0.125 * w
        steps.append(
            (
                w * b3[8 * k : 8 * k + 8],
                wh,
                jnp.where(x > 0, wh, 0.0),
                jnp.where(x < 15, wh, 0.0),
                jnp.where(row > 0, wh, 0.0),
                jnp.where(row < 7, wh, 0.0),
            )
        )
    inside = lane < 64

    def sweep(_, v):
        below = jnp.where(inside, pltpu.roll(v[3], 16, 1), 0.0)
        above = jnp.where(inside, pltpu.roll(v[0], 112, 1), 0.0)
        line = (below, *v, above)
        new = []
        for k in range(4):
            wb, wh, left, right, up, down = steps[k]
            c = v[k]
            t = (0.2 * c + wb) + wh * (line[k] + line[k + 2])
            s = up * pltpu.roll(c, 1, 0) + down * pltpu.roll(c, 7, 0)
            e = left * pltpu.roll(c, 1, 1) + right * pltpu.roll(c, 127, 1)
            new.append((t + s) + e)
        return tuple(new)

    v = lax.fori_loop(0, COARSE_SWEEPS - 1, sweep, tuple(s[0] for s in steps), unroll=True)
    return jnp.concatenate(v, 0)


def pack_body(u, src, cap, b_out, up, dn, cap_out, u_in, src_in, sems):
    copies = [
        pltpu.make_async_copy(cap, cap_out, sems.at[0]),
        pltpu.make_async_copy(u.at[0], u_in, sems.at[1]),
        pltpu.make_async_copy(src.at[0, 0], src_in, sems.at[2]),
    ]
    for copy in copies:
        copy.start()
    for copy in copies:
        copy.wait()
    for p in range(DEPTH):
        c = cap_out[p]
        b = c * u_in[p] + src_in[p]
        b_out[p] = b
        ends, i = (dn, p) if p < 2 else (up, p - 2)
        ends[i] = b
        ends[i + 2] = c


def row_pairs(ref, start, count):
    return ref[pl.ds(start, count, stride=2), :] + ref[pl.ds(start + 1, count, stride=2), :]


def block_sweep(y, w, below, above):
    return 1.2 * y + 0.5 * w * around_block(y, below, above)


def fine_down(first, b_own, cap, lo, hi, w, w1, c1, xs, send, up, dn, block, ys, rs):
    lane = iota((32, 128), 1)
    lo_pick = picks(lambda i, j: (i >> 1) == j, 0.125)
    hi_pick = picks(lambda i, j: (i >> 1) + 64 == j, 0.125)

    def b(p):
        return lo[p + 2] if p < 0 else (b_own[p] if p < DEPTH else hi[p - DEPTH])

    def c(p):
        return lo[p + 4] if p < 0 else (cap[p] if p < DEPTH else hi[p - 2])

    if first:
        s = lax.axis_index("space")
        for p in range(-2, 6):
            v = OMEGA / (c(p) + 6.0)
            if p < 0:
                v = jnp.where(s > 0, v, 0.0)
            if p >= DEPTH:
                v = jnp.where(s < SLABS - 1, v, 0.0)
            w[p + 2] = v
    for p in range(-2, 6):
        ys[p + 2] = w[p + 2] * b(p)
    for p in range(-1, 5):
        i = p + 2
        xs[p + 1] = 1.2 * ys[i] + w[i] * around_plane(ys[i], ys[i - 1], ys[i + 1])
    for half in range(2):
        total = None
        for p in (2 * half, 2 * half + 1):
            i = p + 1
            r = b(p) - (cap[p] + 6.0) * xs[i] + around_plane(xs[i], xs[i - 1], xs[i + 1])
            total = r if total is None else total + r
        rs[pl.ds(64 * half, 64), :] = total
    if first:
        for k, p in enumerate((0, 2, 4, -2)):
            rs[pl.ds(128 + 64 * k, 64), :] = c(p) + c(p + 1)
    low, high = [row_pairs(rs, 0, 32)], [row_pairs(rs, 64, 32)]
    if first:
        low += [row_pairs(rs, 128, 32), row_pairs(rs, 256, 32)]
        high += [row_pairs(rs, 192, 32), row_pairs(rs, 320, 32)]
    blocks = dot(jnp.concatenate(low, 0), lo_pick) + dot(jnp.concatenate(high, 0), hi_pick)
    b1 = blocks[:32]
    if first:
        c1[0], c1[1] = blocks[32:64], blocks[64:]
        wide = OMEGA / (blocks[64:] + 3.0)
        w1[0] = jnp.where((lane >= 64) & (s > 0), wide, 0.0)
        w1[1] = OMEGA / (blocks[32:64] + 3.0)
        w1[2] = jnp.where((lane < 64) & (s < SLABS - 1), wide, 0.0)
    rows = 64 if first else 32
    block[...] = blocks[:rows]
    up[pl.ds(0, rows), :] = blocks[:rows]
    dn[pl.ds(0, rows), :] = blocks[:rows]
    up[pl.ds(rows, 64), :] = xs[3]
    dn[pl.ds(rows, 64), :] = xs[2]

    zero = jnp.zeros((32, 128), F32)
    y = w1[1] * b1
    x = [
        block_sweep(zero, w1[0], zero, y),
        block_sweep(y, w1[1], zero, zero),
        block_sweep(zero, w1[2], y, zero),
    ]
    own, beside = c1[0] + 3.0, c1[1] + 3.0
    r = [
        0.5 * around_block(x[0], zero, x[1]) - beside * x[0],
        b1 - own * x[1] + 0.5 * around_block(x[1], x[0], x[2]),
        0.5 * around_block(x[2], x[1], zero) - beside * x[2],
        c1[0],
    ]
    for k in range(4):
        rs[pl.ds(32 * k, 32), :] = r[k]
    low = dot(row_pairs(rs, 0, 64), picks(lambda i, j: ((i & 63) >> 1) == (j & 31), 0.125))
    group = iota((16, 128), 1) >> 5
    message = low[48:]
    for k in range(3):
        message = jnp.where(group == k, low[16 * k : 16 * k + 16], message)
    for peer in range(SLABS):
        send[peer] = message


def first_down_body(b_own, cap, lo, hi, *rest):
    fine_down(True, b_own, cap, lo, hi, *rest)


def next_down_body(*refs):
    fine_down(False, *refs)


def spread(v):
    v = v + pltpu.roll(v, 64, 1)
    return v + pltpu.roll(v, 32, 1)


def to_coarsest(v, t3):
    for k in range(4):
        t3[pl.ds(16 * k, 16), :] = v[32 * k : 32 * k + 16] + v[32 * k + 16 : 32 * k + 32]
    pick = picks(lambda i, j: (j < 64) & ((i >> 5) == (j >> 4)) & (((i & 31) >> 1) == (j & 15)), 0.125)
    return dot(row_pairs(t3, 0, 32), pick)


def from_coarsest(v, t3):
    pick = picks(lambda i, j: (i < 64) & ((j >> 5) == (i >> 4)) & (((j & 31) >> 1) == (i & 15)), 1.0)
    v = dot(v, pick)
    t3[pl.ds(0, 32, stride=2), :] = v
    t3[pl.ds(1, 32, stride=2), :] = v
    parts = []
    for k in range(4):
        block = t3[pl.ds(16 * k, 16), :]
        parts += [block, block]
    return jnp.concatenate(parts, 0)


def low_levels(first, got, w2, d2, w3, x2, t3):
    group = iota((16, 128), 1) >> 5
    parts, caps = [], []
    for zl in range(8):
        total, cap = None, None
        for zh in range(4):
            z = 8 * zh + zl
            v = jnp.where(group == 1, got[z], 0.0)
            if z + 1 < SLABS:
                v = jnp.where(group == 0, got[z + 1], v)
            if z > 0:
                v = jnp.where(group == 2, got[z - 1], v)
            v = spread(v)
            total = v if total is None else jnp.where(group == zh, v, total)
            if first:
                v = spread(jnp.where(group == 3, got[z], 0.0))
                cap = v if cap is None else jnp.where(group == zh, v, cap)
        parts.append(total)
        caps.append(cap)
    b = jnp.concatenate(parts, 0)
    if first:
        c2 = jnp.concatenate(caps, 0)
        d2[...] = c2 + 1.5
        w2[...] = OMEGA / (c2 + 1.5)
        w3[...] = OMEGA / (to_coarsest(c2, t3) + 0.75)
    w, d = w2[...], d2[...]
    y = w * b
    x = 1.2 * y + 0.25 * w * around_low(y)
    r = b - d * x + 0.25 * around_low(x)
    x = x + from_coarsest(coarsest(to_coarsest(r, t3), w3[...]), t3)
    for _ in range(2):
        x = 0.2 * x + y + 0.25 * w * around_low(x)
    x2[...] = x


def first_low_body(got, w2, d2, w3, x2, t3):
    low_levels(True, got, w2, d2, w3, x2, t3)


def next_low_body(*refs):
    low_levels(False, *refs)


def fine_up(x2, near, first, b_own, lo, hi, w, xs, w1, work, out):
    f1, y1, xa, xb, f0, x0, x9 = work
    s = lax.axis_index("space")
    lo2, lo1, block, hi1, hi2 = near
    for j, ref in enumerate(near):
        if first:
            v = OMEGA / (ref[pl.ds(32, 32), :] + 3.0)
            z = s + (j - 2)
            w1[j] = jnp.where((z >= 0) & (z < SLABS), v, 0.0)
        y1[j] = w1[j] * ref[pl.ds(0, 32), :]
    zero = jnp.zeros((32, 128), F32)
    group = iota((16, 128), 1) >> 5
    parts = []
    for j in range(5):
        z = s + (j - 2)
        v = x2[pl.ds(pl.multiple_of((z & 7) * 16, 16), 16), :]
        parts.append(spread(jnp.where(group == (z >> 3), v, 0.0)))
    pick = picks(lambda i, j: i == ((j & 63) >> 1), 1.0)
    v = dot(jnp.concatenate(parts, 0), pick)
    f1[pl.ds(0, 80, stride=2), :] = v
    f1[pl.ds(1, 80, stride=2), :] = v
    for j in range(5):
        below = y1[j - 1] if j > 0 else zero
        above = y1[j + 1] if j < 4 else zero
        xa[j] = block_sweep(y1[j], w1[j], below, above) + f1[pl.ds(32 * j, 32), :]
    xb[0] = zero
    xb[4] = zero
    for old, new in ((xa, xb), (xb, xa)):
        for j in (1, 2, 3):
            c = old[j]
            t = around_block(c, old[j - 1], old[j + 1])
            new[j] = 0.2 * c + y1[j] + 0.5 * w1[j] * t
    one, two, three = xa[1], xa[2], xa[3]
    low = dot(jnp.concatenate([two, three], 0), picks(lambda i, j: i == (j >> 1), 1.0))
    high = dot(jnp.concatenate([one, two], 0), picks(lambda i, j: i == (j >> 1) + 64, 1.0))
    for q, v in enumerate((high[:32], low[:32], high[32:], low[32:])):
        f0[pl.ds(64 * q, 32, stride=2), :] = v
        f0[pl.ds(64 * q + 1, 32, stride=2), :] = v
    rows = 64 if first else 32
    far_below = jnp.where(s > 0, lo1[pl.ds(rows, 64), :], 0.0)
    far_above = jnp.where(s < SLABS - 1, hi1[pl.ds(rows, 64), :], 0.0)
    for i in range(8):
        v = far_below if i == 0 else (far_above if i == 7 else xs[i - 1])
        x0[i] = v + f0[pl.ds(64 * (i // 2), 64), :]
    for p in range(-1, 5):
        i = p + 2
        b = lo[1] if p < 0 else (b_own[p] if p < DEPTH else hi[0])
        c = x0[i]
        x9[p + 1] = 0.2 * c + w[i] * (b + around_plane(c, x0[i - 1], x0[i + 1]))
    for p in range(DEPTH):
        c = x9[p + 1]
        u = 0.2 * c + w[p + 2] * (b_own[p] + around_plane(c, x9[p], x9[p + 2]))
        out(p, u)


def first_up_body(
    x2, lo2, lo1, block, hi1, hi2, b_own, lo, hi, w, xs, cap, src, u_out, b_out, up, dn, w1, *work
):
    def out(p, u):
        u_out[0, p] = u
        b = cap[p] * u + src[0, 1, p]
        b_out[p] = b
        ends, i = (dn, p) if p < 2 else (up, p - 2)
        ends[i] = b

    near = (lo2, lo1, block, hi1, hi2)
    fine_up(x2, near, True, b_own, lo, hi, w, xs, w1, work, out)


def next_up_body(x2, lo2, lo1, block, hi1, hi2, b_own, lo, hi, w, xs, w1, start, u_out, *work):
    keep = lax.axis_index("tm") == 0

    def out(p, u):
        u_out[0, p] = jnp.where(keep, start[0, p], u)

    near = (lo2, lo1, block, hi1, hi2)
    fine_up(x2, near, False, b_own, lo, hi, w, xs, w1, work, out)


LOW_WORK = [(64, 128)]
LOW_FLOPS = 1 << 31
WORK = [
    (160, 128),
    (5, 32, 128),
    (5, 32, 128),
    (5, 32, 128),
    (256, 128),
    (8, NY, NX),
    (6, NY, NX),
]
DOWN_WORK = [(8, NY, NX), (384, 128)]
PLANE = (NY, NX)
PLANE4 = (DEPTH, NY, NX)
MESSAGE = f32(SLABS, 16, 128)


def moved(x, spans, slabs):
    pairs = []
    for t in range(SPANS):
        for s in range(SLABS):
            pairs.append((t * SLABS + s, (t + spans) % SPANS * SLABS + (s + slabs) % SLABS))
    return lax.ppermute(x, ("tm", "space"), pairs)


def exchanged(send, up, dn, block):
    lo1, hi1 = moved(up, 0, 1), moved(dn, 0, -1)
    lo2, hi2 = moved(block, 0, 2), moved(block, 0, -2)
    got = lax.all_to_all(send, "space", 0, 0, tiled=True)
    return got, lo2, lo1, block, hi1, hi2


def shards(u0, src, cap):
    b, up, dn, cap = call(
        pack_body,
        (f32(4, *PLANE),) * 4,
        [PLANE4, PLANE4],
        *(u0, src, cap),
        space=pl.BlockSpec(memory_space=pltpu.HBM),
        sems=[pltpu.SemaphoreType.DMA((3,))],
    )
    lo, hi = moved(up, 0, 1), moved(dn, 0, -1)
    w, w1, c1, xs, send, up, dn, block = call(
        first_down_body,
        (
            f32(8, *PLANE),
            f32(3, 32, 128),
            f32(2, 32, 128),
            f32(6, *PLANE),
            MESSAGE,
            f32(128, 128),
            f32(128, 128),
            f32(64, 128),
        ),
        DOWN_WORK,
        *(b, cap, lo, hi),
    )
    got, *near = exchanged(send, up, dn, block)
    w2, d2, w3, x2 = call(
        first_low_body,
        (f32(128, 128), f32(128, 128), f32(32, 128), f32(128, 128)),
        LOW_WORK,
        got,
        flops=LOW_FLOPS,
    )
    fpoint, b, up, dn, v1 = call(
        first_up_body,
        (f32(1, *PLANE4), f32(*PLANE4), f32(2, *PLANE), f32(2, *PLANE), f32(5, 32, 128)),
        WORK,
        *(x2, *near, b, lo, hi, w, xs, cap, src),
    )
    b, lo, hi = moved(b, 1, 0), moved(up, 1, 1), moved(dn, 1, -1)
    xs, send, up, dn, block = call(
        next_down_body,
        (f32(6, *PLANE), MESSAGE, f32(96, 128), f32(96, 128), f32(32, 128)),
        DOWN_WORK,
        *(b, cap, lo, hi, w, w1, c1),
    )
    got, *near = exchanged(send, up, dn, block)
    (x2,) = call(next_low_body, (f32(128, 128),), LOW_WORK, *(got, w2, d2, w3), flops=LOW_FLOPS)
    (updated,) = call(
        next_up_body, (f32(1, *PLANE4),), WORK, *(x2, *near, b, lo, hi, w, xs, v1, u0)
    )
    return fpoint, updated


def solution(mesh):
    in_specs = (
        P("tm", "space", None, None),
        P("tm", None, "space", None, None),
        P("space", None, None),
    )
    out_specs = (P("tm", "space", None, None), P("tm", "space", None, None))
    return jax.shard_map(shards, mesh=mesh, in_specs=in_specs, out_specs=out_specs, check_vma=False)
```

```python
import jax
import jax.numpy as jnp
from jax import lax
from jax.experimental import pallas as pl
from jax.experimental.pallas import tpu as pltpu
from jax.sharding import PartitionSpec as P


COARSE_SWEEPS = 24
NY, NX = 64, 128
SLABS = 32
SPANS = 8
DEPTH = 4
OMEGA = 0.8
F32 = jnp.float32
VMEM = pl.BlockSpec(memory_space=pltpu.VMEM)


def f32(*shape):
    return jax.ShapeDtypeStruct(shape, F32)


def call(body, outs, scratch, *args, space=VMEM, flops=None, sems=()):
    return pl.pallas_call(
        body,
        out_shape=outs,
        in_specs=[space] * len(args),
        out_specs=tuple(VMEM for _ in outs),
        scratch_shapes=[pltpu.VMEM(s, F32) for s in scratch] + list(sems),
        compiler_params=pltpu.CompilerParams(vmem_limit_bytes=16 << 20),
        cost_estimate=flops and pl.CostEstimate(flops=flops, transcendentals=0, bytes_accessed=0),
    )(*args)


def dot(a, b):
    return jnp.dot(a, b, precision=lax.Precision.HIGHEST, preferred_element_type=F32)


def iota(shape, axis):
    return lax.broadcasted_iota(jnp.int32, shape, axis)


def picks(test, scale):
    i, j = iota((128, 128), 0), iota((128, 128), 1)
    return jnp.where(test(i, j), jnp.float32(scale), jnp.float32(0.0))


def around_plane(c, below, above):
    row, lane = iota(c.shape, 0), iota(c.shape, 1)
    total = below + above
    total = total + jnp.where(lane > 0, pltpu.roll(c, 1, 1), 0.0)
    total = total + jnp.where(lane < NX - 1, pltpu.roll(c, NX - 1, 1), 0.0)
    total = total + jnp.where(row > 0, pltpu.roll(c, 1, 0), 0.0)
    return total + jnp.where(row < NY - 1, pltpu.roll(c, NY - 1, 0), 0.0)


def around_block(c, below, above):
    row, lane = iota(c.shape, 0), iota(c.shape, 1)
    col = lane & 63
    total = pltpu.roll(c + jnp.where(lane < 64, above, below), 64, 1)
    total = total + jnp.where(col > 0, pltpu.roll(c, 1, 1), 0.0)
    total = total + jnp.where(col < 63, pltpu.roll(c, 127, 1), 0.0)
    total = total + jnp.where(row > 0, pltpu.roll(c, 1, 0), 0.0)
    return total + jnp.where(row < 31, pltpu.roll(c, 31, 0), 0.0)


def around_low(v):
    row, lane = iota(v.shape, 0), iota(v.shape, 1)
    y, x = row & 15, lane & 31
    ends = iota((16, 128), 1)
    below = jnp.where(ends >= 32, pltpu.roll(v[112:], 32, 1), 0.0)
    above = jnp.where(ends < 96, pltpu.roll(v[:16], 96, 1), 0.0)
    total = jnp.concatenate([below, v[:112]], 0) + jnp.concatenate([v[16:], above], 0)
    total = total + jnp.where(x > 0, pltpu.roll(v, 1, 1), 0.0)
    total = total + jnp.where(x < 31, pltpu.roll(v, 127, 1), 0.0)
    total = total + jnp.where(y > 0, pltpu.roll(v, 1, 0), 0.0)
    return total + jnp.where(y < 15, pltpu.roll(v, 127, 0), 0.0)


def coarsest(b3, w3):
    lane, row = iota((8, 128), 1), iota((8, 128), 0)
    x = lane & 15
    steps = []
    for k in range(4):
        w = w3[8 * k : 8 * k + 8]
        wh = 0.125 * w
        steps.append(
            (
                w * b3[8 * k : 8 * k + 8],
                wh,
                jnp.where(x > 0, wh, 0.0),
                jnp.where(x < 15, wh, 0.0),
                jnp.where(row > 0, wh, 0.0),
                jnp.where(row < 7, wh, 0.0),
            )
        )
    inside = lane < 64

    def sweep(_, v):
        below = jnp.where(inside, pltpu.roll(v[3], 16, 1), 0.0)
        above = jnp.where(inside, pltpu.roll(v[0], 112, 1), 0.0)
        line = (below, *v, above)
        new = []
        for k in range(4):
            wb, wh, left, right, up, down = steps[k]
            c = v[k]
            t = (0.2 * c + wb) + wh * (line[k] + line[k + 2])
            s = up * pltpu.roll(c, 1, 0) + down * pltpu.roll(c, 7, 0)
            e = left * pltpu.roll(c, 1, 1) + right * pltpu.roll(c, 127, 1)
            new.append((t + s) + e)
        return tuple(new)

    v = lax.fori_loop(0, COARSE_SWEEPS - 1, sweep, tuple(s[0] for s in steps), unroll=True)
    return jnp.concatenate(v, 0)


def pack_body(u, src, cap, b_out, up, dn, cap_out, u_in, src_in, sems):
    copies = [
        pltpu.make_async_copy(cap, cap_out, sems.at[0]),
        pltpu.make_async_copy(u.at[0], u_in, sems.at[1]),
        pltpu.make_async_copy(src.at[0, 0], src_in, sems.at[2]),
    ]
    for copy in copies:
        copy.start()
    for copy in copies:
        copy.wait()
    for p in range(DEPTH):
        c = cap_out[p]
        b = c * u_in[p] + src_in[p]
        b_out[p] = b
        ends, i = (dn, p) if p < 2 else (up, p - 2)
        ends[i] = b
        ends[i + 2] = c


def row_pairs(ref, start, count):
    return ref[pl.ds(start, count, stride=2), :] + ref[pl.ds(start + 1, count, stride=2), :]


def block_sweep(y, w, below, above):
    return 1.2 * y + 0.5 * w * around_block(y, below, above)


def fine_down(first, b_own, cap, lo, hi, w, w1, c1, xs, up, dn, block, ys, rs):
    lane = iota((32, 128), 1)
    lo_pick = picks(lambda i, j: (i >> 1) == j, 0.125)
    hi_pick = picks(lambda i, j: (i >> 1) + 64 == j, 0.125)

    def b(p):
        return lo[p + 2] if p < 0 else (b_own[p] if p < DEPTH else hi[p - DEPTH])

    def c(p):
        return lo[p + 4] if p < 0 else (cap[p] if p < DEPTH else hi[p - 2])

    if first:
        s = lax.axis_index("space")
        for p in range(-2, 6):
            v = OMEGA / (c(p) + 6.0)
            if p < 0:
                v = jnp.where(s > 0, v, 0.0)
            if p >= DEPTH:
                v = jnp.where(s < SLABS - 1, v, 0.0)
            w[p + 2] = v
    for p in range(-2, 6):
        ys[p + 2] = w[p + 2] * b(p)
    for p in range(-1, 5):
        i = p + 2
        xs[p + 1] = 1.2 * ys[i] + w[i] * around_plane(ys[i], ys[i - 1], ys[i + 1])
    for half in range(2):
        total = None
        for p in (2 * half, 2 * half + 1):
            i = p + 1
            r = b(p) - (cap[p] + 6.0) * xs[i] + around_plane(xs[i], xs[i - 1], xs[i + 1])
            total = r if total is None else total + r
        rs[pl.ds(64 * half, 64), :] = total
    if first:
        for k, p in enumerate((0, 2, 4, -2)):
            rs[pl.ds(128 + 64 * k, 64), :] = c(p) + c(p + 1)
    low, high = [row_pairs(rs, 0, 32)], [row_pairs(rs, 64, 32)]
    if first:
        low += [row_pairs(rs, 128, 32), row_pairs(rs, 256, 32)]
        high += [row_pairs(rs, 192, 32), row_pairs(rs, 320, 32)]
    blocks = dot(jnp.concatenate(low, 0), lo_pick) + dot(jnp.concatenate(high, 0), hi_pick)
    if first:
        c1[0], c1[1] = blocks[32:64], blocks[64:]
        wide = OMEGA / (blocks[64:] + 3.0)
        w1[0] = jnp.where((lane >= 64) & (s > 0), wide, 0.0)
        w1[1] = OMEGA / (blocks[32:64] + 3.0)
        w1[2] = jnp.where((lane < 64) & (s < SLABS - 1), wide, 0.0)
    rows = 64 if first else 32
    block[...] = blocks[:rows]
    up[pl.ds(0, rows), :] = blocks[:rows]
    dn[pl.ds(0, rows), :] = blocks[:rows]
    up[pl.ds(rows, 64), :] = xs[3]
    dn[pl.ds(rows, 64), :] = xs[2]


def share_body(block, w1, c1, send, rs):
    zero = jnp.zeros((32, 128), F32)
    b1 = block[pl.ds(0, 32), :]
    y = w1[1] * b1
    x = [
        block_sweep(zero, w1[0], zero, y),
        block_sweep(y, w1[1], zero, zero),
        block_sweep(zero, w1[2], y, zero),
    ]
    own, beside = c1[0] + 3.0, c1[1] + 3.0
    r = [
        0.5 * around_block(x[0], zero, x[1]) - beside * x[0],
        b1 - own * x[1] + 0.5 * around_block(x[1], x[0], x[2]),
        0.5 * around_block(x[2], x[1], zero) - beside * x[2],
        c1[0],
    ]
    for k in range(4):
        rs[pl.ds(32 * k, 32), :] = r[k]
    low = dot(row_pairs(rs, 0, 64), picks(lambda i, j: ((i & 63) >> 1) == (j & 31), 0.125))
    group = iota((16, 128), 1) >> 5
    message = low[48:]
    for k in range(3):
        message = jnp.where(group == k, low[16 * k : 16 * k + 16], message)
    for peer in range(SLABS):
        send[peer] = message


def first_down_body(b_own, cap, lo, hi, *rest):
    fine_down(True, b_own, cap, lo, hi, *rest)


def next_down_body(*refs):
    fine_down(False, *refs)


def spread(v):
    v = v + pltpu.roll(v, 64, 1)
    return v + pltpu.roll(v, 32, 1)


def to_coarsest(v, t3):
    for k in range(4):
        t3[pl.ds(16 * k, 16), :] = v[32 * k : 32 * k + 16] + v[32 * k + 16 : 32 * k + 32]
    pick = picks(lambda i, j: (j < 64) & ((i >> 5) == (j >> 4)) & (((i & 31) >> 1) == (j & 15)), 0.125)
    return dot(row_pairs(t3, 0, 32), pick)


def from_coarsest(v, t3):
    pick = picks(lambda i, j: (i < 64) & ((j >> 5) == (i >> 4)) & (((j & 31) >> 1) == (i & 15)), 1.0)
    v = dot(v, pick)
    t3[pl.ds(0, 32, stride=2), :] = v
    t3[pl.ds(1, 32, stride=2), :] = v
    parts = []
    for k in range(4):
        block = t3[pl.ds(16 * k, 16), :]
        parts += [block, block]
    return jnp.concatenate(parts, 0)


def low_levels(first, got, w2, d2, w3, x2, t3):
    group = iota((16, 128), 1) >> 5
    parts, caps = [], []
    for zl in range(8):
        total, cap = None, None
        for zh in range(4):
            z = 8 * zh + zl
            v = jnp.where(group == 1, got[z], 0.0)
            if z + 1 < SLABS:
                v = jnp.where(group == 0, got[z + 1], v)
            if z > 0:
                v = jnp.where(group == 2, got[z - 1], v)
            v = spread(v)
            total = v if total is None else jnp.where(group == zh, v, total)
            if first:
                v = spread(jnp.where(group == 3, got[z], 0.0))
                cap = v if cap is None else jnp.where(group == zh, v, cap)
        parts.append(total)
        caps.append(cap)
    b = jnp.concatenate(parts, 0)
    if first:
        c2 = jnp.concatenate(caps, 0)
        d2[...] = c2 + 1.5
        w2[...] = OMEGA / (c2 + 1.5)
        w3[...] = OMEGA / (to_coarsest(c2, t3) + 0.75)
    w, d = w2[...], d2[...]
    y = w * b
    x = 1.2 * y + 0.25 * w * around_low(y)
    r = b - d * x + 0.25 * around_low(x)
    x = x + from_coarsest(coarsest(to_coarsest(r, t3), w3[...]), t3)
    for _ in range(2):
        x = 0.2 * x + y + 0.25 * w * around_low(x)
    x2[...] = x


def first_low_body(got, w2, d2, w3, x2, t3):
    low_levels(True, got, w2, d2, w3, x2, t3)


def next_low_body(*refs):
    low_levels(False, *refs)


def fine_up(x2, near, first, b_own, lo, hi, w, xs, w1, work, out):
    f1, y1, xa, xb, f0, x0, x9 = work
    s = lax.axis_index("space")
    _, lo1, _, hi1, _ = near
    for j, ref in enumerate(near):
        if first:
            v = OMEGA / (ref[pl.ds(32, 32), :] + 3.0)
            z = s + (j - 2)
            w1[j] = jnp.where((z >= 0) & (z < SLABS), v, 0.0)
        y1[j] = w1[j] * ref[pl.ds(0, 32), :]
    zero = jnp.zeros((32, 128), F32)
    group = iota((16, 128), 1) >> 5
    parts = []
    for j in range(5):
        z = s + (j - 2)
        v = x2[pl.ds(pl.multiple_of((z & 7) * 16, 16), 16), :]
        parts.append(spread(jnp.where(group == (z >> 3), v, 0.0)))
    pick = picks(lambda i, j: i == ((j & 63) >> 1), 1.0)
    v = dot(jnp.concatenate(parts, 0), pick)
    f1[pl.ds(0, 80, stride=2), :] = v
    f1[pl.ds(1, 80, stride=2), :] = v
    for j in range(5):
        below = y1[j - 1] if j > 0 else zero
        above = y1[j + 1] if j < 4 else zero
        xa[j] = block_sweep(y1[j], w1[j], below, above) + f1[pl.ds(32 * j, 32), :]
    xb[0] = zero
    xb[4] = zero
    for old, new in ((xa, xb), (xb, xa)):
        for j in (1, 2, 3):
            c = old[j]
            t = around_block(c, old[j - 1], old[j + 1])
            new[j] = 0.2 * c + y1[j] + 0.5 * w1[j] * t
    one, two, three = xa[1], xa[2], xa[3]
    low = dot(jnp.concatenate([two, three], 0), picks(lambda i, j: i == (j >> 1), 1.0))
    high = dot(jnp.concatenate([one, two], 0), picks(lambda i, j: i == (j >> 1) + 64, 1.0))
    for q, v in enumerate((high[:32], low[:32], high[32:], low[32:])):
        f0[pl.ds(64 * q, 32, stride=2), :] = v
        f0[pl.ds(64 * q + 1, 32, stride=2), :] = v
    rows = 64 if first else 32
    far_below = jnp.where(s > 0, lo1[pl.ds(rows, 64), :], 0.0)
    far_above = jnp.where(s < SLABS - 1, hi1[pl.ds(rows, 64), :], 0.0)
    for i in range(8):
        v = far_below if i == 0 else (far_above if i == 7 else xs[i - 1])
        x0[i] = v + f0[pl.ds(64 * (i // 2), 64), :]
    for p in range(-1, 5):
        i = p + 2
        b = lo[1] if p < 0 else (b_own[p] if p < DEPTH else hi[0])
        c = x0[i]
        x9[p + 1] = 0.2 * c + w[i] * (b + around_plane(c, x0[i - 1], x0[i + 1]))
    for p in range(DEPTH):
        c = x9[p + 1]
        u = 0.2 * c + w[p + 2] * (b_own[p] + around_plane(c, x9[p], x9[p + 2]))
        out(p, u)


def first_up_body(
    x2, lo2, lo1, block, hi1, hi2, b_own, lo, hi, w, xs, cap, src, u_out, b_out, up, dn, w1, *work
):
    def out(p, u):
        u_out[0, p] = u
        b = cap[p] * u + src[0, 1, p]
        b_out[p] = b
        ends, i = (dn, p) if p < 2 else (up, p - 2)
        ends[i] = b

    near = (lo2, lo1, block, hi1, hi2)
    fine_up(x2, near, True, b_own, lo, hi, w, xs, w1, work, out)


def next_up_body(x2, lo2, lo1, block, hi1, hi2, b_own, lo, hi, w, xs, w1, start, u_out, *work):
    keep = lax.axis_index("tm") == 0

    def out(p, u):
        u_out[0, p] = jnp.where(keep, start[0, p], u)

    near = (lo2, lo1, block, hi1, hi2)
    fine_up(x2, near, False, b_own, lo, hi, w, xs, w1, work, out)


LOW_WORK = [(64, 128)]
LOW_FLOPS = 1 << 31
WORK = [
    (160, 128),
    (5, 32, 128),
    (5, 32, 128),
    (5, 32, 128),
    (256, 128),
    (8, NY, NX),
    (6, NY, NX),
]
DOWN_WORK = [(8, NY, NX), (384, 128)]
PLANE = (NY, NX)
PLANE4 = (DEPTH, NY, NX)
MESSAGE = f32(SLABS, 16, 128)


def moved(x, spans, slabs):
    pairs = []
    for t in range(SPANS):
        for s in range(SLABS):
            pairs.append((t * SLABS + s, (t + spans) % SPANS * SLABS + (s + slabs) % SLABS))
    return lax.ppermute(x, ("tm", "space"), pairs)


def exchanged(up, dn, block, w1, c1):
    lo1 = moved(up, 0, 1)
    hi1 = moved(dn, 0, -1)
    lo2 = moved(block, 0, 2)
    hi2 = moved(block, 0, -2)
    (send,) = call(share_body, (MESSAGE,), [(128, 128)], block, w1, c1)
    got = lax.all_to_all(send, "space", 0, 0, tiled=True)
    return got, lo2, lo1, block, hi1, hi2


def shards(u0, src, cap):
    b, up, dn, cap = call(
        pack_body,
        (f32(4, *PLANE),) * 4,
        [PLANE4, PLANE4],
        *(pltpu.with_memory_space_constraint(x, pltpu.HBM) for x in (u0, src, cap)),
        space=pl.BlockSpec(memory_space=pltpu.HBM),
        sems=[pltpu.SemaphoreType.DMA((3,))],
    )
    lo, hi = moved(up, 0, 1), moved(dn, 0, -1)
    w, w1, c1, xs, up, dn, block = call(
        first_down_body,
        (
            f32(8, *PLANE),
            f32(3, 32, 128),
            f32(2, 32, 128),
            f32(6, *PLANE),
            f32(128, 128),
            f32(128, 128),
            f32(64, 128),
        ),
        DOWN_WORK,
        *(b, cap, lo, hi),
    )
    got, *near = exchanged(up, dn, block, w1, c1)
    w2, d2, w3, x2 = call(
        first_low_body,
        (f32(128, 128), f32(128, 128), f32(32, 128), f32(128, 128)),
        LOW_WORK,
        got,
        flops=LOW_FLOPS,
    )
    fpoint, b, up, dn, v1 = call(
        first_up_body,
        (f32(1, *PLANE4), f32(*PLANE4), f32(2, *PLANE), f32(2, *PLANE), f32(5, 32, 128)),
        WORK,
        *(x2, *near, b, lo, hi, w, xs, cap, src),
    )
    b, lo, hi = moved(b, 1, 0), moved(up, 1, 1), moved(dn, 1, -1)
    xs, up, dn, block = call(
        next_down_body,
        (f32(6, *PLANE), f32(96, 128), f32(96, 128), f32(32, 128)),
        DOWN_WORK,
        *(b, cap, lo, hi, w, w1, c1),
    )
    got, *near = exchanged(up, dn, block, w1, c1)
    (x2,) = call(next_low_body, (f32(128, 128),), LOW_WORK, *(got, w2, d2, w3), flops=LOW_FLOPS)
    (updated,) = call(
        next_up_body, (f32(1, *PLANE4),), WORK, *(x2, *near, b, lo, hi, w, xs, v1, u0)
    )
    return fpoint, updated


def solution(mesh):
    in_specs = (
        P("tm", "space", None, None),
        P("tm", None, "space", None, None),
        P("space", None, None),
    )
    out_specs = (P("tm", "space", None, None), P("tm", "space", None, None))
    return jax.shard_map(shards, mesh=mesh, in_specs=in_specs, out_specs=out_specs, check_vma=False)
```

```python
import jax
import jax.numpy as jnp
from jax import lax
from jax.experimental import pallas as pl
from jax.experimental.pallas import tpu as pltpu
from jax.sharding import PartitionSpec as P

COARSE_SWEEPS = 24
NY, NX = 64, 128
SLABS = 32
SPANS = 8
DEPTH = 4
OMEGA = 0.8
F32 = jnp.float32
VMEM = pl.BlockSpec(memory_space=pltpu.VMEM)


def f32(*shape):
    return jax.ShapeDtypeStruct(shape, F32)


def call(body, outs, scratch, *args, space=VMEM, flops=None, sems=()):
    return pl.pallas_call(
        body,
        out_shape=outs,
        in_specs=[space] * len(args),
        out_specs=tuple(VMEM for _ in outs),
        scratch_shapes=[pltpu.VMEM(s, F32) for s in scratch] + list(sems),
        compiler_params=pltpu.CompilerParams(vmem_limit_bytes=16 << 20),
        cost_estimate=flops and pl.CostEstimate(flops=flops, transcendentals=0, bytes_accessed=0),
    )(*args)


def dot(a, pick):
    high = a.astype(jnp.bfloat16)
    rest = a - high.astype(F32)
    middle = rest.astype(jnp.bfloat16)
    low = (rest - middle.astype(F32)).astype(jnp.bfloat16)
    rows = a.shape[0]
    out = jnp.dot(jnp.concatenate([high, middle, low], 0), pick, preferred_element_type=F32)
    return (out[2 * rows :] + out[rows : 2 * rows]) + out[:rows]


def iota(shape, axis):
    return lax.broadcasted_iota(jnp.int32, shape, axis)


def picks(test, scale):
    i, j = iota((128, 128), 0), iota((128, 128), 1)
    return jnp.where(test(i, j), jnp.float32(scale), jnp.float32(0.0)).astype(jnp.bfloat16)


def inside_plane(c):
    row, lane = iota(c.shape, 0), iota(c.shape, 1)
    total = jnp.where(lane > 0, pltpu.roll(c, 1, 1), 0.0)
    total = total + jnp.where(lane < NX - 1, pltpu.roll(c, NX - 1, 1), 0.0)
    total = total + jnp.where(row > 0, pltpu.roll(c, 1, 0), 0.0)
    return total + jnp.where(row < NY - 1, pltpu.roll(c, NY - 1, 0), 0.0)


def around_plane(c, below, above):
    return inside_plane(c) + (below + above)


def around_block(c, below, above):
    row, lane = iota(c.shape, 0), iota(c.shape, 1)
    col = lane & 63
    total = pltpu.roll(c + jnp.where(lane < 64, above, below), 64, 1)
    total = total + jnp.where(col > 0, pltpu.roll(c, 1, 1), 0.0)
    total = total + jnp.where(col < 63, pltpu.roll(c, 127, 1), 0.0)
    total = total + jnp.where(row > 0, pltpu.roll(c, 1, 0), 0.0)
    return total + jnp.where(row < 31, pltpu.roll(c, 31, 0), 0.0)


def around_low(v):
    row, lane = iota(v.shape, 0), iota(v.shape, 1)
    y, x = row & 15, lane & 31
    ends = iota((16, 128), 1)
    below = jnp.where(ends >= 32, pltpu.roll(v[112:], 32, 1), 0.0)
    above = jnp.where(ends < 96, pltpu.roll(v[:16], 96, 1), 0.0)
    total = jnp.concatenate([below, v[:112]], 0) + jnp.concatenate([v[16:], above], 0)
    total = total + jnp.where(x > 0, pltpu.roll(v, 1, 1), 0.0)
    total = total + jnp.where(x < 31, pltpu.roll(v, 127, 1), 0.0)
    total = total + jnp.where(y > 0, pltpu.roll(v, 1, 0), 0.0)
    return total + jnp.where(y < 15, pltpu.roll(v, 127, 0), 0.0)


def coarsest(b3, w3):
    lane, row = iota((8, 128), 1), iota((8, 128), 0)
    x = lane & 15
    steps = []
    for k in range(4):
        w = w3[8 * k : 8 * k + 8]
        wh = 0.125 * w
        steps.append(
            (
                w * b3[8 * k : 8 * k + 8],
                wh,
                jnp.where(x > 0, wh, 0.0),
                jnp.where(x < 15, wh, 0.0),
                jnp.where(row > 0, wh, 0.0),
                jnp.where(row < 7, wh, 0.0),
            )
        )
    inside = lane < 64

    def sweep(_, v):
        below = jnp.where(inside, pltpu.roll(v[3], 16, 1), 0.0)
        above = jnp.where(inside, pltpu.roll(v[0], 112, 1), 0.0)
        line = (below, *v, above)
        new = []
        for k in range(4):
            wb, wh, left, right, up, down = steps[k]
            c = v[k]
            t = (0.2 * c + wb) + wh * (line[k] + line[k + 2])
            s = up * pltpu.roll(c, 1, 0) + down * pltpu.roll(c, 7, 0)
            e = left * pltpu.roll(c, 1, 1) + right * pltpu.roll(c, 127, 1)
            new.append((t + s) + e)
        return tuple(new)

    v = lax.fori_loop(0, COARSE_SWEEPS - 1, sweep, tuple(s[0] for s in steps), unroll=True)
    return jnp.concatenate(v, 0)


def row_pairs(ref, start, count):
    return ref[pl.ds(start, count, stride=2), :] + ref[pl.ds(start + 1, count, stride=2), :]


def block_sweep(y, w, below, above):
    return 1.2 * y + 0.5 * w * around_block(y, below, above)


def plane_picks():
    return (
        picks(lambda i, j: (i >> 1) == j, 0.125),
        picks(lambda i, j: (i >> 1) + 64 == j, 0.125),
    )


def local_down(b, cap, w, y, x, rs, lo_pick, hi_pick, first):
    for p in range(DEPTH):
        y[p] = w[p] * b(p)
    zero = jnp.zeros((NY, NX), F32)
    for p in range(DEPTH):
        below = y[p - 1] if p > 0 else zero
        above = y[p + 1] if p < 3 else zero
        x[p] = 1.2 * y[p] + w[p] * around_plane(y[p], below, above)
    for half in range(2):
        total = None
        for p in (2 * half, 2 * half + 1):
            below = x[p - 1] if p > 0 else zero
            above = x[p + 1] if p < 3 else zero
            r = b(p) - (cap[p] + 6.0) * x[p] + around_plane(x[p], below, above)
            total = r if total is None else total + r
        rs[pl.ds(64 * half, 64), :] = total
        if first:
            rs[pl.ds(128 + 64 * half, 64), :] = cap[2 * half] + cap[2 * half + 1]
    low, high = row_pairs(rs, 0, 32), row_pairs(rs, 64, 32)
    if first:
        low = jnp.concatenate([low, row_pairs(rs, 128, 32)], 0)
        high = jnp.concatenate([high, row_pairs(rs, 192, 32)], 0)
    return dot(low, lo_pick) + dot(high, hi_pick)


def fill_edges(up, dn, y, x):
    for edge, p, q in ((up, 3, 2), (dn, 0, 1)):
        edge[pl.ds(0, 64), :] = y[p]
        edge[pl.ds(64, 64), :] = x[p]
        edge[pl.ds(128, 64), :] = x[q]


def pack_body(u, src, cap, w, y, x, block, up, dn, cap_out, u_in, src_in, rs, sems):
    copies = [
        pltpu.make_async_copy(cap, cap_out, sems.at[0]),
        pltpu.make_async_copy(u.at[0], u_in, sems.at[1]),
        pltpu.make_async_copy(src.at[0, 0], src_in, sems.at[2]),
    ]
    for copy in copies:
        copy.start()
    lo_pick, hi_pick = plane_picks()
    for copy in copies:
        copy.wait()
    for p in range(DEPTH):
        w[p] = OMEGA / (cap_out[p] + 6.0)
        u_in[p] = cap_out[p] * u_in[p] + src_in[p]
    blocks = local_down(lambda p: u_in[p], cap_out, w, y, x, rs, lo_pick, hi_pick, True)
    block[...] = blocks
    fill_edges(up, dn, y, x)
    lane = iota((32, 128), 1)
    b1, c1 = blocks[:32], blocks[32:]
    up[pl.ds(192, 32), :] = jnp.where(lane < 64, pltpu.roll(b1, 64, 1), c1)
    dn[pl.ds(192, 32), :] = jnp.where(lane < 64, b1, pltpu.roll(c1, 64, 1))
    up[pl.ds(224, 64), :] = w[3]
    dn[pl.ds(224, 64), :] = w[0]


def finish_down(first, w, y, x, b1, c1, lo, hi, wx, yx, xs, pair, send, rs, lo_pick, hi_pick):
    s = lax.axis_index("space")
    lane = iota((32, 128), 1)

    def edge(ref, there):
        return [
            jnp.where(there, ref[pl.ds(start, 64), :], 0.0)
            for start in ((0, 64, 128, 224) if first else (0, 64, 128))
        ]

    sides = []
    for ref, there, i, p in ((lo, s > 0, 0, 0), (hi, s < SLABS - 1, 5, 3)):
        ye, xe, xs_far, *we = edge(ref, there)
        if first:
            wx[i] = we[0]
        yx[i] = ye
        near = w[p] * ye
        far = wx[i] * y[p]
        x_near, x_far = x[p] + near, xe + far
        j = 1 if p == 0 else 6
        xs[j] = x_far
        xs[0 if p == 0 else 7] = xs_far
        xs[p + 2] = x_near
        own = (near - OMEGA * ye) + inside_plane(near) + x_far
        beside = (far - OMEGA * y[p]) + inside_plane(far) + x_near
        sides.append((own, jnp.where(there, beside, 0.0)))
    for p in range(DEPTH):
        yx[p + 1] = y[p]
        if first:
            wx[p + 1] = w[p]
    xs[3] = x[1]
    xs[4] = x[2]
    for k, v in enumerate((sides[0][0], sides[1][1], sides[1][0], sides[0][1])):
        rs[pl.ds(64 * k, 64), :] = v
    low = jnp.concatenate([row_pairs(rs, 0, 32), row_pairs(rs, 64, 32)], 0)
    high = jnp.concatenate([row_pairs(rs, 128, 32), row_pairs(rs, 192, 32)], 0)
    terms = dot(low, lo_pick) + dot(high, hi_pick)
    lo_block, hi_block = lo[pl.ds(192, 32), :], hi[pl.ds(192, 32), :]
    if first:
        pair[pl.ds(64, 32), :] = c1
        pair[pl.ds(96, 32), :] = jnp.where(lane < 64, pltpu.roll(hi_block, 64, 1), lo_block)
        lo_block = pltpu.roll(lo_block, 64, 1)
    own = b1 + terms[:32]
    pair[pl.ds(0, 32), :] = own
    pair[pl.ds(32, 32), :] = jnp.where(lane < 64, hi_block, lo_block) + terms[32:]
    return own


def share(b1, c1, c_mix, send, rs):
    s = lax.axis_index("space")
    lane = iota((32, 128), 1)
    zero = jnp.zeros((32, 128), F32)
    own, beside = c1 + 3.0, c_mix + 3.0
    w_own, w_mix = OMEGA / own, OMEGA / beside
    y = w_own * b1
    x = [
        block_sweep(zero, jnp.where((lane >= 64) & (s > 0), w_mix, 0.0), zero, y),
        block_sweep(y, w_own, zero, zero),
        block_sweep(zero, jnp.where((lane < 64) & (s < SLABS - 1), w_mix, 0.0), y, zero),
    ]
    r = [
        0.5 * around_block(x[0], zero, x[1]) - beside * x[0],
        b1 - own * x[1] + 0.5 * around_block(x[1], x[0], x[2]),
        0.5 * around_block(x[2], x[1], zero) - beside * x[2],
        c1,
    ]
    for k in range(4):
        rs[pl.ds(32 * k, 32), :] = r[k]
    low = dot(row_pairs(rs, 0, 64), picks(lambda i, j: ((i & 63) >> 1) == (j & 31), 0.125))
    group = iota((16, 128), 1) >> 5
    message = low[48:]
    for k in range(3):
        message = jnp.where(group == k, low[16 * k : 16 * k + 16], message)
    for peer in range(SLABS):
        send[peer] = message


def first_down_body(w, y, x, block, lo, hi, wx, yx, xs, pair, send, rs):
    b1, c1 = block[pl.ds(0, 32), :], block[pl.ds(32, 32), :]
    own = finish_down(True, w, y, x, b1, c1, lo, hi, wx, yx, xs, pair, send, rs, *plane_picks())
    share(own, c1, pair[pl.ds(96, 32), :], send, rs)


def next_down_body(b, lo, hi, cap, w, wx, old, yx, xs, pair, send, y, x, rs):
    lo_pick, hi_pick = plane_picks()
    b1 = local_down(lambda p: b[p], cap, w, y, x, rs, lo_pick, hi_pick, False)
    own = finish_down(
        False, w, y, x, b1, None, lo, hi, wx, yx, xs, pair, send, rs, lo_pick, hi_pick
    )
    share(own, old[pl.ds(64, 32), :], old[pl.ds(96, 32), :], send, rs)


def spread(v):
    v = v + pltpu.roll(v, 64, 1)
    return v + pltpu.roll(v, 32, 1)


def to_coarsest(v, t3):
    for k in range(4):
        t3[pl.ds(16 * k, 16), :] = v[32 * k : 32 * k + 16] + v[32 * k + 16 : 32 * k + 32]
    pick = picks(lambda i, j: (j < 64) & ((i >> 5) == (j >> 4)) & (((i & 31) >> 1) == (j & 15)), 0.125)
    return dot(row_pairs(t3, 0, 32), pick)


def from_coarsest(v, t3):
    pick = picks(lambda i, j: (i < 64) & ((j >> 5) == (i >> 4)) & (((j & 31) >> 1) == (i & 15)), 1.0)
    v = dot(v, pick)
    t3[pl.ds(0, 32, stride=2), :] = v
    t3[pl.ds(1, 32, stride=2), :] = v
    parts = []
    for k in range(4):
        block = t3[pl.ds(16 * k, 16), :]
        parts += [block, block]
    return jnp.concatenate(parts, 0)


def low_levels(first, got, w2, d2, w3, x2, t3):
    group = iota((16, 128), 1) >> 5
    parts, caps = [], []
    for zl in range(8):
        total, cap = None, None
        for zh in range(4):
            z = 8 * zh + zl
            v = jnp.where(group == 1, got[z], 0.0)
            if z + 1 < SLABS:
                v = jnp.where(group == 0, got[z + 1], v)
            if z > 0:
                v = jnp.where(group == 2, got[z - 1], v)
            v = spread(v)
            total = v if total is None else jnp.where(group == zh, v, total)
            if first:
                v = spread(jnp.where(group == 3, got[z], 0.0))
                cap = v if cap is None else jnp.where(group == zh, v, cap)
        parts.append(total)
        caps.append(cap)
    b = jnp.concatenate(parts, 0)
    if first:
        c2 = jnp.concatenate(caps, 0)
        d2[...] = c2 + 1.5
        w2[...] = OMEGA / (c2 + 1.5)
        w3[...] = OMEGA / (to_coarsest(c2, t3) + 0.75)
    w, d = w2[...], d2[...]
    y = w * b
    x = 1.2 * y + 0.25 * w * around_low(y)
    r = b - d * x + 0.25 * around_low(x)
    x = x + from_coarsest(coarsest(to_coarsest(r, t3), w3[...]), t3)
    for _ in range(2):
        x = 0.2 * x + y + 0.25 * w * around_low(x)
    x2[...] = x


def first_low_body(got, w2, d2, w3, x2, t3):
    low_levels(True, got, w2, d2, w3, x2, t3)


def next_low_body(*refs):
    low_levels(False, *refs)


def fine_up(x2, lo2, pair, hi2, first, wx, yx, xs, w1, work, out):
    f1, y1, xa, xb, f0, x0, x9 = work
    s = lax.axis_index("space")
    lane = iota((32, 128), 1)

    def blocks(start):
        mixed = [ref[pl.ds(start + 32, 32), :] for ref in (lo2, pair, hi2)]
        return (
            lo2[pl.ds(start, 32), :],
            jnp.where(lane < 64, mixed[0], mixed[1]),
            pair[pl.ds(start, 32), :],
            jnp.where(lane < 64, mixed[1], mixed[2]),
            hi2[pl.ds(start, 32), :],
        )

    if first:
        for j, c in enumerate(blocks(64)):
            z = s + (j - 2)
            w1[j] = jnp.where((z >= 0) & (z < SLABS), OMEGA / (c + 3.0), 0.0)
    for j, b in enumerate(blocks(0)):
        y1[j] = w1[j] * b
    zero = jnp.zeros((32, 128), F32)
    group = iota((16, 128), 1) >> 5
    parts = []
    for j in range(5):
        z = s + (j - 2)
        v = x2[pl.ds(pl.multiple_of((z & 7) * 16, 16), 16), :]
        parts.append(spread(jnp.where(group == (z >> 3), v, 0.0)))
    pick = picks(lambda i, j: i == ((j & 63) >> 1), 1.0)
    v = dot(jnp.concatenate(parts, 0), pick)
    f1[pl.ds(0, 80, stride=2), :] = v
    f1[pl.ds(1, 80, stride=2), :] = v
    for j in range(5):
        below = y1[j - 1] if j > 0 else zero
        above = y1[j + 1] if j < 4 else zero
        xa[j] = block_sweep(y1[j], w1[j], below, above) + f1[pl.ds(32 * j, 32), :]
    xb[0] = zero
    xb[4] = zero
    for old, new in ((xa, xb), (xb, xa)):
        for j in (1, 2, 3):
            c = old[j]
            t = around_block(c, old[j - 1], old[j + 1])
            new[j] = 0.2 * c + y1[j] + 0.5 * w1[j] * t
    one, two, three = xa[1], xa[2], xa[3]
    low = dot(jnp.concatenate([two, three], 0), picks(lambda i, j: i == (j >> 1), 1.0))
    high = dot(jnp.concatenate([one, two], 0), picks(lambda i, j: i == (j >> 1) + 64, 1.0))
    for q, v in enumerate((high[:32], low[:32], high[32:], low[32:])):
        f0[pl.ds(64 * q, 32, stride=2), :] = v
        f0[pl.ds(64 * q + 1, 32, stride=2), :] = v
    for i in range(8):
        x0[i] = xs[i] + f0[pl.ds(64 * (i // 2), 64), :]
    for i in range(6):
        c = x0[i + 1]
        x9[i] = 0.2 * c + yx[i] + wx[i] * around_plane(c, x0[i], x0[i + 2])
    for p in range(DEPTH):
        c = x9[p + 1]
        out(p, 0.2 * c + yx[p + 1] + wx[p + 1] * around_plane(c, x9[p], x9[p + 2]))


def first_up_body(
    x2, lo2, pair, hi2, wx, yx, xs, w, cap, src, u_out, b_out, up, dn, w1, y, x, rs, *work
):
    def out(p, u):
        u_out[0, p] = u
        b_out[p] = cap[p] * u + src[0, 1, p]

    fine_up(x2, lo2, pair, hi2, True, wx, yx, xs, w1, work, out)
    block = local_down(lambda p: b_out[p], cap, w, y, x, rs, *plane_picks(), False)
    fill_edges(up, dn, y, x)
    up[pl.ds(192, 32), :] = block
    dn[pl.ds(192, 32), :] = block


def next_up_body(x2, lo2, pair, hi2, wx, yx, xs, w1, start, u_out, *work):
    keep = lax.axis_index("tm") == 0

    def out(p, u):
        u_out[0, p] = jnp.where(keep, start[0, p], u)

    fine_up(x2, lo2, pair, hi2, False, wx, yx, xs, w1, work, out)


LOW_WORK = [(64, 128)]
LOW_FLOPS = 1 << 31
WORK = [
    (160, 128),
    (5, 32, 128),
    (5, 32, 128),
    (5, 32, 128),
    (256, 128),
    (8, NY, NX),
    (6, NY, NX),
]
EDGE_SUMS = (256, 128)
PLANE = (NY, NX)
PLANE4 = (DEPTH, NY, NX)
MESSAGE = f32(SLABS, 16, 128)


def moved(x, spans, slabs):
    pairs = []
    for t in range(SPANS):
        for s in range(SLABS):
            pairs.append((t * SLABS + s, (t + spans) % SPANS * SLABS + (s + slabs) % SLABS))
    return lax.ppermute(x, ("tm", "space"), pairs)


def exchanged(send, pair):
    got = lax.all_to_all(send, "space", 0, 0, tiled=True)
    return got, moved(pair, 0, 2), pair, moved(pair, 0, -2)


def shards(u0, src, cap):
    slab = f32(*PLANE4)
    w, y, x, block, up, dn, cap_in = call(
        pack_body,
        (slab, slab, slab, f32(64, 128), f32(288, 128), f32(288, 128), slab),
        [PLANE4, PLANE4, EDGE_SUMS],
        *(pltpu.with_memory_space_constraint(v, pltpu.HBM) for v in (u0, src, cap)),
        space=pl.BlockSpec(memory_space=pltpu.HBM),
        sems=[pltpu.SemaphoreType.DMA((3,))],
    )
    lo, hi = moved(up, 0, 1), moved(dn, 0, -1)
    wx, yx, xs, pair, send = call(
        first_down_body,
        (f32(6, *PLANE), f32(6, *PLANE), f32(8, *PLANE), f32(128, 128), MESSAGE),
        [EDGE_SUMS],
        *(w, y, x, block, lo, hi),
    )
    got, *near = exchanged(send, pair)
    w2, d2, w3, x2 = call(
        first_low_body,
        (f32(128, 128), f32(128, 128), f32(32, 128), f32(128, 128)),
        LOW_WORK,
        got,
        flops=LOW_FLOPS,
    )
    fpoint, b, up, dn, w1 = call(
        first_up_body,
        (f32(1, *PLANE4), slab, f32(224, 128), f32(224, 128), f32(5, 32, 128)),
        [PLANE4, PLANE4, EDGE_SUMS, *WORK],
        *(x2, *near, wx, yx, xs, w, cap_in, src),
    )
    b, lo, hi = moved(b, 1, 0), moved(up, 1, 1), moved(dn, 1, -1)
    yx, xs, pair, send = call(
        next_down_body,
        (f32(6, *PLANE), f32(8, *PLANE), f32(64, 128), MESSAGE),
        [PLANE4, PLANE4, EDGE_SUMS],
        *(b, lo, hi, cap_in, w, wx, pair),
    )
    got, *near = exchanged(send, pair)
    (x2,) = call(next_low_body, (f32(128, 128),), LOW_WORK, *(got, w2, d2, w3), flops=LOW_FLOPS)
    (updated,) = call(
        next_up_body, (f32(1, *PLANE4),), WORK, *(x2, *near, wx, yx, xs, w1, u0)
    )
    return fpoint, updated


def solution(mesh):
    in_specs = (
        P("tm", "space", None, None),
        P("tm", None, "space", None, None),
        P("space", None, None),
    )
    out_specs = (P("tm", "space", None, None), P("tm", "space", None, None))
    return jax.shard_map(shards, mesh=mesh, in_specs=in_specs, out_specs=out_specs, check_vma=False)
```

```python
import jax
import jax.numpy as jnp
from jax import lax
from jax.experimental import pallas as pl
from jax.experimental.pallas import tpu as pltpu
from jax.sharding import PartitionSpec as P

COARSE_SWEEPS = 24
NY, NX = 64, 128
SLABS = 32
SPANS = 8
DEPTH = 4
OMEGA = 0.8
F32 = jnp.float32
VMEM = pl.BlockSpec(memory_space=pltpu.VMEM)


def f32(*shape):
    return jax.ShapeDtypeStruct(shape, F32)


def call(body, outs, scratch, *args, space=VMEM, flops=None, sems=()):
    return pl.pallas_call(
        body,
        out_shape=outs,
        in_specs=[space] * len(args),
        out_specs=tuple(VMEM for _ in outs),
        scratch_shapes=[pltpu.VMEM(s, F32) for s in scratch] + list(sems),
        compiler_params=pltpu.CompilerParams(vmem_limit_bytes=16 << 20),
        cost_estimate=flops and pl.CostEstimate(flops=flops, transcendentals=0, bytes_accessed=0),
    )(*args)


def dot(a, pick):
    high = a.astype(jnp.bfloat16)
    rest = a - high.astype(F32)
    middle = rest.astype(jnp.bfloat16)
    low = (rest - middle.astype(F32)).astype(jnp.bfloat16)
    rows = a.shape[0]
    out = jnp.dot(jnp.concatenate([high, middle, low], 0), pick, preferred_element_type=F32)
    return (out[2 * rows :] + out[rows : 2 * rows]) + out[:rows]


def iota(shape, axis):
    return lax.broadcasted_iota(jnp.int32, shape, axis)


def picks(test, scale):
    i, j = iota((128, 128), 0), iota((128, 128), 1)
    return jnp.where(test(i, j), jnp.float32(scale), jnp.float32(0.0)).astype(jnp.bfloat16)


def inside_plane(c):
    row, lane = iota(c.shape, 0), iota(c.shape, 1)
    total = jnp.where(lane > 0, pltpu.roll(c, 1, 1), 0.0)
    total = total + jnp.where(lane < NX - 1, pltpu.roll(c, NX - 1, 1), 0.0)
    total = total + jnp.where(row > 0, pltpu.roll(c, 1, 0), 0.0)
    return total + jnp.where(row < NY - 1, pltpu.roll(c, NY - 1, 0), 0.0)


def around_plane(c, below, above):
    return inside_plane(c) + (below + above)


def around_block(c, below, above):
    row, lane = iota(c.shape, 0), iota(c.shape, 1)
    col = lane & 63
    total = pltpu.roll(c + jnp.where(lane < 64, above, below), 64, 1)
    total = total + jnp.where(col > 0, pltpu.roll(c, 1, 1), 0.0)
    total = total + jnp.where(col < 63, pltpu.roll(c, 127, 1), 0.0)
    total = total + jnp.where(row > 0, pltpu.roll(c, 1, 0), 0.0)
    return total + jnp.where(row < 31, pltpu.roll(c, 31, 0), 0.0)


def around_low(v):
    row, lane = iota(v.shape, 0), iota(v.shape, 1)
    y, x = row & 15, lane & 31
    ends = iota((16, 128), 1)
    below = jnp.where(ends >= 32, pltpu.roll(v[112:], 32, 1), 0.0)
    above = jnp.where(ends < 96, pltpu.roll(v[:16], 96, 1), 0.0)
    total = jnp.concatenate([below, v[:112]], 0) + jnp.concatenate([v[16:], above], 0)
    total = total + jnp.where(x > 0, pltpu.roll(v, 1, 1), 0.0)
    total = total + jnp.where(x < 31, pltpu.roll(v, 127, 1), 0.0)
    total = total + jnp.where(y > 0, pltpu.roll(v, 1, 0), 0.0)
    return total + jnp.where(y < 15, pltpu.roll(v, 127, 0), 0.0)


def coarsest(b3, w3):
    lane, row = iota((8, 128), 1), iota((8, 128), 0)
    x = lane & 15
    steps = []
    for k in range(4):
        w = w3[8 * k : 8 * k + 8]
        wh = 0.125 * w
        steps.append(
            (
                w * b3[8 * k : 8 * k + 8],
                wh,
                jnp.where(x > 0, wh, 0.0),
                jnp.where(x < 15, wh, 0.0),
                jnp.where(row > 0, wh, 0.0),
                jnp.where(row < 7, wh, 0.0),
            )
        )
    inside = lane < 64

    def sweep(_, v):
        below = jnp.where(inside, pltpu.roll(v[3], 16, 1), 0.0)
        above = jnp.where(inside, pltpu.roll(v[0], 112, 1), 0.0)
        line = (below, *v, above)
        new = []
        for k in range(4):
            wb, wh, left, right, up, down = steps[k]
            c = v[k]
            t = (0.2 * c + wb) + wh * (line[k] + line[k + 2])
            s = up * pltpu.roll(c, 1, 0) + down * pltpu.roll(c, 7, 0)
            e = left * pltpu.roll(c, 1, 1) + right * pltpu.roll(c, 127, 1)
            new.append((t + s) + e)
        return tuple(new)

    v = lax.fori_loop(0, COARSE_SWEEPS - 1, sweep, tuple(s[0] for s in steps), unroll=True)
    return jnp.concatenate(v, 0)


def row_pairs(ref, start, count):
    return ref[pl.ds(start, count, stride=2), :] + ref[pl.ds(start + 1, count, stride=2), :]


def block_sweep(y, w, below, above):
    return 1.2 * y + 0.5 * w * around_block(y, below, above)


def plane_picks():
    return (
        picks(lambda i, j: (i >> 1) == j, 0.125),
        picks(lambda i, j: (i >> 1) + 64 == j, 0.125),
    )


def local_down(b, cap, w, y, x, rs, lo_pick, hi_pick, first):
    for p in range(DEPTH):
        y[p] = w[p] * b(p)
    zero = jnp.zeros((NY, NX), F32)
    for p in range(DEPTH):
        below = y[p - 1] if p > 0 else zero
        above = y[p + 1] if p < 3 else zero
        x[p] = 1.2 * y[p] + w[p] * around_plane(y[p], below, above)
    for half in range(2):
        total = None
        for p in (2 * half, 2 * half + 1):
            below = x[p - 1] if p > 0 else zero
            above = x[p + 1] if p < 3 else zero
            r = b(p) - (cap[p] + 6.0) * x[p] + around_plane(x[p], below, above)
            total = r if total is None else total + r
        rs[pl.ds(64 * half, 64), :] = total
        if first:
            rs[pl.ds(128 + 64 * half, 64), :] = cap[2 * half] + cap[2 * half + 1]
    low, high = row_pairs(rs, 0, 32), row_pairs(rs, 64, 32)
    if first:
        low = jnp.concatenate([low, row_pairs(rs, 128, 32)], 0)
        high = jnp.concatenate([high, row_pairs(rs, 192, 32)], 0)
    return dot(low, lo_pick) + dot(high, hi_pick)


def fill_edges(up, dn, y, x):
    for edge, p, q in ((up, 3, 2), (dn, 0, 1)):
        edge[pl.ds(0, 64), :] = y[p]
        edge[pl.ds(64, 64), :] = x[p]
        edge[pl.ds(128, 64), :] = x[q]


def pack_body(u, src, cap, w, y, x, block, up, dn, cap_out, u_in, src_in, rs, sems):
    copies = [
        pltpu.make_async_copy(cap, cap_out, sems.at[0]),
        pltpu.make_async_copy(u.at[0], u_in, sems.at[1]),
        pltpu.make_async_copy(src.at[0, 0], src_in, sems.at[2]),
    ]
    for copy in copies:
        copy.start()
    lo_pick, hi_pick = plane_picks()
    for copy in copies:
        copy.wait()
    for p in range(DEPTH):
        w[p] = OMEGA / (cap_out[p] + 6.0)
        u_in[p] = cap_out[p] * u_in[p] + src_in[p]
    blocks = local_down(lambda p: u_in[p], cap_out, w, y, x, rs, lo_pick, hi_pick, True)
    block[...] = blocks
    fill_edges(up, dn, y, x)
    lane = iota((32, 128), 1)
    b1, c1 = blocks[:32], blocks[32:]
    up[pl.ds(192, 32), :] = jnp.where(lane < 64, pltpu.roll(b1, 64, 1), c1)
    dn[pl.ds(192, 32), :] = jnp.where(lane < 64, b1, pltpu.roll(c1, 64, 1))
    up[pl.ds(224, 64), :] = w[3]
    dn[pl.ds(224, 64), :] = w[0]


def finish_down(first, w, y, x, b1, c1, lo, hi, wx, yx, xs, pair, rs):
    lo_pick, hi_pick = plane_picks()
    s = lax.axis_index("space")
    lane = iota((32, 128), 1)

    def edge(ref, there):
        return [
            jnp.where(there, ref[pl.ds(start, 64), :], 0.0)
            for start in ((0, 64, 128, 224) if first else (0, 64, 128))
        ]

    sides = []
    for ref, there, i, p in ((lo, s > 0, 0, 0), (hi, s < SLABS - 1, 5, 3)):
        ye, xe, xs_far, *we = edge(ref, there)
        if first:
            wx[i] = we[0]
        yx[i] = ye
        near = w[p] * ye
        far = wx[i] * y[p]
        x_near, x_far = x[p] + near, xe + far
        j = 1 if p == 0 else 6
        xs[j] = x_far
        xs[0 if p == 0 else 7] = xs_far
        xs[p + 2] = x_near
        own = (near - OMEGA * ye) + inside_plane(near) + x_far
        beside = (far - OMEGA * y[p]) + inside_plane(far) + x_near
        sides.append((own, jnp.where(there, beside, 0.0)))
    for p in range(DEPTH):
        yx[p + 1] = y[p]
        if first:
            wx[p + 1] = w[p]
    xs[3] = x[1]
    xs[4] = x[2]
    for k, v in enumerate((sides[0][0], sides[1][1], sides[1][0], sides[0][1])):
        rs[pl.ds(64 * k, 64), :] = v
    low = jnp.concatenate([row_pairs(rs, 0, 32), row_pairs(rs, 64, 32)], 0)
    high = jnp.concatenate([row_pairs(rs, 128, 32), row_pairs(rs, 192, 32)], 0)
    terms = dot(low, lo_pick) + dot(high, hi_pick)
    lo_block, hi_block = lo[pl.ds(192, 32), :], hi[pl.ds(192, 32), :]
    if first:
        pair[pl.ds(64, 32), :] = c1
        pair[pl.ds(96, 32), :] = jnp.where(lane < 64, pltpu.roll(hi_block, 64, 1), lo_block)
        lo_block = pltpu.roll(lo_block, 64, 1)
    own = b1 + terms[:32]
    pair[pl.ds(0, 32), :] = own
    pair[pl.ds(32, 32), :] = jnp.where(lane < 64, hi_block, lo_block) + terms[32:]
    return own


def share(b1, c1, c_mix, send, rs):
    s = lax.axis_index("space")
    lane = iota((32, 128), 1)
    zero = jnp.zeros((32, 128), F32)
    own, beside = c1 + 3.0, c_mix + 3.0
    w_own, w_mix = OMEGA / own, OMEGA / beside
    y = w_own * b1
    x = [
        block_sweep(zero, jnp.where((lane >= 64) & (s > 0), w_mix, 0.0), zero, y),
        block_sweep(y, w_own, zero, zero),
        block_sweep(zero, jnp.where((lane < 64) & (s < SLABS - 1), w_mix, 0.0), y, zero),
    ]
    r = [
        0.5 * around_block(x[0], zero, x[1]) - beside * x[0],
        b1 - own * x[1] + 0.5 * around_block(x[1], x[0], x[2]),
        0.5 * around_block(x[2], x[1], zero) - beside * x[2],
        c1,
    ]
    for k in range(4):
        rs[pl.ds(32 * k, 32), :] = r[k]
    low = dot(row_pairs(rs, 0, 64), picks(lambda i, j: ((i & 63) >> 1) == (j & 31), 0.125))
    group = iota((16, 128), 1) >> 5
    message = low[48:]
    for k in range(3):
        message = jnp.where(group == k, low[16 * k : 16 * k + 16], message)
    for peer in range(SLABS):
        send[peer] = message


def first_down_body(w, y, x, block, lo, hi, wx, yx, xs, pair, send, rs):
    b1, c1 = block[pl.ds(0, 32), :], block[pl.ds(32, 32), :]
    own = finish_down(True, w, y, x, b1, c1, lo, hi, wx, yx, xs, pair, rs)
    share(own, c1, pair[pl.ds(96, 32), :], send, rs)


def next_down_body(y, x, block, lo, hi, w, wx, yx, xs, pair, rs):
    finish_down(False, w, y, x, block[...], None, lo, hi, wx, yx, xs, pair, rs)


def wide_share(block, y, x, wx, w1, c1, send, rs):
    lane = iota((32, 128), 1)
    zero = jnp.zeros((32, 128), F32)
    for k, (i, p) in enumerate(((0, 0), (5, 3))):
        far = wx[i] * y[p]
        rs[pl.ds(64 * k, 64), :] = far
        rs[pl.ds(128 + 64 * k, 64), :] = (far - OMEGA * y[p]) + inside_plane(far) + x[p]
    lo_pick, hi_pick = plane_picks()
    low = jnp.concatenate([row_pairs(rs, 0, 32), row_pairs(rs, 192, 32)], 0)
    high = jnp.concatenate([row_pairs(rs, 64, 32), row_pairs(rs, 128, 32)], 0)
    terms = dot(low, lo_pick) + dot(high, hi_pick)
    mix = terms[32:]
    b = [jnp.where(lane >= 64, mix, 0.0), block + terms[:32], jnp.where(lane < 64, mix, 0.0)]
    v = [zero] + [w1[j + 1] * b[j] for j in range(3)] + [zero]
    v = [zero] + [block_sweep(v[j], w1[j], v[j - 1], v[j + 1]) for j in (1, 2, 3)] + [zero]
    r = [0.5 * around_block(zero, zero, v[1])]
    for j in (1, 2, 3):
        r.append(b[j - 1] - (c1[j] + 3.0) * v[j] + 0.5 * around_block(v[j], v[j - 1], v[j + 1]))
    r.append(0.5 * around_block(zero, v[3], zero))
    for k in range(5):
        rs[pl.ds(32 * k, 32), :] = r[k]
    low = dot(row_pairs(rs, 0, 80), picks(lambda i, j: ((i & 63) >> 1) == (j & 31), 0.125))
    group = iota((16, 128), 1) >> 5
    message = low[:16]
    for k in (1, 2, 3):
        message = jnp.where(group == k, low[16 * k : 16 * k + 16], message)
    last = jnp.where(group[:8] == 0, low[64:72], low[72:80])
    for peer in range(SLABS):
        send[peer, pl.ds(0, 16), :] = message
        send[peer, pl.ds(16, 8), :] = last


def spread(v):
    v = v + pltpu.roll(v, 64, 1)
    return v + pltpu.roll(v, 32, 1)


def to_coarsest(v, t3):
    for k in range(4):
        t3[pl.ds(16 * k, 16), :] = v[32 * k : 32 * k + 16] + v[32 * k + 16 : 32 * k + 32]
    pick = picks(lambda i, j: (j < 64) & ((i >> 5) == (j >> 4)) & (((i & 31) >> 1) == (j & 15)), 0.125)
    return dot(row_pairs(t3, 0, 32), pick)


def from_coarsest(v, t3):
    pick = picks(lambda i, j: (i < 64) & ((j >> 5) == (i >> 4)) & (((j & 31) >> 1) == (i & 15)), 1.0)
    v = dot(v, pick)
    t3[pl.ds(0, 32, stride=2), :] = v
    t3[pl.ds(1, 32, stride=2), :] = v
    parts = []
    for k in range(4):
        block = t3[pl.ds(16 * k, 16), :]
        parts += [block, block]
    return jnp.concatenate(parts, 0)


def low_levels(first, got, w2, d2, w3, x2, t3):
    group = iota((16, 128), 1) >> 5
    narrow = iota((8, 128), 1) >> 5
    reach = 1 if first else 2
    parts, caps = [], []
    for zl in range(8):
        total, cap = None, None
        for zh in range(4):
            z = 8 * zh + zl
            v = jnp.zeros((16, 128), F32)
            for k in range(3 if first else 4):
                if 0 <= z + reach - k < SLABS:
                    v = jnp.where(group == k, got[z + reach - k, pl.ds(0, 16), :], v)
            if not first and z >= 2:
                last = got[z - 2, pl.ds(16, 8), :]
                halves = [jnp.where(narrow == k, last, 0.0) for k in range(2)]
                v = v + jnp.concatenate(halves, 0)
            v = spread(v)
            total = v if total is None else jnp.where(group == zh, v, total)
            if first:
                v = spread(jnp.where(group == 3, got[z], 0.0))
                cap = v if cap is None else jnp.where(group == zh, v, cap)
        parts.append(total)
        caps.append(cap)
    b = jnp.concatenate(parts, 0)
    if first:
        c2 = jnp.concatenate(caps, 0)
        d2[...] = c2 + 1.5
        w2[...] = OMEGA / (c2 + 1.5)
        w3[...] = OMEGA / (to_coarsest(c2, t3) + 0.75)
    w, d = w2[...], d2[...]
    y = w * b
    x = 1.2 * y + 0.25 * w * around_low(y)
    r = b - d * x + 0.25 * around_low(x)
    x = x + from_coarsest(coarsest(to_coarsest(r, t3), w3[...]), t3)
    for _ in range(2):
        x = 0.2 * x + y + 0.25 * w * around_low(x)
    x2[...] = x


def first_low_body(got, w2, d2, w3, x2, t3):
    low_levels(True, got, w2, d2, w3, x2, t3)


def next_low_body(got, w2, d2, w3, after, x2, t3):
    low_levels(False, got, w2, d2, w3, x2, t3)


def fine_up(x2, lo2, pair, hi2, c1, wx, yx, xs, w1, work, out):
    f1, y1, xa, xb, f0, x0, x9 = work
    s = lax.axis_index("space")
    lane = iota((32, 128), 1)

    def blocks(start):
        mixed = [ref[pl.ds(start + 32, 32), :] for ref in (lo2, pair, hi2)]
        return (
            lo2[pl.ds(start, 32), :],
            jnp.where(lane < 64, mixed[0], mixed[1]),
            pair[pl.ds(start, 32), :],
            jnp.where(lane < 64, mixed[1], mixed[2]),
            hi2[pl.ds(start, 32), :],
        )

    if c1 is not None:
        for j, c in enumerate(blocks(64)):
            c1[j] = c
            z = s + (j - 2)
            w1[j] = jnp.where((z >= 0) & (z < SLABS), OMEGA / (c + 3.0), 0.0)
    for j, b in enumerate(blocks(0)):
        y1[j] = w1[j] * b
    zero = jnp.zeros((32, 128), F32)
    group = iota((16, 128), 1) >> 5
    parts = []
    for j in range(5):
        z = s + (j - 2)
        v = x2[pl.ds(pl.multiple_of((z & 7) * 16, 16), 16), :]
        parts.append(spread(jnp.where(group == (z >> 3), v, 0.0)))
    pick = picks(lambda i, j: i == ((j & 63) >> 1), 1.0)
    v = dot(jnp.concatenate(parts, 0), pick)
    f1[pl.ds(0, 80, stride=2), :] = v
    f1[pl.ds(1, 80, stride=2), :] = v
    for j in range(5):
        below = y1[j - 1] if j > 0 else zero
        above = y1[j + 1] if j < 4 else zero
        xa[j] = block_sweep(y1[j], w1[j], below, above) + f1[pl.ds(32 * j, 32), :]
    xb[0] = zero
    xb[4] = zero
    for old, new in ((xa, xb), (xb, xa)):
        for j in (1, 2, 3):
            c = old[j]
            t = around_block(c, old[j - 1], old[j + 1])
            new[j] = 0.2 * c + y1[j] + 0.5 * w1[j] * t
    one, two, three = xa[1], xa[2], xa[3]
    low = dot(jnp.concatenate([two, three], 0), picks(lambda i, j: i == (j >> 1), 1.0))
    high = dot(jnp.concatenate([one, two], 0), picks(lambda i, j: i == (j >> 1) + 64, 1.0))
    for q, v in enumerate((high[:32], low[:32], high[32:], low[32:])):
        f0[pl.ds(64 * q, 32, stride=2), :] = v
        f0[pl.ds(64 * q + 1, 32, stride=2), :] = v
    for i in range(8):
        x0[i] = xs[i] + f0[pl.ds(64 * (i // 2), 64), :]
    for i in range(6):
        c = x0[i + 1]
        x9[i] = 0.2 * c + yx[i] + wx[i] * around_plane(c, x0[i], x0[i + 2])
    for p in range(DEPTH):
        c = x9[p + 1]
        out(p, 0.2 * c + yx[p + 1] + wx[p + 1] * around_plane(c, x9[p], x9[p + 2]))


def first_up_body(
    x2, lo2, pair, hi2, wx, yx, xs, w, cap, src, u_out, y, x, block, up, dn, w1, send, *work
):
    b_out, c1, rs, *work = work

    def out(p, u):
        u_out[0, p] = u
        b_out[p] = cap[p] * u + src[0, 1, p]

    fine_up(x2, lo2, pair, hi2, c1, wx, yx, xs, w1, work, out)
    own = local_down(lambda p: b_out[p], cap, w, y, x, rs, *plane_picks(), False)
    wide_share(own, y, x, wx, w1, c1, send, rs)
    block[...] = own
    fill_edges(up, dn, y, x)
    up[pl.ds(192, 32), :] = own
    dn[pl.ds(192, 32), :] = own


def next_up_body(x2, lo2, pair, hi2, wx, yx, xs, w1, u_out, *work):
    def out(p, u):
        u_out[0, p] = u

    fine_up(x2, lo2, pair, hi2, None, wx, yx, xs, w1, work, out)


LOW_WORK = [(64, 128)]
LOW_FLOPS = 1 << 31
WORK = [
    (160, 128),
    (5, 32, 128),
    (5, 32, 128),
    (5, 32, 128),
    (256, 128),
    (8, NY, NX),
    (6, NY, NX),
]
EDGE_SUMS = (256, 128)
PLANE = (NY, NX)
PLANE4 = (DEPTH, NY, NX)
MESSAGE = f32(SLABS, 16, 128)
WIDE_MESSAGE = f32(SLABS, 24, 128)


def moved(x, spans, slabs):
    pairs = []
    for t in range(SPANS):
        for s in range(SLABS):
            pairs.append((t * SLABS + s, (t + spans) % SPANS * SLABS + (s + slabs) % SLABS))
    return lax.ppermute(x, ("tm", "space"), pairs)


def gathered(send):
    return lax.all_to_all(send, "space", 0, 0, tiled=True)


def near(pair):
    return moved(pair, 0, 2), pair, moved(pair, 0, -2)


def shards(u0, src, cap):
    slab = f32(*PLANE4)
    w, y, x, block, up, dn, cap_in = call(
        pack_body,
        (slab, slab, slab, f32(64, 128), f32(288, 128), f32(288, 128), slab),
        [PLANE4, PLANE4, EDGE_SUMS],
        *(pltpu.with_memory_space_constraint(v, pltpu.HBM) for v in (u0, src, cap)),
        space=pl.BlockSpec(memory_space=pltpu.HBM),
        sems=[pltpu.SemaphoreType.DMA((3,))],
    )
    lo, hi = moved(up, 0, 1), moved(dn, 0, -1)
    wx, yx, xs, pair, send = call(
        first_down_body,
        (f32(6, *PLANE), f32(6, *PLANE), f32(8, *PLANE), f32(128, 128), MESSAGE),
        [EDGE_SUMS],
        *(w, y, x, block, lo, hi),
    )
    got = gathered(send)
    w2, d2, w3, x2 = call(
        first_low_body,
        (f32(128, 128), f32(128, 128), f32(32, 128), f32(128, 128)),
        LOW_WORK,
        got,
        flops=LOW_FLOPS,
    )
    fpoint, y, x, block, up, dn, w1, send = call(
        first_up_body,
        (
            f32(1, *PLANE4),
            slab,
            slab,
            f32(32, 128),
            f32(224, 128),
            f32(224, 128),
            f32(5, 32, 128),
            WIDE_MESSAGE,
        ),
        [PLANE4, (5, 32, 128), EDGE_SUMS, *WORK],
        *(x2, *near(pair), wx, yx, xs, w, cap_in, src),
    )
    got = gathered(send)
    lo, hi = moved(up, 0, 1), moved(dn, 0, -1)
    yx, xs, pair = call(
        next_down_body,
        (f32(6, *PLANE), f32(8, *PLANE), f32(64, 128)),
        [EDGE_SUMS],
        *(y, x, block, lo, hi, w, wx),
    )
    (x2,) = call(
        next_low_body, (f32(128, 128),), LOW_WORK, *(got, w2, d2, w3, pair), flops=LOW_FLOPS
    )
    (u,) = call(next_up_body, (f32(1, *PLANE4),), WORK, *(x2, *near(pair), wx, yx, xs, w1))
    updated = jnp.where(lax.axis_index("tm") == 0, u0, moved(u, 1, 0))
    return fpoint, updated


def solution(mesh):
    in_specs = (
        P("tm", "space", None, None),
        P("tm", None, "space", None, None),
        P("space", None, None),
    )
    out_specs = (P("tm", "space", None, None), P("tm", "space", None, None))
    return jax.shard_map(shards, mesh=mesh, in_specs=in_specs, out_specs=out_specs, check_vma=False)
```

```python
import jax
import jax.numpy as jnp
from jax import lax
from jax.experimental import pallas as pl
from jax.experimental.pallas import tpu as pltpu
from jax.sharding import PartitionSpec as P


COARSE_SWEEPS = 24
NY, NX = 64, 128
SLABS = 32
SPANS = 8
DEPTH = 4
OMEGA = 0.8
F32 = jnp.float32
VMEM = pl.BlockSpec(memory_space=pltpu.VMEM)


def f32(*shape):
    return jax.ShapeDtypeStruct(shape, F32)


def call(body, outs, scratch, *args, space=VMEM, flops=None, sems=()):
    return pl.pallas_call(
        body,
        out_shape=outs,
        in_specs=[space] * len(args),
        out_specs=tuple(VMEM for _ in outs),
        scratch_shapes=[pltpu.VMEM(s, F32) for s in scratch] + list(sems),
        compiler_params=pltpu.CompilerParams(vmem_limit_bytes=16 << 20),
        cost_estimate=flops and pl.CostEstimate(flops=flops, transcendentals=0, bytes_accessed=0),
    )(*args)


def dot(a, pick):
    high = a.astype(jnp.bfloat16)
    rest = a - high.astype(F32)
    middle = rest.astype(jnp.bfloat16)
    low = (rest - middle.astype(F32)).astype(jnp.bfloat16)
    rows = a.shape[0]
    out = jnp.dot(jnp.concatenate([high, middle, low], 0), pick, preferred_element_type=F32)
    return (out[2 * rows :] + out[rows : 2 * rows]) + out[:rows]


def iota(shape, axis):
    return lax.broadcasted_iota(jnp.int32, shape, axis)


def picks(test, scale):
    i, j = iota((128, 128), 0), iota((128, 128), 1)
    return jnp.where(test(i, j), jnp.float32(scale), jnp.float32(0.0)).astype(jnp.bfloat16)


def inside_plane(c):
    row, lane = iota(c.shape, 0), iota(c.shape, 1)
    total = jnp.where(lane > 0, pltpu.roll(c, 1, 1), 0.0)
    total = total + jnp.where(lane < NX - 1, pltpu.roll(c, NX - 1, 1), 0.0)
    total = total + jnp.where(row > 0, pltpu.roll(c, 1, 0), 0.0)
    return total + jnp.where(row < NY - 1, pltpu.roll(c, NY - 1, 0), 0.0)


def around_plane(c, below, above):
    return inside_plane(c) + (below + above)


def around_block(c, below, above):
    row, lane = iota(c.shape, 0), iota(c.shape, 1)
    col = lane & 63
    total = pltpu.roll(c + jnp.where(lane < 64, above, below), 64, 1)
    total = total + jnp.where(col > 0, pltpu.roll(c, 1, 1), 0.0)
    total = total + jnp.where(col < 63, pltpu.roll(c, 127, 1), 0.0)
    total = total + jnp.where(row > 0, pltpu.roll(c, 1, 0), 0.0)
    return total + jnp.where(row < 31, pltpu.roll(c, 31, 0), 0.0)


def around_low(v):
    row, lane = iota(v.shape, 0), iota(v.shape, 1)
    y, x = row & 15, lane & 31
    ends = iota((16, 128), 1)
    below = jnp.where(ends >= 32, pltpu.roll(v[112:], 32, 1), 0.0)
    above = jnp.where(ends < 96, pltpu.roll(v[:16], 96, 1), 0.0)
    total = jnp.concatenate([below, v[:112]], 0) + jnp.concatenate([v[16:], above], 0)
    total = total + jnp.where(x > 0, pltpu.roll(v, 1, 1), 0.0)
    total = total + jnp.where(x < 31, pltpu.roll(v, 127, 1), 0.0)
    total = total + jnp.where(y > 0, pltpu.roll(v, 1, 0), 0.0)
    return total + jnp.where(y < 15, pltpu.roll(v, 127, 0), 0.0)


def rolled(v, k, j):
    return pltpu.roll(v[k % 4], (j - 16 * (k // 4)) % 128, 1) if (k // 4 or j) else v[k]


CENTRE = [(k, 0) for k in range(4)]
FIRST = [(k, j) for k in range(4) for j in (-1, 0, 1)] + [(-1, 0), (4, 0)]


def coarsest(b3, w3):
    lane, row = iota((8, 128), 1), iota((8, 128), 0)
    x = lane & 15
    used = lane < 64
    base, own = [], []
    for k in range(4):
        w = jnp.where(used, w3[8 * k : 8 * k + 8], 0.0)
        wh = 0.125 * w
        own.append(w * b3[8 * k : 8 * k + 8])
        base.append(
            (
                wh,
                jnp.where(x > 0, wh, 0.0),
                jnp.where(x < 15, wh, 0.0),
                jnp.where(row > 0, wh, 0.0),
                jnp.where(row < 7, wh, 0.0),
            )
        )
    terms = list(zip(*base))
    steps = {
        (k, j): (rolled(own, k, j), *(rolled(t, k, j) for t in terms)) for k, j in FIRST
    }

    def sweep(v, k, j):
        wb, wh, left, right, up, down = steps[k, j]
        c = v[k, j]
        t = (0.2 * c + wb) + wh * (v[k - 1, j] + v[k + 1, j])
        s = up * pltpu.roll(c, 1, 0) + down * pltpu.roll(c, 7, 0)
        return (t + s) + (left * v[k, j + 1] + right * v[k, j - 1])

    def copies(v, reach):
        return {
            (k, j): rolled(v, k, j)
            for k in range(-reach, 4 + reach)
            for j in range(-reach, reach + 1)
            if max(0, -k, k - 3) + abs(j) <= reach
        }

    def one(v):
        v = copies(v, 1)
        return [sweep(v, k, j) for k, j in CENTRE]

    def two(_, v):
        v = copies(v, 2)
        v = {(k, j): sweep(v, k, j) for k, j in FIRST}
        return tuple(sweep(v, k, j) for k, j in CENTRE)

    pairs, rest = divmod(COARSE_SWEEPS - 1, 2)
    v = one(own) if rest else own
    v = lax.fori_loop(0, pairs, two, tuple(v), unroll=True)
    return jnp.concatenate(v, 0)


def row_pairs(ref, start, count):
    return ref[pl.ds(start, count, stride=2), :] + ref[pl.ds(start + 1, count, stride=2), :]


def block_sweep(y, w, below, above):
    return 1.2 * y + 0.5 * w * around_block(y, below, above)


def plane_picks():
    return (
        picks(lambda i, j: (i >> 1) == j, 0.125),
        picks(lambda i, j: (i >> 1) + 64 == j, 0.125),
    )


def local_down(b, cap, w, y, x, rs, lo_pick, hi_pick, first):
    for p in range(DEPTH):
        y[p] = w[p] * b(p)
    zero = jnp.zeros((NY, NX), F32)
    for p in range(DEPTH):
        below = y[p - 1] if p > 0 else zero
        above = y[p + 1] if p < 3 else zero
        x[p] = 1.2 * y[p] + w[p] * around_plane(y[p], below, above)
    for half in range(2):
        total = None
        for p in (2 * half, 2 * half + 1):
            below = x[p - 1] if p > 0 else zero
            above = x[p + 1] if p < 3 else zero
            r = b(p) - (cap[p] + 6.0) * x[p] + around_plane(x[p], below, above)
            total = r if total is None else total + r
        rs[pl.ds(64 * half, 64), :] = total
        if first:
            rs[pl.ds(128 + 64 * half, 64), :] = cap[2 * half] + cap[2 * half + 1]
    low, high = row_pairs(rs, 0, 32), row_pairs(rs, 64, 32)
    if first:
        low = jnp.concatenate([low, row_pairs(rs, 128, 32)], 0)
        high = jnp.concatenate([high, row_pairs(rs, 192, 32)], 0)
    return dot(low, lo_pick) + dot(high, hi_pick)


def fill_edges(up, dn, y, x):
    for edge, p, q in ((up, 3, 2), (dn, 0, 1)):
        edge[pl.ds(0, 64), :] = y[p]
        edge[pl.ds(64, 64), :] = x[p]
        edge[pl.ds(128, 64), :] = x[q]


def pack_body(u, src, cap, w, y, x, block, up, dn, cap_out, u_in, src_in, rs, sems):
    copies = [
        pltpu.make_async_copy(cap, cap_out, sems.at[0]),
        pltpu.make_async_copy(u.at[0], u_in, sems.at[1]),
        pltpu.make_async_copy(src.at[0, 0], src_in, sems.at[2]),
    ]
    for copy in copies:
        copy.start()
    lo_pick, hi_pick = plane_picks()
    for copy in copies:
        copy.wait()
    for p in range(DEPTH):
        w[p] = OMEGA / (cap_out[p] + 6.0)
        u_in[p] = cap_out[p] * u_in[p] + src_in[p]
    blocks = local_down(lambda p: u_in[p], cap_out, w, y, x, rs, lo_pick, hi_pick, True)
    block[...] = blocks
    fill_edges(up, dn, y, x)
    lane = iota((32, 128), 1)
    b1, c1 = blocks[:32], blocks[32:]
    up[pl.ds(192, 32), :] = jnp.where(lane < 64, pltpu.roll(b1, 64, 1), c1)
    dn[pl.ds(192, 32), :] = jnp.where(lane < 64, b1, pltpu.roll(c1, 64, 1))
    up[pl.ds(224, 64), :] = w[3]
    dn[pl.ds(224, 64), :] = w[0]


def finish_down(first, w, y, x, b1, c1, lo, hi, wx, yx, xs, pair, rs):
    lo_pick, hi_pick = plane_picks()
    s = lax.axis_index("space")
    lane = iota((32, 128), 1)

    def edge(ref, there):
        return [
            jnp.where(there, ref[pl.ds(start, 64), :], 0.0)
            for start in ((0, 64, 128, 224) if first else (0, 64, 128))
        ]

    sides = []
    for ref, there, i, p in ((lo, s > 0, 0, 0), (hi, s < SLABS - 1, 5, 3)):
        ye, xe, xs_far, *we = edge(ref, there)
        if first:
            wx[i] = we[0]
        yx[i] = ye
        near = w[p] * ye
        far = wx[i] * y[p]
        x_near, x_far = x[p] + near, xe + far
        j = 1 if p == 0 else 6
        xs[j] = x_far
        xs[0 if p == 0 else 7] = xs_far
        xs[p + 2] = x_near
        own = (near - OMEGA * ye) + inside_plane(near) + x_far
        beside = (far - OMEGA * y[p]) + inside_plane(far) + x_near
        sides.append((own, jnp.where(there, beside, 0.0)))
    for p in range(DEPTH):
        yx[p + 1] = y[p]
        if first:
            wx[p + 1] = w[p]
    xs[3] = x[1]
    xs[4] = x[2]
    for k, v in enumerate((sides[0][0], sides[1][1], sides[1][0], sides[0][1])):
        rs[pl.ds(64 * k, 64), :] = v
    low = jnp.concatenate([row_pairs(rs, 0, 32), row_pairs(rs, 64, 32)], 0)
    high = jnp.concatenate([row_pairs(rs, 128, 32), row_pairs(rs, 192, 32)], 0)
    terms = dot(low, lo_pick) + dot(high, hi_pick)
    lo_block, hi_block = lo[pl.ds(192, 32), :], hi[pl.ds(192, 32), :]
    if first:
        pair[pl.ds(64, 32), :] = c1
        pair[pl.ds(96, 32), :] = jnp.where(lane < 64, pltpu.roll(hi_block, 64, 1), lo_block)
        lo_block = pltpu.roll(lo_block, 64, 1)
    own = b1 + terms[:32]
    pair[pl.ds(0, 32), :] = own
    pair[pl.ds(32, 32), :] = jnp.where(lane < 64, hi_block, lo_block) + terms[32:]
    return own


def share(b1, c1, c_mix, send, rs):
    s = lax.axis_index("space")
    lane = iota((32, 128), 1)
    zero = jnp.zeros((32, 128), F32)
    own, beside = c1 + 3.0, c_mix + 3.0
    w_own, w_mix = OMEGA / own, OMEGA / beside
    y = w_own * b1
    x = [
        block_sweep(zero, jnp.where((lane >= 64) & (s > 0), w_mix, 0.0), zero, y),
        block_sweep(y, w_own, zero, zero),
        block_sweep(zero, jnp.where((lane < 64) & (s < SLABS - 1), w_mix, 0.0), y, zero),
    ]
    r = [
        0.5 * around_block(x[0], zero, x[1]) - beside * x[0],
        b1 - own * x[1] + 0.5 * around_block(x[1], x[0], x[2]),
        0.5 * around_block(x[2], x[1], zero) - beside * x[2],
        c1,
    ]
    for k in range(4):
        rs[pl.ds(32 * k, 32), :] = r[k]
    low = dot(row_pairs(rs, 0, 64), picks(lambda i, j: ((i & 63) >> 1) == (j & 31), 0.125))
    group = iota((16, 128), 1) >> 5
    message = low[48:]
    for k in range(3):
        message = jnp.where(group == k, low[16 * k : 16 * k + 16], message)
    for peer in range(SLABS):
        send[peer] = message


def first_down_body(w, y, x, block, lo, hi, wx, yx, xs, pair, send, rs):
    b1, c1 = block[pl.ds(0, 32), :], block[pl.ds(32, 32), :]
    own = finish_down(True, w, y, x, b1, c1, lo, hi, wx, yx, xs, pair, rs)
    share(own, c1, pair[pl.ds(96, 32), :], send, rs)


def next_down_body(y, x, block, lo, hi, w, wx, yx, xs, pair, rs):
    finish_down(False, w, y, x, block[...], None, lo, hi, wx, yx, xs, pair, rs)


def wide_share(block, y, x, wx, w1, c1, send, rs):
    lane = iota((32, 128), 1)
    zero = jnp.zeros((32, 128), F32)
    for k, (i, p) in enumerate(((0, 0), (5, 3))):
        far = wx[i] * y[p]
        rs[pl.ds(64 * k, 64), :] = far
        rs[pl.ds(128 + 64 * k, 64), :] = (far - OMEGA * y[p]) + inside_plane(far) + x[p]
    lo_pick, hi_pick = plane_picks()
    low = jnp.concatenate([row_pairs(rs, 0, 32), row_pairs(rs, 192, 32)], 0)
    high = jnp.concatenate([row_pairs(rs, 64, 32), row_pairs(rs, 128, 32)], 0)
    terms = dot(low, lo_pick) + dot(high, hi_pick)
    mix = terms[32:]
    b = [jnp.where(lane >= 64, mix, 0.0), block + terms[:32], jnp.where(lane < 64, mix, 0.0)]
    v = [zero] + [w1[j + 1] * b[j] for j in range(3)] + [zero]
    v = [zero] + [block_sweep(v[j], w1[j], v[j - 1], v[j + 1]) for j in (1, 2, 3)] + [zero]
    r = [0.5 * around_block(zero, zero, v[1])]
    for j in (1, 2, 3):
        r.append(b[j - 1] - (c1[j] + 3.0) * v[j] + 0.5 * around_block(v[j], v[j - 1], v[j + 1]))
    r.append(0.5 * around_block(zero, v[3], zero))
    for k in range(5):
        rs[pl.ds(32 * k, 32), :] = r[k]
    low = dot(row_pairs(rs, 0, 80), picks(lambda i, j: ((i & 63) >> 1) == (j & 31), 0.125))
    group = iota((16, 128), 1) >> 5
    message = low[:16]
    for k in (1, 2, 3):
        message = jnp.where(group == k, low[16 * k : 16 * k + 16], message)
    last = jnp.where(group[:8] == 0, low[64:72], low[72:80])
    for peer in range(SLABS):
        send[peer, pl.ds(0, 16), :] = message
        send[peer, pl.ds(16, 8), :] = last


def spread(v):
    v = v + pltpu.roll(v, 64, 1)
    return v + pltpu.roll(v, 32, 1)


def to_coarsest(v, t3):
    for k in range(4):
        t3[pl.ds(16 * k, 16), :] = v[32 * k : 32 * k + 16] + v[32 * k + 16 : 32 * k + 32]
    pick = picks(lambda i, j: (j < 64) & ((i >> 5) == (j >> 4)) & (((i & 31) >> 1) == (j & 15)), 0.125)
    return dot(row_pairs(t3, 0, 32), pick)


def from_coarsest(v, t3):
    pick = picks(lambda i, j: (i < 64) & ((j >> 5) == (i >> 4)) & (((j & 31) >> 1) == (i & 15)), 1.0)
    v = dot(v, pick)
    t3[pl.ds(0, 32, stride=2), :] = v
    t3[pl.ds(1, 32, stride=2), :] = v
    parts = []
    for k in range(4):
        block = t3[pl.ds(16 * k, 16), :]
        parts += [block, block]
    return jnp.concatenate(parts, 0)


def low_levels(first, got, w2, d2, w3, x2, t3):
    group = iota((16, 128), 1) >> 5
    narrow = iota((8, 128), 1) >> 5
    reach = 1 if first else 2
    parts, caps = [], []
    for zl in range(8):
        total, cap = None, None
        for zh in range(4):
            z = 8 * zh + zl
            v = jnp.zeros((16, 128), F32)
            for k in range(3 if first else 4):
                if 0 <= z + reach - k < SLABS:
                    v = jnp.where(group == k, got[z + reach - k, pl.ds(0, 16), :], v)
            if not first and z >= 2:
                last = got[z - 2, pl.ds(16, 8), :]
                halves = [jnp.where(narrow == k, last, 0.0) for k in range(2)]
                v = v + jnp.concatenate(halves, 0)
            v = spread(v)
            total = v if total is None else jnp.where(group == zh, v, total)
            if first:
                v = spread(jnp.where(group == 3, got[z], 0.0))
                cap = v if cap is None else jnp.where(group == zh, v, cap)
        parts.append(total)
        caps.append(cap)
    b = jnp.concatenate(parts, 0)
    if first:
        c2 = jnp.concatenate(caps, 0)
        d2[...] = c2 + 1.5
        w2[...] = OMEGA / (c2 + 1.5)
        w3[...] = OMEGA / (to_coarsest(c2, t3) + 0.75)
    w, d = w2[...], d2[...]
    y = w * b
    x = 1.2 * y + 0.25 * w * around_low(y)
    r = b - d * x + 0.25 * around_low(x)
    x = x + from_coarsest(coarsest(to_coarsest(r, t3), w3[...]), t3)
    for _ in range(2):
        x = 0.2 * x + y + 0.25 * w * around_low(x)
    x2[...] = x


def first_low_body(got, w2, d2, w3, x2, t3):
    low_levels(True, got, w2, d2, w3, x2, t3)


def next_low_body(got, w2, d2, w3, after, x2, t3):
    low_levels(False, got, w2, d2, w3, x2, t3)


def fine_up(x2, lo2, pair, hi2, c1, wx, yx, xs, w1, work, out):
    f1, y1, xa, xb, f0, x0, x9 = work
    s = lax.axis_index("space")
    lane = iota((32, 128), 1)

    def blocks(start):
        mixed = [ref[pl.ds(start + 32, 32), :] for ref in (lo2, pair, hi2)]
        return (
            lo2[pl.ds(start, 32), :],
            jnp.where(lane < 64, mixed[0], mixed[1]),
            pair[pl.ds(start, 32), :],
            jnp.where(lane < 64, mixed[1], mixed[2]),
            hi2[pl.ds(start, 32), :],
        )

    if c1 is not None:
        for j, c in enumerate(blocks(64)):
            c1[j] = c
            z = s + (j - 2)
            w1[j] = jnp.where((z >= 0) & (z < SLABS), OMEGA / (c + 3.0), 0.0)
    for j, b in enumerate(blocks(0)):
        y1[j] = w1[j] * b
    zero = jnp.zeros((32, 128), F32)
    group = iota((16, 128), 1) >> 5
    parts = []
    for j in range(5):
        z = s + (j - 2)
        v = x2[pl.ds(pl.multiple_of((z & 7) * 16, 16), 16), :]
        parts.append(spread(jnp.where(group == (z >> 3), v, 0.0)))
    pick = picks(lambda i, j: i == ((j & 63) >> 1), 1.0)
    v = dot(jnp.concatenate(parts, 0), pick)
    f1[pl.ds(0, 80, stride=2), :] = v
    f1[pl.ds(1, 80, stride=2), :] = v
    for j in range(5):
        below = y1[j - 1] if j > 0 else zero
        above = y1[j + 1] if j < 4 else zero
        xa[j] = block_sweep(y1[j], w1[j], below, above) + f1[pl.ds(32 * j, 32), :]
    xb[0] = zero
    xb[4] = zero
    for old, new in ((xa, xb), (xb, xa)):
        for j in (1, 2, 3):
            c = old[j]
            t = around_block(c, old[j - 1], old[j + 1])
            new[j] = 0.2 * c + y1[j] + 0.5 * w1[j] * t
    one, two, three = xa[1], xa[2], xa[3]
    low = dot(jnp.concatenate([two, three], 0), picks(lambda i, j: i == (j >> 1), 1.0))
    high = dot(jnp.concatenate([one, two], 0), picks(lambda i, j: i == (j >> 1) + 64, 1.0))
    for q, v in enumerate((high[:32], low[:32], high[32:], low[32:])):
        f0[pl.ds(64 * q, 32, stride=2), :] = v
        f0[pl.ds(64 * q + 1, 32, stride=2), :] = v
    for i in range(8):
        x0[i] = xs[i] + f0[pl.ds(64 * (i // 2), 64), :]
    for i in range(6):
        c = x0[i + 1]
        x9[i] = 0.2 * c + yx[i] + wx[i] * around_plane(c, x0[i], x0[i + 2])
    for p in range(DEPTH):
        c = x9[p + 1]
        out(p, 0.2 * c + yx[p + 1] + wx[p + 1] * around_plane(c, x9[p], x9[p + 2]))


def first_up_body(
    x2, lo2, pair, hi2, wx, yx, xs, w, cap, src, u_out, y, x, block, up, dn, w1, send, *work
):
    b_out, c1, rs, *work = work

    def out(p, u):
        u_out[0, p] = u
        b_out[p] = cap[p] * u + src[0, 1, p]

    fine_up(x2, lo2, pair, hi2, c1, wx, yx, xs, w1, work, out)
    own = local_down(lambda p: b_out[p], cap, w, y, x, rs, *plane_picks(), False)
    wide_share(own, y, x, wx, w1, c1, send, rs)
    block[...] = own
    fill_edges(up, dn, y, x)
    up[pl.ds(192, 32), :] = own
    dn[pl.ds(192, 32), :] = own


def next_up_body(x2, lo2, pair, hi2, wx, yx, xs, w1, u_out, *work):
    def out(p, u):
        u_out[0, p] = u

    fine_up(x2, lo2, pair, hi2, None, wx, yx, xs, w1, work, out)


LOW_WORK = [(64, 128)]
LOW_FLOPS = 1 << 31
WORK = [
    (160, 128),
    (5, 32, 128),
    (5, 32, 128),
    (5, 32, 128),
    (256, 128),
    (8, NY, NX),
    (6, NY, NX),
]
EDGE_SUMS = (256, 128)
PLANE = (NY, NX)
PLANE4 = (DEPTH, NY, NX)
MESSAGE = f32(SLABS, 16, 128)
WIDE_MESSAGE = f32(SLABS, 24, 128)


def moved(x, spans, slabs):
    pairs = []
    for t in range(SPANS):
        for s in range(SLABS):
            pairs.append((t * SLABS + s, (t + spans) % SPANS * SLABS + (s + slabs) % SLABS))
    return lax.ppermute(x, ("tm", "space"), pairs)


def gathered(send):
    return lax.all_to_all(send, "space", 0, 0, tiled=True)


def near(pair):
    return moved(pair, 0, 2), pair, moved(pair, 0, -2)


def shards(u0, src, cap):
    slab = f32(*PLANE4)
    w, y, x, block, up, dn, cap_in = call(
        pack_body,
        (slab, slab, slab, f32(64, 128), f32(288, 128), f32(288, 128), slab),
        [PLANE4, PLANE4, EDGE_SUMS],
        *(pltpu.with_memory_space_constraint(v, pltpu.HBM) for v in (u0, src, cap)),
        space=pl.BlockSpec(memory_space=pltpu.HBM),
        sems=[pltpu.SemaphoreType.DMA((3,))],
    )
    lo, hi = moved(up, 0, 1), moved(dn, 0, -1)
    wx, yx, xs, pair, send = call(
        first_down_body,
        (f32(6, *PLANE), f32(6, *PLANE), f32(8, *PLANE), f32(128, 128), MESSAGE),
        [EDGE_SUMS],
        *(w, y, x, block, lo, hi),
    )
    got = gathered(send)
    w2, d2, w3, x2 = call(
        first_low_body,
        (f32(128, 128), f32(128, 128), f32(32, 128), f32(128, 128)),
        LOW_WORK,
        got,
        flops=LOW_FLOPS,
    )
    fpoint, y, x, block, up, dn, w1, send = call(
        first_up_body,
        (
            f32(1, *PLANE4),
            slab,
            slab,
            f32(32, 128),
            f32(224, 128),
            f32(224, 128),
            f32(5, 32, 128),
            WIDE_MESSAGE,
        ),
        [PLANE4, (5, 32, 128), EDGE_SUMS, *WORK],
        *(x2, *near(pair), wx, yx, xs, w, cap_in, src),
    )
    got = gathered(send)
    lo = moved(up, 0, 1)
    hi = moved(dn, 0, -1)
    yx, xs, pair = call(
        next_down_body,
        (f32(6, *PLANE), f32(8, *PLANE), f32(64, 128)),
        [EDGE_SUMS],
        *(y, x, block, lo, hi, w, wx),
    )
    (x2,) = call(
        next_low_body, (f32(128, 128),), LOW_WORK, *(got, w2, d2, w3, pair), flops=LOW_FLOPS
    )
    (u,) = call(next_up_body, (f32(1, *PLANE4),), WORK, *(x2, *near(pair), wx, yx, xs, w1))
    updated = jnp.where(lax.axis_index("tm") == 0, u0, moved(u, 1, 0))
    return fpoint, updated


def solution(mesh):
    in_specs = (
        P("tm", "space", None, None),
        P("tm", None, "space", None, None),
        P("space", None, None),
    )
    out_specs = (P("tm", "space", None, None), P("tm", "space", None, None))
    return jax.shard_map(shards, mesh=mesh, in_specs=in_specs, out_specs=out_specs, check_vma=False)
```

```python
import jax
import jax.numpy as jnp
from jax import lax
from jax.experimental import pallas as pl
from jax.experimental.pallas import tpu as pltpu
from jax.sharding import PartitionSpec as P


COARSE_SWEEPS = 24
NY, NX = 64, 128
SLABS = 32
SPANS = 8
DEPTH = 4
OMEGA = 0.8
F32 = jnp.float32
VMEM = pl.BlockSpec(memory_space=pltpu.VMEM)


def f32(*shape):
    return jax.ShapeDtypeStruct(shape, F32)


def call(body, outs, scratch, *args, space=VMEM, flops=None, sems=()):
    return pl.pallas_call(
        body,
        out_shape=outs,
        in_specs=[space] * len(args),
        out_specs=tuple(VMEM for _ in outs),
        scratch_shapes=[pltpu.VMEM(s, F32) for s in scratch] + list(sems),
        compiler_params=pltpu.CompilerParams(vmem_limit_bytes=16 << 20),
        cost_estimate=flops and pl.CostEstimate(flops=flops, transcendentals=0, bytes_accessed=0),
    )(*args)


def lanes_of(v, lane):
    return jnp.take_along_axis(v, lane, axis=1, mode="promise_in_bounds")


def iota(shape, axis):
    return lax.broadcasted_iota(jnp.int32, shape, axis)


def halves(low, high):
    lane = iota(low.shape, 1)
    at = (lane & 63) * 2
    low = lanes_of(low, at) + lanes_of(low, at + 1)
    high = lanes_of(high, at) + lanes_of(high, at + 1)
    return 0.125 * jnp.where(lane < 64, low, high)


def quarters(v):
    at = (iota(v.shape, 1) & 31) * 2
    low = lanes_of(v, at) + lanes_of(v, at + 1)
    return 0.125 * (low + (lanes_of(v, at + 64) + lanes_of(v, at + 65)))


def inside_plane(c):
    row, lane = iota(c.shape, 0), iota(c.shape, 1)
    total = jnp.where(lane > 0, pltpu.roll(c, 1, 1), 0.0)
    total = total + jnp.where(lane < NX - 1, pltpu.roll(c, NX - 1, 1), 0.0)
    total = total + jnp.where(row > 0, pltpu.roll(c, 1, 0), 0.0)
    return total + jnp.where(row < NY - 1, pltpu.roll(c, NY - 1, 0), 0.0)


def around_plane(c, below, above):
    return inside_plane(c) + (below + above)


def around_block(c, below, above):
    row, lane = iota(c.shape, 0), iota(c.shape, 1)
    col = lane & 63
    total = pltpu.roll(c + jnp.where(lane < 64, above, below), 64, 1)
    total = total + jnp.where(col > 0, pltpu.roll(c, 1, 1), 0.0)
    total = total + jnp.where(col < 63, pltpu.roll(c, 127, 1), 0.0)
    total = total + jnp.where(row > 0, pltpu.roll(c, 1, 0), 0.0)
    return total + jnp.where(row < 31, pltpu.roll(c, 31, 0), 0.0)


def around_low(v):
    row, lane = iota(v.shape, 0), iota(v.shape, 1)
    y, x = row & 15, lane & 31
    ends = iota((16, 128), 1)
    below = jnp.where(ends >= 32, pltpu.roll(v[112:], 32, 1), 0.0)
    above = jnp.where(ends < 96, pltpu.roll(v[:16], 96, 1), 0.0)
    total = jnp.concatenate([below, v[:112]], 0) + jnp.concatenate([v[16:], above], 0)
    total = total + jnp.where(x > 0, pltpu.roll(v, 1, 1), 0.0)
    total = total + jnp.where(x < 31, pltpu.roll(v, 127, 1), 0.0)
    total = total + jnp.where(y > 0, pltpu.roll(v, 1, 0), 0.0)
    return total + jnp.where(y < 15, pltpu.roll(v, 127, 0), 0.0)


def rolled(v, k, j):
    return pltpu.roll(v[k % 4], (2 * j - 32 * (k // 4)) % 128, 1) if (k // 4 or j) else v[k]


CENTRE = [(k, 0) for k in range(4)]
FIRST = [(k, j) for k in range(4) for j in (-1, 0, 1)] + [(-1, 0), (4, 0)]


def coarsest(b3, w3):
    lane, row = iota((8, 128), 1), iota((8, 128), 0)
    x = (lane & 31) >> 1
    base, own = [], []
    for k in range(4):
        w = w3[8 * k : 8 * k + 8]
        wh = 0.125 * w
        own.append(w * b3[8 * k : 8 * k + 8])
        base.append(
            (
                jnp.where(lane >= 32, wh, 0.0) if k == 0 else wh,
                jnp.where(lane < 96, wh, 0.0) if k == 3 else wh,
                jnp.where(x > 0, wh, 0.0),
                jnp.where(x < 15, wh, 0.0),
                jnp.where(row > 0, wh, 0.0),
                jnp.where(row < 7, wh, 0.0),
            )
        )
    terms = list(zip(*base))
    steps = {
        (k, j): (rolled(own, k, j), *(rolled(t, k, j) for t in terms)) for k, j in FIRST
    }

    def sweep(v, k, j):
        wb, below, above, left, right, up, down = steps[k, j]
        c = v[k, j]
        t = (0.2 * c + wb) + (below * v[k - 1, j] + above * v[k + 1, j])
        s = up * pltpu.roll(c, 1, 0) + down * pltpu.roll(c, 7, 0)
        return (t + s) + (left * v[k, j + 1] + right * v[k, j - 1])

    def copies(v, reach):
        return {
            (k, j): rolled(v, k, j)
            for k in range(-reach, 4 + reach)
            for j in range(-reach, reach + 1)
            if max(0, -k, k - 3) + abs(j) <= reach
        }

    def one(v):
        v = copies(v, 1)
        return [sweep(v, k, j) for k, j in CENTRE]

    def two(_, v):
        v = copies(v, 2)
        v = {(k, j): sweep(v, k, j) for k, j in FIRST}
        return tuple(sweep(v, k, j) for k, j in CENTRE)

    pairs, rest = divmod(COARSE_SWEEPS - 1, 2)
    v = one(own) if rest else own
    v = lax.fori_loop(0, pairs, two, tuple(v), unroll=True)
    return jnp.concatenate(v, 0)


def row_pairs(ref, start, count):
    return ref[pl.ds(start, count, stride=2), :] + ref[pl.ds(start + 1, count, stride=2), :]


def block_sweep(y, w, below, above):
    return 1.2 * y + 0.5 * w * around_block(y, below, above)


def local_down(b, cap, w, y, x, rs, first):
    for p in range(DEPTH):
        y[p] = w[p] * b(p)
    zero = jnp.zeros((NY, NX), F32)
    for p in range(DEPTH):
        below = y[p - 1] if p > 0 else zero
        above = y[p + 1] if p < 3 else zero
        x[p] = 1.2 * y[p] + w[p] * around_plane(y[p], below, above)
    for half in range(2):
        total = None
        for p in (2 * half, 2 * half + 1):
            below = x[p - 1] if p > 0 else zero
            above = x[p + 1] if p < 3 else zero
            r = b(p) - (cap[p] + 6.0) * x[p] + around_plane(x[p], below, above)
            total = r if total is None else total + r
        rs[pl.ds(64 * half, 64), :] = total
        if first:
            rs[pl.ds(128 + 64 * half, 64), :] = cap[2 * half] + cap[2 * half + 1]
    low, high = row_pairs(rs, 0, 32), row_pairs(rs, 64, 32)
    if first:
        low = jnp.concatenate([low, row_pairs(rs, 128, 32)], 0)
        high = jnp.concatenate([high, row_pairs(rs, 192, 32)], 0)
    return halves(low, high)


def fill_edges(up, dn, y, x):
    for edge, p, q in ((up, 3, 2), (dn, 0, 1)):
        edge[pl.ds(0, 64), :] = y[p]
        edge[pl.ds(64, 64), :] = x[p]
        edge[pl.ds(128, 64), :] = x[q]


def pack_body(u, src, cap, w, y, x, block, up, dn, cap_out, u_in, src_in, rs, sems):
    copies = [
        pltpu.make_async_copy(cap, cap_out, sems.at[0]),
        pltpu.make_async_copy(u.at[0], u_in, sems.at[1]),
        pltpu.make_async_copy(src.at[0, 0], src_in, sems.at[2]),
    ]
    for copy in copies:
        copy.start()
    for copy in copies:
        copy.wait()
    for p in range(DEPTH):
        w[p] = OMEGA / (cap_out[p] + 6.0)
        u_in[p] = cap_out[p] * u_in[p] + src_in[p]
    blocks = local_down(lambda p: u_in[p], cap_out, w, y, x, rs, True)
    block[...] = blocks
    fill_edges(up, dn, y, x)
    lane = iota((32, 128), 1)
    b1, c1 = blocks[:32], blocks[32:]
    up[pl.ds(192, 32), :] = jnp.where(lane < 64, pltpu.roll(b1, 64, 1), c1)
    dn[pl.ds(192, 32), :] = jnp.where(lane < 64, b1, pltpu.roll(c1, 64, 1))
    up[pl.ds(224, 64), :] = w[3]
    dn[pl.ds(224, 64), :] = w[0]


def finish_down(first, w, y, x, b1, c1, lo, hi, wx, yx, xs, pair, rs):
    s = lax.axis_index("space")
    lane = iota((32, 128), 1)

    def edge(ref, there):
        return [
            jnp.where(there, ref[pl.ds(start, 64), :], 0.0)
            for start in ((0, 64, 128, 224) if first else (0, 64, 128))
        ]

    sides = []
    for ref, there, i, p in ((lo, s > 0, 0, 0), (hi, s < SLABS - 1, 5, 3)):
        ye, xe, xs_far, *we = edge(ref, there)
        if first:
            wx[i] = we[0]
        yx[i] = ye
        near = w[p] * ye
        far = wx[i] * y[p]
        x_near, x_far = x[p] + near, xe + far
        j = 1 if p == 0 else 6
        xs[j] = x_far
        xs[0 if p == 0 else 7] = xs_far
        xs[p + 2] = x_near
        own = (near - OMEGA * ye) + inside_plane(near) + x_far
        beside = (far - OMEGA * y[p]) + inside_plane(far) + x_near
        sides.append((own, jnp.where(there, beside, 0.0)))
    for p in range(DEPTH):
        yx[p + 1] = y[p]
        if first:
            wx[p + 1] = w[p]
    xs[3] = x[1]
    xs[4] = x[2]
    for k, v in enumerate((sides[0][0], sides[1][1], sides[1][0], sides[0][1])):
        rs[pl.ds(64 * k, 64), :] = v
    low = jnp.concatenate([row_pairs(rs, 0, 32), row_pairs(rs, 64, 32)], 0)
    high = jnp.concatenate([row_pairs(rs, 128, 32), row_pairs(rs, 192, 32)], 0)
    terms = halves(low, high)
    lo_block, hi_block = lo[pl.ds(192, 32), :], hi[pl.ds(192, 32), :]
    if first:
        pair[pl.ds(64, 32), :] = c1
        pair[pl.ds(96, 32), :] = jnp.where(lane < 64, pltpu.roll(hi_block, 64, 1), lo_block)
        lo_block = pltpu.roll(lo_block, 64, 1)
    own = b1 + terms[:32]
    pair[pl.ds(0, 32), :] = own
    pair[pl.ds(32, 32), :] = jnp.where(lane < 64, hi_block, lo_block) + terms[32:]
    return own


def share(b1, c1, c_mix, send, rs):
    s = lax.axis_index("space")
    lane = iota((32, 128), 1)
    zero = jnp.zeros((32, 128), F32)
    own, beside = c1 + 3.0, c_mix + 3.0
    w_own, w_mix = OMEGA / own, OMEGA / beside
    y = w_own * b1
    x = [
        block_sweep(zero, jnp.where((lane >= 64) & (s > 0), w_mix, 0.0), zero, y),
        block_sweep(y, w_own, zero, zero),
        block_sweep(zero, jnp.where((lane < 64) & (s < SLABS - 1), w_mix, 0.0), y, zero),
    ]
    r = [
        0.5 * around_block(x[0], zero, x[1]) - beside * x[0],
        b1 - own * x[1] + 0.5 * around_block(x[1], x[0], x[2]),
        0.5 * around_block(x[2], x[1], zero) - beside * x[2],
        c1,
    ]
    for k in range(4):
        rs[pl.ds(32 * k, 32), :] = r[k]
    low = quarters(row_pairs(rs, 0, 64))
    group = iota((16, 128), 1) >> 5
    message = low[48:]
    for k in range(3):
        message = jnp.where(group == k, low[16 * k : 16 * k + 16], message)
    for peer in range(SLABS):
        send[peer] = message


def first_down_body(w, y, x, block, lo, hi, wx, yx, xs, pair, send, rs):
    b1, c1 = block[pl.ds(0, 32), :], block[pl.ds(32, 32), :]
    own = finish_down(True, w, y, x, b1, c1, lo, hi, wx, yx, xs, pair, rs)
    share(own, c1, pair[pl.ds(96, 32), :], send, rs)


def next_down_body(y, x, block, lo, hi, w, wx, yx, xs, pair, rs):
    finish_down(False, w, y, x, block[...], None, lo, hi, wx, yx, xs, pair, rs)


def wide_share(block, y, x, wx, w1, c1, send, rs):
    lane = iota((32, 128), 1)
    zero = jnp.zeros((32, 128), F32)
    for k, (i, p) in enumerate(((0, 0), (5, 3))):
        far = wx[i] * y[p]
        rs[pl.ds(64 * k, 64), :] = far
        rs[pl.ds(128 + 64 * k, 64), :] = (far - OMEGA * y[p]) + inside_plane(far) + x[p]
    low = jnp.concatenate([row_pairs(rs, 0, 32), row_pairs(rs, 192, 32)], 0)
    high = jnp.concatenate([row_pairs(rs, 64, 32), row_pairs(rs, 128, 32)], 0)
    terms = halves(low, high)
    mix = terms[32:]
    b = [jnp.where(lane >= 64, mix, 0.0), block + terms[:32], jnp.where(lane < 64, mix, 0.0)]
    v = [zero] + [w1[j + 1] * b[j] for j in range(3)] + [zero]
    v = [zero] + [block_sweep(v[j], w1[j], v[j - 1], v[j + 1]) for j in (1, 2, 3)] + [zero]
    r = [0.5 * around_block(zero, zero, v[1])]
    for j in (1, 2, 3):
        r.append(b[j - 1] - (c1[j] + 3.0) * v[j] + 0.5 * around_block(v[j], v[j - 1], v[j + 1]))
    r.append(0.5 * around_block(zero, v[3], zero))
    for k in range(5):
        rs[pl.ds(32 * k, 32), :] = r[k]
    low = quarters(row_pairs(rs, 0, 80))
    group = iota((16, 128), 1) >> 5
    message = low[:16]
    for k in (1, 2, 3):
        message = jnp.where(group == k, low[16 * k : 16 * k + 16], message)
    pieces = [message[4 * k : 4 * k + 4] for k in range(4)]
    last = low[64:68]
    for k in (1, 2, 3):
        last = jnp.where(group[:4] == k, low[64 + 4 * k : 68 + 4 * k], last)
    pieces.append(last)
    for peer in range(SLABS):
        for k in range(5):
            send[5 * peer + k] = pieces[k]


def spread(v):
    v = v + pltpu.roll(v, 64, 1)
    return v + pltpu.roll(v, 32, 1)


def to_coarsest(v, t3):
    for k in range(4):
        t3[pl.ds(16 * k, 16), :] = v[32 * k : 32 * k + 16] + v[32 * k + 16 : 32 * k + 32]
    v = row_pairs(t3, 0, 32)
    return 0.125 * (v + pltpu.roll(v, 127, 1))


def from_coarsest(v, t3):
    v = jnp.where((iota(v.shape, 1) & 1) == 0, v, 0.0)
    v = v + pltpu.roll(v, 1, 1)
    t3[pl.ds(0, 32, stride=2), :] = v
    t3[pl.ds(1, 32, stride=2), :] = v
    parts = []
    for k in range(4):
        block = t3[pl.ds(16 * k, 16), :]
        parts += [block, block]
    return jnp.concatenate(parts, 0)


def low_levels(first, got, w2, d2, w3, x2, t3, joined=None):
    group = iota((16, 128), 1) >> 5
    quarter = iota((16, 128), 0) >> 2
    if not first:
        for z in range(SLABS):
            for k in range(4):
                joined[z, pl.ds(4 * k, 4), :] = got[5 * z + k]
                joined[z, pl.ds(16 + 4 * k, 4), :] = got[5 * z + 4]
    rows = got if first else joined
    reach = 1 if first else 2
    parts, caps = [], []
    for zl in range(8):
        total, cap = None, None
        for zh in range(4):
            z = 8 * zh + zl
            v = jnp.zeros((16, 128), F32)
            for k in range(3 if first else 4):
                if 0 <= z + reach - k < SLABS:
                    v = jnp.where(group == k, rows[z + reach - k, pl.ds(0, 16), :], v)
            if not first and z >= 2:
                v = v + jnp.where(group == quarter, rows[z - 2, pl.ds(16, 16), :], 0.0)
            v = spread(v)
            total = v if total is None else jnp.where(group == zh, v, total)
            if first:
                v = spread(jnp.where(group == 3, got[z], 0.0))
                cap = v if cap is None else jnp.where(group == zh, v, cap)
        parts.append(total)
        caps.append(cap)
    b = jnp.concatenate(parts, 0)
    if first:
        c2 = jnp.concatenate(caps, 0)
        d2[...] = c2 + 1.5
        w2[...] = OMEGA / (c2 + 1.5)
        w3[...] = OMEGA / (to_coarsest(c2, t3) + 0.75)
    w, d = w2[...], d2[...]
    y = w * b
    x = 1.2 * y + 0.25 * w * around_low(y)
    r = b - d * x + 0.25 * around_low(x)
    x = x + from_coarsest(coarsest(to_coarsest(r, t3), w3[...]), t3)
    for _ in range(2):
        x = 0.2 * x + y + 0.25 * w * around_low(x)
    x2[...] = x


def first_low_body(got, w2, d2, w3, x2, t3):
    low_levels(True, got, w2, d2, w3, x2, t3)


def next_low_body(got, w2, d2, w3, after, x2, t3, joined):
    low_levels(False, got, w2, d2, w3, x2, t3, joined)


def fine_up(x2, lo2, pair, hi2, c1, wx, yx, xs, w1, work, out):
    f1, y1, xa, xb, f0, x0, x9 = work
    s = lax.axis_index("space")
    lane = iota((32, 128), 1)

    def blocks(start):
        mixed = [ref[pl.ds(start + 32, 32), :] for ref in (lo2, pair, hi2)]
        return (
            lo2[pl.ds(start, 32), :],
            jnp.where(lane < 64, mixed[0], mixed[1]),
            pair[pl.ds(start, 32), :],
            jnp.where(lane < 64, mixed[1], mixed[2]),
            hi2[pl.ds(start, 32), :],
        )

    if c1 is not None:
        for j, c in enumerate(blocks(64)):
            c1[j] = c
            z = s + (j - 2)
            w1[j] = jnp.where((z >= 0) & (z < SLABS), OMEGA / (c + 3.0), 0.0)
    for j, b in enumerate(blocks(0)):
        y1[j] = w1[j] * b
    zero = jnp.zeros((32, 128), F32)
    lane = iota((16, 128), 1)
    for j in range(5):
        z = s + (j - 2)
        v = x2[pl.ds(pl.multiple_of((z & 7) * 16, 16), 16), :]
        v = lanes_of(v, ((lane & 63) >> 1) + ((z >> 3) & 3) * 32)
        v = jnp.where((z >= 0) & (z < SLABS), v, 0.0)
        f1[pl.ds(32 * j, 16, stride=2), :] = v
        f1[pl.ds(32 * j + 1, 16, stride=2), :] = v
    for j in range(5):
        below = y1[j - 1] if j > 0 else zero
        above = y1[j + 1] if j < 4 else zero
        xa[j] = block_sweep(y1[j], w1[j], below, above) + f1[pl.ds(32 * j, 32), :]
    xb[0] = zero
    xb[4] = zero
    for old, new in ((xa, xb), (xb, xa)):
        for j in (1, 2, 3):
            c = old[j]
            t = around_block(c, old[j - 1], old[j + 1])
            new[j] = 0.2 * c + y1[j] + 0.5 * w1[j] * t
    one, two, three = xa[1], xa[2], xa[3]
    half = iota((32, 128), 1) >> 1
    wide = (
        lanes_of(one, half + 64),
        lanes_of(two, half),
        lanes_of(two, half + 64),
        lanes_of(three, half),
    )
    for q, v in enumerate(wide):
        f0[pl.ds(64 * q, 32, stride=2), :] = v
        f0[pl.ds(64 * q + 1, 32, stride=2), :] = v
    for i in range(8):
        x0[i] = xs[i] + f0[pl.ds(64 * (i // 2), 64), :]
    for i in range(6):
        c = x0[i + 1]
        x9[i] = 0.2 * c + yx[i] + wx[i] * around_plane(c, x0[i], x0[i + 2])
    for p in range(DEPTH):
        c = x9[p + 1]
        out(p, 0.2 * c + yx[p + 1] + wx[p + 1] * around_plane(c, x9[p], x9[p + 2]))


def first_up_body(
    x2, lo2, pair, hi2, wx, yx, xs, w, cap, src, u_out, y, x, block, up, dn, w1, send, *work
):
    b_out, c1, rs, *work = work

    def out(p, u):
        u_out[0, p] = u
        b_out[p] = cap[p] * u + src[0, 1, p]

    fine_up(x2, lo2, pair, hi2, c1, wx, yx, xs, w1, work, out)
    own = local_down(lambda p: b_out[p], cap, w, y, x, rs, False)
    wide_share(own, y, x, wx, w1, c1, send, rs)
    block[...] = own
    fill_edges(up, dn, y, x)
    up[pl.ds(192, 32), :] = own
    dn[pl.ds(192, 32), :] = own


def next_up_body(x2, lo2, pair, hi2, wx, yx, xs, w1, u_out, *work):
    def out(p, u):
        u_out[0, p] = u

    fine_up(x2, lo2, pair, hi2, None, wx, yx, xs, w1, work, out)


LOW_WORK = [(64, 128)]
LOW_FLOPS = 1 << 31
WORK = [
    (160, 128),
    (5, 32, 128),
    (5, 32, 128),
    (5, 32, 128),
    (256, 128),
    (8, NY, NX),
    (6, NY, NX),
]
EDGE_SUMS = (256, 128)
PLANE = (NY, NX)
PLANE4 = (DEPTH, NY, NX)
MESSAGE = f32(SLABS, 16, 128)
WIDE_MESSAGE = f32(SLABS * 5, 4, 128)


def moved(x, spans, slabs):
    pairs = []
    for t in range(SPANS):
        for s in range(SLABS):
            pairs.append((t * SLABS + s, (t + spans) % SPANS * SLABS + (s + slabs) % SLABS))
    return lax.ppermute(x, ("tm", "space"), pairs)


def gathered(send):
    return lax.all_to_all(send, "space", 0, 0, tiled=True)


def near(pair):
    return moved(pair, 0, 2), pair, moved(pair, 0, -2)


def shards(u0, src, cap):
    slab = f32(*PLANE4)
    w, y, x, block, up, dn, cap_in = call(
        pack_body,
        (slab, slab, slab, f32(64, 128), f32(288, 128), f32(288, 128), slab),
        [PLANE4, PLANE4, EDGE_SUMS],
        *(pltpu.with_memory_space_constraint(v, pltpu.HBM) for v in (u0, src, cap)),
        space=pl.BlockSpec(memory_space=pltpu.HBM),
        sems=[pltpu.SemaphoreType.DMA((3,))],
    )
    lo, hi = moved(up, 0, 1), moved(dn, 0, -1)
    wx, yx, xs, pair, send = call(
        first_down_body,
        (f32(6, *PLANE), f32(6, *PLANE), f32(8, *PLANE), f32(128, 128), MESSAGE),
        [EDGE_SUMS],
        *(w, y, x, block, lo, hi),
    )
    got = gathered(send)
    w2, d2, w3, x2 = call(
        first_low_body,
        (f32(128, 128), f32(128, 128), f32(32, 128), f32(128, 128)),
        LOW_WORK,
        got,
        flops=LOW_FLOPS,
    )
    fpoint, y, x, block, up, dn, w1, send = call(
        first_up_body,
        (
            f32(1, *PLANE4),
            slab,
            slab,
            f32(32, 128),
            f32(224, 128),
            f32(224, 128),
            f32(5, 32, 128),
            WIDE_MESSAGE,
        ),
        [PLANE4, (5, 32, 128), EDGE_SUMS, *WORK],
        *(x2, *near(pair), wx, yx, xs, w, cap_in, src),
    )
    got = gathered(send)
    lo = moved(up, 0, 1)
    hi = moved(dn, 0, -1)
    yx, xs, pair = call(
        next_down_body,
        (f32(6, *PLANE), f32(8, *PLANE), f32(64, 128)),
        [EDGE_SUMS],
        *(y, x, block, lo, hi, w, wx),
    )
    (x2,) = call(
        next_low_body,
        (f32(128, 128),),
        [*LOW_WORK, (SLABS, 32, 128)],
        *(got, w2, d2, w3, pair),
        flops=LOW_FLOPS,
    )
    (u,) = call(next_up_body, (f32(1, *PLANE4),), WORK, *(x2, *near(pair), wx, yx, xs, w1))
    updated = jnp.where(lax.axis_index("tm") == 0, u0, moved(u, 1, 0))
    return fpoint, updated


def solution(mesh):
    in_specs = (
        P("tm", "space", None, None),
        P("tm", None, "space", None, None),
        P("space", None, None),
    )
    out_specs = (P("tm", "space", None, None), P("tm", "space", None, None))
    return jax.shard_map(shards, mesh=mesh, in_specs=in_specs, out_specs=out_specs, check_vma=False)
```

```python
import jax
import jax.numpy as jnp
from jax import lax
from jax.experimental import pallas as pl
from jax.experimental.pallas import tpu as pltpu
from jax.sharding import PartitionSpec as P


COARSE_SWEEPS = 24
NY, NX = 64, 128
SLABS = 32
SPANS = 8
DEPTH = 4
OMEGA = 0.8
F32 = jnp.float32
VMEM = pl.BlockSpec(memory_space=pltpu.VMEM)


def f32(*shape):
    return jax.ShapeDtypeStruct(shape, F32)


def call(body, outs, scratch, *args, space=VMEM, flops=None, sems=()):
    return pl.pallas_call(
        body,
        out_shape=outs,
        in_specs=[space] * len(args),
        out_specs=tuple(VMEM for _ in outs),
        scratch_shapes=[pltpu.VMEM(s, F32) for s in scratch] + list(sems),
        compiler_params=pltpu.CompilerParams(vmem_limit_bytes=16 << 20),
        cost_estimate=flops and pl.CostEstimate(flops=flops, transcendentals=0, bytes_accessed=0),
    )(*args)


def lanes_of(v, lane):
    return jnp.take_along_axis(v, lane, axis=1, mode="promise_in_bounds")


def iota(shape, axis):
    return lax.broadcasted_iota(jnp.int32, shape, axis)


def halves(low, high):
    lane = iota(low.shape, 1)
    at = (lane & 63) * 2
    low = lanes_of(low, at) + lanes_of(low, at + 1)
    high = lanes_of(high, at) + lanes_of(high, at + 1)
    return 0.125 * jnp.where(lane < 64, low, high)


def quarters(v):
    at = (iota(v.shape, 1) & 31) * 2
    low = lanes_of(v, at) + lanes_of(v, at + 1)
    return 0.125 * (low + (lanes_of(v, at + 64) + lanes_of(v, at + 65)))


def inside_plane(c):
    row, lane = iota(c.shape, 0), iota(c.shape, 1)
    total = jnp.where(lane > 0, pltpu.roll(c, 1, 1), 0.0)
    total = total + jnp.where(lane < NX - 1, pltpu.roll(c, NX - 1, 1), 0.0)
    total = total + jnp.where(row > 0, pltpu.roll(c, 1, 0), 0.0)
    return total + jnp.where(row < NY - 1, pltpu.roll(c, NY - 1, 0), 0.0)


def around_plane(c, below, above):
    return inside_plane(c) + (below + above)


def around_block(c, below, above):
    row, lane = iota(c.shape, 0), iota(c.shape, 1)
    col = lane & 63
    total = pltpu.roll(c + jnp.where(lane < 64, above, below), 64, 1)
    total = total + jnp.where(col > 0, pltpu.roll(c, 1, 1), 0.0)
    total = total + jnp.where(col < 63, pltpu.roll(c, 127, 1), 0.0)
    total = total + jnp.where(row > 0, pltpu.roll(c, 1, 0), 0.0)
    return total + jnp.where(row < 31, pltpu.roll(c, 31, 0), 0.0)


def around_low(v):
    row, lane = iota(v.shape, 0), iota(v.shape, 1)
    y, x = row & 15, lane & 31
    ends = iota((16, 128), 1)
    below = jnp.where(ends >= 32, pltpu.roll(v[112:], 32, 1), 0.0)
    above = jnp.where(ends < 96, pltpu.roll(v[:16], 96, 1), 0.0)
    total = jnp.concatenate([below, v[:112]], 0) + jnp.concatenate([v[16:], above], 0)
    total = total + jnp.where(x > 0, pltpu.roll(v, 1, 1), 0.0)
    total = total + jnp.where(x < 31, pltpu.roll(v, 127, 1), 0.0)
    total = total + jnp.where(y > 0, pltpu.roll(v, 1, 0), 0.0)
    return total + jnp.where(y < 15, pltpu.roll(v, 127, 0), 0.0)


def rolled(v, k, j):
    return pltpu.roll(v[k % 2], (j - 16 * (k // 2)) % 128, 1) if (k // 2 or j) else v[k]


CENTRE = [(k, 0) for k in range(2)]
FIRST = [(k, j) for k in range(2) for j in (-1, 0, 1)] + [(-1, 0), (2, 0)]


def coarsest(b3, w3):
    lane, row = iota((8, 128), 1), iota((8, 128), 0)
    x = lane & 15
    base, own = [], []
    for k in range(2):
        w = w3[8 * k : 8 * k + 8]
        wh = 0.125 * w
        own.append(w * b3[8 * k : 8 * k + 8])
        base.append(
            (
                jnp.where(lane >= 16, wh, 0.0) if k == 0 else wh,
                jnp.where(lane < 112, wh, 0.0) if k == 1 else wh,
                jnp.where(x > 0, wh, 0.0),
                jnp.where(x < 15, wh, 0.0),
                jnp.where(row > 0, wh, 0.0),
                jnp.where(row < 7, wh, 0.0),
            )
        )
    terms = list(zip(*base))
    steps = {
        (k, j): (rolled(own, k, j), *(rolled(t, k, j) for t in terms)) for k, j in FIRST
    }

    def sweep(v, k, j):
        wb, below, above, left, right, up, down = steps[k, j]
        c = v[k, j]
        t = (0.2 * c + wb) + (below * v[k - 1, j] + above * v[k + 1, j])
        s = up * pltpu.roll(c, 1, 0) + down * pltpu.roll(c, 7, 0)
        return (t + s) + (left * v[k, j + 1] + right * v[k, j - 1])

    def copies(v, reach):
        return {
            (k, j): rolled(v, k, j)
            for k in range(-reach, 2 + reach)
            for j in range(-reach, reach + 1)
            if max(0, -k, k - 1) + abs(j) <= reach
        }

    def one(v):
        v = copies(v, 1)
        return [sweep(v, k, j) for k, j in CENTRE]

    def two(_, v):
        v = copies(v, 2)
        v = {(k, j): sweep(v, k, j) for k, j in FIRST}
        return tuple(sweep(v, k, j) for k, j in CENTRE)

    pairs, rest = divmod(COARSE_SWEEPS - 1, 2)
    v = one(own) if rest else own
    v = lax.fori_loop(0, pairs, two, tuple(v), unroll=True)
    return jnp.concatenate(v, 0)


def row_pairs(ref, start, count):
    return ref[pl.ds(start, count, stride=2), :] + ref[pl.ds(start + 1, count, stride=2), :]


def block_sweep(y, w, below, above):
    return 1.2 * y + 0.5 * w * around_block(y, below, above)


def local_down(b, cap, w, y, x, rs, first):
    for p in range(DEPTH):
        y[p] = w[p] * b(p)
    zero = jnp.zeros((NY, NX), F32)
    for p in range(DEPTH):
        below = y[p - 1] if p > 0 else zero
        above = y[p + 1] if p < 3 else zero
        x[p] = 1.2 * y[p] + w[p] * around_plane(y[p], below, above)
    for half in range(2):
        total = None
        for p in (2 * half, 2 * half + 1):
            below = x[p - 1] if p > 0 else zero
            above = x[p + 1] if p < 3 else zero
            r = b(p) - (cap[p] + 6.0) * x[p] + around_plane(x[p], below, above)
            total = r if total is None else total + r
        rs[pl.ds(64 * half, 64), :] = total
        if first:
            rs[pl.ds(128 + 64 * half, 64), :] = cap[2 * half] + cap[2 * half + 1]
    low, high = row_pairs(rs, 0, 32), row_pairs(rs, 64, 32)
    if first:
        low = jnp.concatenate([low, row_pairs(rs, 128, 32)], 0)
        high = jnp.concatenate([high, row_pairs(rs, 192, 32)], 0)
    return halves(low, high)


def fill_edges(up, dn, y, x):
    for edge, p, q in ((up, 3, 2), (dn, 0, 1)):
        edge[pl.ds(0, 64), :] = y[p]
        edge[pl.ds(64, 64), :] = x[p]
        edge[pl.ds(128, 64), :] = x[q]


def pack_body(u, src, cap, w, y, x, block, up, dn, cap_out, u_in, src_in, rs, sems):
    copies = [
        pltpu.make_async_copy(cap, cap_out, sems.at[0]),
        pltpu.make_async_copy(u.at[0], u_in, sems.at[1]),
        pltpu.make_async_copy(src.at[0, 0], src_in, sems.at[2]),
    ]
    for copy in copies:
        copy.start()
    for copy in copies:
        copy.wait()
    for p in range(DEPTH):
        w[p] = OMEGA / (cap_out[p] + 6.0)
        u_in[p] = cap_out[p] * u_in[p] + src_in[p]
    blocks = local_down(lambda p: u_in[p], cap_out, w, y, x, rs, True)
    block[...] = blocks
    fill_edges(up, dn, y, x)
    lane = iota((32, 128), 1)
    b1, c1 = blocks[:32], blocks[32:]
    up[pl.ds(192, 32), :] = jnp.where(lane < 64, pltpu.roll(b1, 64, 1), c1)
    dn[pl.ds(192, 32), :] = jnp.where(lane < 64, b1, pltpu.roll(c1, 64, 1))
    up[pl.ds(224, 64), :] = w[3]
    dn[pl.ds(224, 64), :] = w[0]


def finish_down(first, w, y, x, b1, c1, lo, hi, wx, yx, xs, pair, rs):
    s = lax.axis_index("space")
    lane = iota((32, 128), 1)

    def edge(ref, there):
        return [
            jnp.where(there, ref[pl.ds(start, 64), :], 0.0)
            for start in ((0, 64, 128, 224) if first else (0, 64, 128))
        ]

    sides = []
    for ref, there, i, p in ((lo, s > 0, 0, 0), (hi, s < SLABS - 1, 5, 3)):
        ye, xe, xs_far, *we = edge(ref, there)
        if first:
            wx[i] = we[0]
        yx[i] = ye
        near = w[p] * ye
        far = wx[i] * y[p]
        x_near, x_far = x[p] + near, xe + far
        j = 1 if p == 0 else 6
        xs[j] = x_far
        xs[0 if p == 0 else 7] = xs_far
        xs[p + 2] = x_near
        own = (near - OMEGA * ye) + inside_plane(near) + x_far
        beside = (far - OMEGA * y[p]) + inside_plane(far) + x_near
        sides.append((own, jnp.where(there, beside, 0.0)))
    for p in range(DEPTH):
        yx[p + 1] = y[p]
        if first:
            wx[p + 1] = w[p]
    xs[3] = x[1]
    xs[4] = x[2]
    for k, v in enumerate((sides[0][0], sides[1][1], sides[1][0], sides[0][1])):
        rs[pl.ds(64 * k, 64), :] = v
    low = jnp.concatenate([row_pairs(rs, 0, 32), row_pairs(rs, 64, 32)], 0)
    high = jnp.concatenate([row_pairs(rs, 128, 32), row_pairs(rs, 192, 32)], 0)
    terms = halves(low, high)
    lo_block, hi_block = lo[pl.ds(192, 32), :], hi[pl.ds(192, 32), :]
    if first:
        pair[pl.ds(64, 32), :] = c1
        pair[pl.ds(96, 32), :] = jnp.where(lane < 64, pltpu.roll(hi_block, 64, 1), lo_block)
        lo_block = pltpu.roll(lo_block, 64, 1)
    own = b1 + terms[:32]
    pair[pl.ds(0, 32), :] = own
    pair[pl.ds(32, 32), :] = jnp.where(lane < 64, hi_block, lo_block) + terms[32:]
    return own


def share(b1, c1, c_mix, send, rs):
    s = lax.axis_index("space")
    lane = iota((32, 128), 1)
    zero = jnp.zeros((32, 128), F32)
    own, beside = c1 + 3.0, c_mix + 3.0
    w_own, w_mix = OMEGA / own, OMEGA / beside
    y = w_own * b1
    x = [
        block_sweep(zero, jnp.where((lane >= 64) & (s > 0), w_mix, 0.0), zero, y),
        block_sweep(y, w_own, zero, zero),
        block_sweep(zero, jnp.where((lane < 64) & (s < SLABS - 1), w_mix, 0.0), y, zero),
    ]
    r = [
        0.5 * around_block(x[0], zero, x[1]) - beside * x[0],
        b1 - own * x[1] + 0.5 * around_block(x[1], x[0], x[2]),
        0.5 * around_block(x[2], x[1], zero) - beside * x[2],
        c1,
    ]
    for k in range(4):
        rs[pl.ds(32 * k, 32), :] = r[k]
    low = quarters(row_pairs(rs, 0, 64))
    group = iota((16, 128), 1) >> 5
    message = low[48:]
    for k in range(3):
        message = jnp.where(group == k, low[16 * k : 16 * k + 16], message)
    for peer in range(SLABS):
        send[peer] = message


def first_down_body(w, y, x, block, lo, hi, wx, yx, xs, pair, send, rs):
    b1, c1 = block[pl.ds(0, 32), :], block[pl.ds(32, 32), :]
    own = finish_down(True, w, y, x, b1, c1, lo, hi, wx, yx, xs, pair, rs)
    share(own, c1, pair[pl.ds(96, 32), :], send, rs)


def next_down_body(y, x, block, lo, hi, w, wx, yx, xs, pair, rs):
    finish_down(False, w, y, x, block[...], None, lo, hi, wx, yx, xs, pair, rs)


def wide_share(block, y, x, wx, w1, c1, send, rs):
    lane = iota((32, 128), 1)
    zero = jnp.zeros((32, 128), F32)
    for k, (i, p) in enumerate(((0, 0), (5, 3))):
        far = wx[i] * y[p]
        rs[pl.ds(64 * k, 64), :] = far
        rs[pl.ds(128 + 64 * k, 64), :] = (far - OMEGA * y[p]) + inside_plane(far) + x[p]
    low = jnp.concatenate([row_pairs(rs, 0, 32), row_pairs(rs, 192, 32)], 0)
    high = jnp.concatenate([row_pairs(rs, 64, 32), row_pairs(rs, 128, 32)], 0)
    terms = halves(low, high)
    mix = terms[32:]
    b = [jnp.where(lane >= 64, mix, 0.0), block + terms[:32], jnp.where(lane < 64, mix, 0.0)]
    v = [zero] + [w1[j + 1] * b[j] for j in range(3)] + [zero]
    v = [zero] + [block_sweep(v[j], w1[j], v[j - 1], v[j + 1]) for j in (1, 2, 3)] + [zero]
    r = [0.5 * around_block(zero, zero, v[1])]
    for j in (1, 2, 3):
        r.append(b[j - 1] - (c1[j] + 3.0) * v[j] + 0.5 * around_block(v[j], v[j - 1], v[j + 1]))
    r.append(0.5 * around_block(zero, v[3], zero))
    for k in range(5):
        rs[pl.ds(32 * k, 32), :] = r[k]
    low = quarters(row_pairs(rs, 0, 80))
    group = iota((16, 128), 1) >> 5
    message = low[:16]
    for k in (1, 2, 3):
        message = jnp.where(group == k, low[16 * k : 16 * k + 16], message)
    pieces = [message[4 * k : 4 * k + 4] for k in range(4)]
    last = low[64:68]
    for k in (1, 2, 3):
        last = jnp.where(group[:4] == k, low[64 + 4 * k : 68 + 4 * k], last)
    pieces.append(last)
    for peer in range(SLABS):
        for k in range(5):
            send[5 * peer + k] = pieces[k]


def spread(v):
    v = v + pltpu.roll(v, 64, 1)
    return v + pltpu.roll(v, 32, 1)


def to_coarsest(v, t3):
    for k in range(4):
        t3[pl.ds(16 * k, 16), :] = v[32 * k : 32 * k + 16] + v[32 * k + 16 : 32 * k + 32]
    v = row_pairs(t3, 0, 32)
    lane = iota(v.shape, 1)
    at = (lane & 96) + 2 * (lane & 15)
    v = 0.125 * (lanes_of(v, at) + lanes_of(v, at + 1))
    return jnp.where((lane[:16] & 16) == 0, v[:16], v[16:])


def from_coarsest(v, t3):
    lane = iota(v.shape, 1)
    at = (lane & 96) + ((lane & 31) >> 1)
    v = jnp.concatenate([lanes_of(v, at), lanes_of(v, at + 16)], 0)
    t3[pl.ds(0, 32, stride=2), :] = v
    t3[pl.ds(1, 32, stride=2), :] = v
    parts = []
    for k in range(4):
        block = t3[pl.ds(16 * k, 16), :]
        parts += [block, block]
    return jnp.concatenate(parts, 0)


def low_levels(first, got, w2, d2, w3, x2, t3, joined=None):
    group = iota((16, 128), 1) >> 5
    quarter = iota((16, 128), 0) >> 2
    if not first:
        for z in range(SLABS):
            for k in range(4):
                joined[z, pl.ds(4 * k, 4), :] = got[5 * z + k]
                joined[z, pl.ds(16 + 4 * k, 4), :] = got[5 * z + 4]
    rows = got if first else joined
    reach = 1 if first else 2
    parts, caps = [], []
    for zl in range(8):
        total, cap = None, None
        for zh in range(4):
            z = 8 * zh + zl
            v = jnp.zeros((16, 128), F32)
            for k in range(3 if first else 4):
                if 0 <= z + reach - k < SLABS:
                    v = jnp.where(group == k, rows[z + reach - k, pl.ds(0, 16), :], v)
            if not first and z >= 2:
                v = v + jnp.where(group == quarter, rows[z - 2, pl.ds(16, 16), :], 0.0)
            v = spread(v)
            total = v if total is None else jnp.where(group == zh, v, total)
            if first:
                v = spread(jnp.where(group == 3, got[z], 0.0))
                cap = v if cap is None else jnp.where(group == zh, v, cap)
        parts.append(total)
        caps.append(cap)
    b = jnp.concatenate(parts, 0)
    if first:
        c2 = jnp.concatenate(caps, 0)
        d2[...] = c2 + 1.5
        w2[...] = OMEGA / (c2 + 1.5)
        w3[...] = OMEGA / (to_coarsest(c2, t3) + 0.75)
    w, d = w2[...], d2[...]
    y = w * b
    x = 1.2 * y + 0.25 * w * around_low(y)
    r = b - d * x + 0.25 * around_low(x)
    x = x + from_coarsest(coarsest(to_coarsest(r, t3), w3[...]), t3)
    for _ in range(2):
        x = 0.2 * x + y + 0.25 * w * around_low(x)
    x2[...] = x


def first_low_body(got, w2, d2, w3, x2, t3):
    low_levels(True, got, w2, d2, w3, x2, t3)


def next_low_body(got, w2, d2, w3, after, x2, t3, joined):
    low_levels(False, got, w2, d2, w3, x2, t3, joined)


def fine_up(x2, lo2, pair, hi2, c1, wx, yx, xs, w1, work, out):
    f1, y1, xa, xb, f0, x0, x9 = work
    s = lax.axis_index("space")
    lane = iota((32, 128), 1)

    def blocks(start):
        mixed = [ref[pl.ds(start + 32, 32), :] for ref in (lo2, pair, hi2)]
        return (
            lo2[pl.ds(start, 32), :],
            jnp.where(lane < 64, mixed[0], mixed[1]),
            pair[pl.ds(start, 32), :],
            jnp.where(lane < 64, mixed[1], mixed[2]),
            hi2[pl.ds(start, 32), :],
        )

    if c1 is not None:
        for j, c in enumerate(blocks(64)):
            c1[j] = c
            z = s + (j - 2)
            w1[j] = jnp.where((z >= 0) & (z < SLABS), OMEGA / (c + 3.0), 0.0)
    for j, b in enumerate(blocks(0)):
        y1[j] = w1[j] * b
    zero = jnp.zeros((32, 128), F32)
    lane = iota((16, 128), 1)
    for j in range(5):
        z = s + (j - 2)
        v = x2[pl.ds(pl.multiple_of((z & 7) * 16, 16), 16), :]
        v = lanes_of(v, ((lane & 63) >> 1) + ((z >> 3) & 3) * 32)
        v = jnp.where((z >= 0) & (z < SLABS), v, 0.0)
        f1[pl.ds(32 * j, 16, stride=2), :] = v
        f1[pl.ds(32 * j + 1, 16, stride=2), :] = v
    for j in range(5):
        below = y1[j - 1] if j > 0 else zero
        above = y1[j + 1] if j < 4 else zero
        xa[j] = block_sweep(y1[j], w1[j], below, above) + f1[pl.ds(32 * j, 32), :]
    xb[0] = zero
    xb[4] = zero
    for old, new in ((xa, xb), (xb, xa)):
        for j in (1, 2, 3):
            c = old[j]
            t = around_block(c, old[j - 1], old[j + 1])
            new[j] = 0.2 * c + y1[j] + 0.5 * w1[j] * t
    one, two, three = xa[1], xa[2], xa[3]
    half = iota((32, 128), 1) >> 1
    wide = (
        lanes_of(one, half + 64),
        lanes_of(two, half),
        lanes_of(two, half + 64),
        lanes_of(three, half),
    )
    for q, v in enumerate(wide):
        f0[pl.ds(64 * q, 32, stride=2), :] = v
        f0[pl.ds(64 * q + 1, 32, stride=2), :] = v
    for i in range(8):
        x0[i] = xs[i] + f0[pl.ds(64 * (i // 2), 64), :]
    for i in range(6):
        c = x0[i + 1]
        x9[i] = 0.2 * c + yx[i] + wx[i] * around_plane(c, x0[i], x0[i + 2])
    for p in range(DEPTH):
        c = x9[p + 1]
        out(p, 0.2 * c + yx[p + 1] + wx[p + 1] * around_plane(c, x9[p], x9[p + 2]))


def first_up_body(
    x2, lo2, pair, hi2, wx, yx, xs, w, cap, src, u_out, y, x, block, up, dn, w1, send, *work
):
    b_out, c1, rs, *work = work

    def out(p, u):
        u_out[0, p] = u
        b_out[p] = cap[p] * u + src[0, 1, p]

    fine_up(x2, lo2, pair, hi2, c1, wx, yx, xs, w1, work, out)
    own = local_down(lambda p: b_out[p], cap, w, y, x, rs, False)
    wide_share(own, y, x, wx, w1, c1, send, rs)
    block[...] = own
    fill_edges(up, dn, y, x)
    up[pl.ds(192, 32), :] = own
    dn[pl.ds(192, 32), :] = own


def next_up_body(x2, lo2, pair, hi2, wx, yx, xs, w1, u_out, *work):
    def out(p, u):
        u_out[0, p] = u

    fine_up(x2, lo2, pair, hi2, None, wx, yx, xs, w1, work, out)


LOW_WORK = [(64, 128)]
LOW_FLOPS = 1 << 31
WORK = [
    (160, 128),
    (5, 32, 128),
    (5, 32, 128),
    (5, 32, 128),
    (256, 128),
    (8, NY, NX),
    (6, NY, NX),
]
EDGE_SUMS = (256, 128)
PLANE = (NY, NX)
PLANE4 = (DEPTH, NY, NX)
MESSAGE = f32(SLABS, 16, 128)
WIDE_MESSAGE = f32(SLABS * 5, 4, 128)


def moved(x, spans, slabs):
    pairs = []
    for t in range(SPANS):
        for s in range(SLABS):
            pairs.append((t * SLABS + s, (t + spans) % SPANS * SLABS + (s + slabs) % SLABS))
    return lax.ppermute(x, ("tm", "space"), pairs)


def gathered(send):
    return lax.all_to_all(send, "space", 0, 0, tiled=True)


def both(up, dn, reach):
    lo = moved(up, 0, reach)
    hi = moved(dn, 0, -reach)
    return lo, hi


def near(pair):
    lo, hi = both(pair, pair, 2)
    return lo, pair, hi


def shards(u0, src, cap):
    slab = f32(*PLANE4)
    w, y, x, block, up, dn, cap_in = call(
        pack_body,
        (slab, slab, slab, f32(64, 128), f32(288, 128), f32(288, 128), slab),
        [PLANE4, PLANE4, EDGE_SUMS],
        *(pltpu.with_memory_space_constraint(v, pltpu.HBM) for v in (u0, src, cap)),
        space=pl.BlockSpec(memory_space=pltpu.HBM),
        sems=[pltpu.SemaphoreType.DMA((3,))],
    )
    lo, hi = both(up, dn, 1)
    wx, yx, xs, pair, send = call(
        first_down_body,
        (f32(6, *PLANE), f32(6, *PLANE), f32(8, *PLANE), f32(128, 128), MESSAGE),
        [EDGE_SUMS],
        *(w, y, x, block, lo, hi),
    )
    got = gathered(send)
    w2, d2, w3, x2 = call(
        first_low_body,
        (f32(128, 128), f32(128, 128), f32(16, 128), f32(128, 128)),
        LOW_WORK,
        got,
        flops=LOW_FLOPS,
    )
    fpoint, y, x, block, up, dn, w1, send = call(
        first_up_body,
        (
            f32(1, *PLANE4),
            slab,
            slab,
            f32(32, 128),
            f32(224, 128),
            f32(224, 128),
            f32(5, 32, 128),
            WIDE_MESSAGE,
        ),
        [PLANE4, (5, 32, 128), EDGE_SUMS, *WORK],
        *(x2, *near(pair), wx, yx, xs, w, cap_in, src),
    )
    got = gathered(send)
    lo, hi = both(up, dn, 1)
    yx, xs, pair = call(
        next_down_body,
        (f32(6, *PLANE), f32(8, *PLANE), f32(64, 128)),
        [EDGE_SUMS],
        *(y, x, block, lo, hi, w, wx),
    )
    (x2,) = call(
        next_low_body,
        (f32(128, 128),),
        [*LOW_WORK, (SLABS, 32, 128)],
        *(got, w2, d2, w3, pair),
        flops=LOW_FLOPS,
    )
    (u,) = call(next_up_body, (f32(1, *PLANE4),), WORK, *(x2, *near(pair), wx, yx, xs, w1))
    updated = jnp.where(lax.axis_index("tm") == 0, u0, moved(u, 1, 0))
    return fpoint, updated


def solution(mesh):
    in_specs = (
        P("tm", "space", None, None),
        P("tm", None, "space", None, None),
        P("space", None, None),
    )
    out_specs = (P("tm", "space", None, None), P("tm", "space", None, None))
    return jax.shard_map(shards, mesh=mesh, in_specs=in_specs, out_specs=out_specs, check_vma=False)
```

```python
import jax
import jax.numpy as jnp
from jax import lax
from jax.experimental import pallas as pl
from jax.experimental.pallas import tpu as pltpu
from jax.sharding import PartitionSpec as P


COARSE_SWEEPS = 24
NY, NX = 64, 128
SLABS = 32
SPANS = 8
DEPTH = 4
OMEGA = 0.8
F32 = jnp.float32
VMEM = pl.BlockSpec(memory_space=pltpu.VMEM)


def f32(*shape):
    return jax.ShapeDtypeStruct(shape, F32)


def call(body, outs, scratch, *args, space=VMEM, flops=None, sems=()):
    return pl.pallas_call(
        body,
        out_shape=outs,
        in_specs=[space] * len(args),
        out_specs=tuple(VMEM for _ in outs),
        scratch_shapes=[pltpu.VMEM(s, F32) for s in scratch] + list(sems),
        compiler_params=pltpu.CompilerParams(vmem_limit_bytes=16 << 20),
        cost_estimate=flops and pl.CostEstimate(flops=flops, transcendentals=0, bytes_accessed=0),
    )(*args)


def lanes_of(v, lane):
    return jnp.take_along_axis(v, lane, axis=1, mode="promise_in_bounds")


def iota(shape, axis):
    return lax.broadcasted_iota(jnp.int32, shape, axis)


def halves(low, high):
    lane = iota(low.shape, 1)
    at = (lane & 63) * 2
    low = lanes_of(low, at) + lanes_of(low, at + 1)
    high = lanes_of(high, at) + lanes_of(high, at + 1)
    return 0.125 * jnp.where(lane < 64, low, high)


def quarters(v):
    at = (iota(v.shape, 1) & 31) * 2
    low = lanes_of(v, at) + lanes_of(v, at + 1)
    return 0.125 * (low + (lanes_of(v, at + 64) + lanes_of(v, at + 65)))


def inside_plane(c):
    row, lane = iota(c.shape, 0), iota(c.shape, 1)
    total = jnp.where(lane > 0, pltpu.roll(c, 1, 1), 0.0)
    total = total + jnp.where(lane < NX - 1, pltpu.roll(c, NX - 1, 1), 0.0)
    total = total + jnp.where(row > 0, pltpu.roll(c, 1, 0), 0.0)
    return total + jnp.where(row < NY - 1, pltpu.roll(c, NY - 1, 0), 0.0)


def around_plane(c, below, above):
    return inside_plane(c) + (below + above)


def around_block(c, below, above):
    row, lane = iota(c.shape, 0), iota(c.shape, 1)
    col = lane & 63
    total = pltpu.roll(c + jnp.where(lane < 64, above, below), 64, 1)
    total = total + jnp.where(col > 0, pltpu.roll(c, 1, 1), 0.0)
    total = total + jnp.where(col < 63, pltpu.roll(c, 127, 1), 0.0)
    total = total + jnp.where(row > 0, pltpu.roll(c, 1, 0), 0.0)
    return total + jnp.where(row < 31, pltpu.roll(c, 31, 0), 0.0)


def around_low(v):
    row, lane = iota(v.shape, 0), iota(v.shape, 1)
    y, x = row & 15, lane & 31
    ends = iota((16, 128), 1)
    below = jnp.where(ends >= 32, pltpu.roll(v[112:], 32, 1), 0.0)
    above = jnp.where(ends < 96, pltpu.roll(v[:16], 96, 1), 0.0)
    total = jnp.concatenate([below, v[:112]], 0) + jnp.concatenate([v[16:], above], 0)
    total = total + jnp.where(x > 0, pltpu.roll(v, 1, 1), 0.0)
    total = total + jnp.where(x < 31, pltpu.roll(v, 127, 1), 0.0)
    total = total + jnp.where(y > 0, pltpu.roll(v, 1, 0), 0.0)
    return total + jnp.where(y < 15, pltpu.roll(v, 127, 0), 0.0)


def rolled(v, k, j):
    return pltpu.roll(v[k % 2], (j - 16 * (k // 2)) % 128, 1) if (k // 2 or j) else v[k]


def within(reach):
    return [
        (k, j)
        for k in range(-reach, 2 + reach)
        for j in range(-reach, reach + 1)
        if max(0, -k, k - 1) + abs(j) <= reach
    ]


def coarsest(b3, w3, most):
    lane, row = iota((8, 128), 1), iota((8, 128), 0)
    x = lane & 15
    base, own = [], []
    for k in range(2):
        w = w3[8 * k : 8 * k + 8]
        wh = 0.125 * w
        own.append(w * b3[8 * k : 8 * k + 8])
        base.append(
            (
                jnp.where(lane >= 16, wh, 0.0) if k == 0 else wh,
                jnp.where(lane < 112, wh, 0.0) if k == 1 else wh,
                jnp.where(x > 0, wh, 0.0),
                jnp.where(x < 15, wh, 0.0),
                jnp.where(row > 0, wh, 0.0),
                jnp.where(row < 7, wh, 0.0),
            )
        )
    terms = list(zip(*base))
    steps = {
        (k, j): (rolled(own, k, j), *(rolled(t, k, j) for t in terms)) for k, j in within(most - 1)
    }

    def sweep(v, k, j):
        wb, below, above, left, right, up, down = steps[k, j]
        c = v[k, j]
        t = (0.2 * c + wb) + (below * v[k - 1, j] + above * v[k + 1, j])
        s = up * pltpu.roll(c, 1, 0) + down * pltpu.roll(c, 7, 0)
        return (t + s) + (left * v[k, j + 1] + right * v[k, j - 1])

    v, remaining = own, COARSE_SWEEPS - 1
    while remaining:
        count = min(most, remaining)
        v = {(k, j): rolled(v, k, j) for k, j in within(count)}
        for reach in reversed(range(count)):
            v = {(k, j): sweep(v, k, j) for k, j in within(reach)}
        v = [v[k, 0] for k in range(2)]
        remaining -= count
    return jnp.concatenate(v, 0)


def row_pairs(ref, start, count):
    return ref[pl.ds(start, count, stride=2), :] + ref[pl.ds(start + 1, count, stride=2), :]


def block_sweep(y, w, below, above):
    return 1.2 * y + 0.5 * w * around_block(y, below, above)


def local_down(b, cap, w, y, x, rs, first):
    for p in range(DEPTH):
        y[p] = w[p] * b(p)
    zero = jnp.zeros((NY, NX), F32)
    for p in range(DEPTH):
        below = y[p - 1] if p > 0 else zero
        above = y[p + 1] if p < 3 else zero
        x[p] = 1.2 * y[p] + w[p] * around_plane(y[p], below, above)
    for half in range(2):
        total = None
        for p in (2 * half, 2 * half + 1):
            below = x[p - 1] if p > 0 else zero
            above = x[p + 1] if p < 3 else zero
            r = b(p) - (cap[p] + 6.0) * x[p] + around_plane(x[p], below, above)
            total = r if total is None else total + r
        rs[pl.ds(64 * half, 64), :] = total
        if first:
            rs[pl.ds(128 + 64 * half, 64), :] = cap[2 * half] + cap[2 * half + 1]
    low, high = row_pairs(rs, 0, 32), row_pairs(rs, 64, 32)
    if first:
        low = jnp.concatenate([low, row_pairs(rs, 128, 32)], 0)
        high = jnp.concatenate([high, row_pairs(rs, 192, 32)], 0)
    return halves(low, high)


def fill_edges(up, dn, y, x):
    for edge, p, q in ((up, 3, 2), (dn, 0, 1)):
        edge[pl.ds(0, 64), :] = y[p]
        edge[pl.ds(64, 64), :] = x[p]
        edge[pl.ds(128, 64), :] = x[q]


def pack_body(u, src, cap, w, y, x, block, up, dn, cap_out, u_in, src_in, rs, sems):
    copies = [
        pltpu.make_async_copy(cap, cap_out, sems.at[0]),
        pltpu.make_async_copy(u.at[0], u_in, sems.at[1]),
        pltpu.make_async_copy(src.at[0, 0], src_in, sems.at[2]),
    ]
    for copy in copies:
        copy.start()
    copies[0].wait()
    for p in range(DEPTH):
        w[p] = OMEGA / (cap_out[p] + 6.0)
    for copy in copies[1:]:
        copy.wait()
    for p in range(DEPTH):
        u_in[p] = cap_out[p] * u_in[p] + src_in[p]
    blocks = local_down(lambda p: u_in[p], cap_out, w, y, x, rs, True)
    block[...] = blocks
    fill_edges(up, dn, y, x)
    lane = iota((32, 128), 1)
    b1, c1 = blocks[:32], blocks[32:]
    up[pl.ds(192, 32), :] = jnp.where(lane < 64, pltpu.roll(b1, 64, 1), c1)
    dn[pl.ds(192, 32), :] = jnp.where(lane < 64, b1, pltpu.roll(c1, 64, 1))
    up[pl.ds(224, 64), :] = w[3]
    dn[pl.ds(224, 64), :] = w[0]


def finish_down(first, w, y, x, b1, c1, lo, hi, wx, yx, xs, pair, rs):
    s = lax.axis_index("space")
    lane = iota((32, 128), 1)

    def edge(ref, there):
        return [
            jnp.where(there, ref[pl.ds(start, 64), :], 0.0)
            for start in ((0, 64, 128, 224) if first else (0, 64, 128))
        ]

    sides = []
    for ref, there, i, p in ((lo, s > 0, 0, 0), (hi, s < SLABS - 1, 5, 3)):
        ye, xe, xs_far, *we = edge(ref, there)
        if first:
            wx[i] = we[0]
        yx[i] = ye
        near = w[p] * ye
        far = wx[i] * y[p]
        x_near, x_far = x[p] + near, xe + far
        j = 1 if p == 0 else 6
        xs[j] = x_far
        xs[0 if p == 0 else 7] = xs_far
        xs[p + 2] = x_near
        own = (near - OMEGA * ye) + inside_plane(near) + x_far
        beside = (far - OMEGA * y[p]) + inside_plane(far) + x_near
        sides.append((own, jnp.where(there, beside, 0.0)))
    for p in range(DEPTH):
        yx[p + 1] = y[p]
        if first:
            wx[p + 1] = w[p]
    xs[3] = x[1]
    xs[4] = x[2]
    for k, v in enumerate((sides[0][0], sides[1][1], sides[1][0], sides[0][1])):
        rs[pl.ds(64 * k, 64), :] = v
    low = jnp.concatenate([row_pairs(rs, 0, 32), row_pairs(rs, 64, 32)], 0)
    high = jnp.concatenate([row_pairs(rs, 128, 32), row_pairs(rs, 192, 32)], 0)
    terms = halves(low, high)
    lo_block, hi_block = lo[pl.ds(192, 32), :], hi[pl.ds(192, 32), :]
    if first:
        pair[pl.ds(64, 32), :] = c1
        pair[pl.ds(96, 32), :] = jnp.where(lane < 64, pltpu.roll(hi_block, 64, 1), lo_block)
        lo_block = pltpu.roll(lo_block, 64, 1)
    own = b1 + terms[:32]
    pair[pl.ds(0, 32), :] = own
    pair[pl.ds(32, 32), :] = jnp.where(lane < 64, hi_block, lo_block) + terms[32:]
    return own


def share(b1, c1, c_mix, send, rs):
    s = lax.axis_index("space")
    lane = iota((32, 128), 1)
    zero = jnp.zeros((32, 128), F32)
    own, beside = c1 + 3.0, c_mix + 3.0
    w_own, w_mix = OMEGA / own, OMEGA / beside
    y = w_own * b1
    x = [
        block_sweep(zero, jnp.where((lane >= 64) & (s > 0), w_mix, 0.0), zero, y),
        block_sweep(y, w_own, zero, zero),
        block_sweep(zero, jnp.where((lane < 64) & (s < SLABS - 1), w_mix, 0.0), y, zero),
    ]
    r = [
        0.5 * around_block(x[0], zero, x[1]) - beside * x[0],
        b1 - own * x[1] + 0.5 * around_block(x[1], x[0], x[2]),
        0.5 * around_block(x[2], x[1], zero) - beside * x[2],
        c1,
    ]
    for k in range(4):
        rs[pl.ds(32 * k, 32), :] = r[k]
    low = quarters(row_pairs(rs, 0, 64))
    group = iota((16, 128), 1) >> 5
    message = low[48:]
    for k in range(3):
        message = jnp.where(group == k, low[16 * k : 16 * k + 16], message)
    for peer in range(SLABS):
        send[peer] = message


def first_down_body(w, y, x, block, lo, hi, wx, yx, xs, pair, send, rs):
    b1, c1 = block[pl.ds(0, 32), :], block[pl.ds(32, 32), :]
    own = finish_down(True, w, y, x, b1, c1, lo, hi, wx, yx, xs, pair, rs)
    share(own, c1, pair[pl.ds(96, 32), :], send, rs)


def next_down_body(y, x, block, lo, hi, w, wx, yx, xs, pair, rs):
    finish_down(False, w, y, x, block[...], None, lo, hi, wx, yx, xs, pair, rs)


def wide_share(block, y, x, wx, w1, c1, send, rs):
    lane = iota((32, 128), 1)
    zero = jnp.zeros((32, 128), F32)
    for k, (i, p) in enumerate(((0, 0), (5, 3))):
        far = wx[i] * y[p]
        rs[pl.ds(64 * k, 64), :] = far
        rs[pl.ds(128 + 64 * k, 64), :] = (far - OMEGA * y[p]) + inside_plane(far) + x[p]
    low = jnp.concatenate([row_pairs(rs, 0, 32), row_pairs(rs, 192, 32)], 0)
    high = jnp.concatenate([row_pairs(rs, 64, 32), row_pairs(rs, 128, 32)], 0)
    terms = halves(low, high)
    mix = terms[32:]
    b = [jnp.where(lane >= 64, mix, 0.0), block + terms[:32], jnp.where(lane < 64, mix, 0.0)]
    v = [zero] + [w1[j + 1] * b[j] for j in range(3)] + [zero]
    v = [zero] + [block_sweep(v[j], w1[j], v[j - 1], v[j + 1]) for j in (1, 2, 3)] + [zero]
    r = [0.5 * around_block(zero, zero, v[1])]
    for j in (1, 2, 3):
        r.append(b[j - 1] - (c1[j] + 3.0) * v[j] + 0.5 * around_block(v[j], v[j - 1], v[j + 1]))
    r.append(0.5 * around_block(zero, v[3], zero))
    for k in range(5):
        rs[pl.ds(32 * k, 32), :] = r[k]
    low = quarters(row_pairs(rs, 0, 80))
    group = iota((16, 128), 1) >> 5
    message = low[:16]
    for k in (1, 2, 3):
        message = jnp.where(group == k, low[16 * k : 16 * k + 16], message)
    pieces = [message[4 * k : 4 * k + 4] for k in range(4)]
    last = low[64:68]
    for k in (1, 2, 3):
        last = jnp.where(group[:4] == k, low[64 + 4 * k : 68 + 4 * k], last)
    pieces.append(last)
    for peer in range(SLABS):
        for k in range(5):
            send[5 * peer + k] = pieces[k]


def spread(v):
    v = v + pltpu.roll(v, 64, 1)
    return v + pltpu.roll(v, 32, 1)


def to_coarsest(v, t3):
    for k in range(4):
        t3[pl.ds(16 * k, 16), :] = v[32 * k : 32 * k + 16] + v[32 * k + 16 : 32 * k + 32]
    v = row_pairs(t3, 0, 32)
    lane = iota(v.shape, 1)
    at = (lane & 96) + 2 * (lane & 15)
    v = 0.125 * (lanes_of(v, at) + lanes_of(v, at + 1))
    return jnp.where((lane[:16] & 16) == 0, v[:16], v[16:])


def from_coarsest(v, t3):
    lane = iota(v.shape, 1)
    at = (lane & 96) + ((lane & 31) >> 1)
    v = jnp.concatenate([lanes_of(v, at), lanes_of(v, at + 16)], 0)
    t3[pl.ds(0, 32, stride=2), :] = v
    t3[pl.ds(1, 32, stride=2), :] = v
    parts = []
    for k in range(4):
        block = t3[pl.ds(16 * k, 16), :]
        parts += [block, block]
    return jnp.concatenate(parts, 0)


def low_levels(first, got, w2, d2, w3, x2, t3, joined=None):
    group = iota((16, 128), 1) >> 5
    quarter = iota((16, 128), 0) >> 2
    if not first:
        for z in range(SLABS):
            for k in range(4):
                joined[z, pl.ds(4 * k, 4), :] = got[5 * z + k]
                joined[z, pl.ds(16 + 4 * k, 4), :] = got[5 * z + 4]
    rows = got if first else joined
    reach = 1 if first else 2
    parts, caps = [], []
    for zl in range(8):
        total, cap = None, None
        for zh in range(4):
            z = 8 * zh + zl
            v = jnp.zeros((16, 128), F32)
            for k in range(3 if first else 4):
                if 0 <= z + reach - k < SLABS:
                    v = jnp.where(group == k, rows[z + reach - k, pl.ds(0, 16), :], v)
            if not first and z >= 2:
                v = v + jnp.where(group == quarter, rows[z - 2, pl.ds(16, 16), :], 0.0)
            v = spread(v)
            total = v if total is None else jnp.where(group == zh, v, total)
            if first:
                v = spread(jnp.where(group == 3, got[z], 0.0))
                cap = v if cap is None else jnp.where(group == zh, v, cap)
        parts.append(total)
        caps.append(cap)
    b = jnp.concatenate(parts, 0)
    if first:
        c2 = jnp.concatenate(caps, 0)
        d2[...] = c2 + 1.5
        w2[...] = OMEGA / (c2 + 1.5)
        w3[...] = OMEGA / (to_coarsest(c2, t3) + 0.75)
    w, d = w2[...], d2[...]
    y = w * b
    x = 1.2 * y + 0.25 * w * around_low(y)
    r = b - d * x + 0.25 * around_low(x)
    x = x + from_coarsest(coarsest(to_coarsest(r, t3), w3[...], 2 if first else 3), t3)
    for _ in range(2):
        x = 0.2 * x + y + 0.25 * w * around_low(x)
    x2[...] = x


def first_low_body(got, w2, d2, w3, x2, t3):
    low_levels(True, got, w2, d2, w3, x2, t3)


def next_low_body(got, w2, d2, w3, after, x2, t3, joined):
    low_levels(False, got, w2, d2, w3, x2, t3, joined)


def fine_up(x2, lo2, pair, hi2, c1, wx, yx, xs, w1, work, out):
    f1, y1, xa, xb, f0, x0, x9 = work
    s = lax.axis_index("space")
    lane = iota((32, 128), 1)

    def blocks(start):
        mixed = [ref[pl.ds(start + 32, 32), :] for ref in (lo2, pair, hi2)]
        return (
            lo2[pl.ds(start, 32), :],
            jnp.where(lane < 64, mixed[0], mixed[1]),
            pair[pl.ds(start, 32), :],
            jnp.where(lane < 64, mixed[1], mixed[2]),
            hi2[pl.ds(start, 32), :],
        )

    if c1 is not None:
        for j, c in enumerate(blocks(64)):
            c1[j] = c
            z = s + (j - 2)
            w1[j] = jnp.where((z >= 0) & (z < SLABS), OMEGA / (c + 3.0), 0.0)
    for j, b in enumerate(blocks(0)):
        y1[j] = w1[j] * b
    zero = jnp.zeros((32, 128), F32)
    lane = iota((16, 128), 1)
    for j in range(5):
        z = s + (j - 2)
        v = x2[pl.ds(pl.multiple_of((z & 7) * 16, 16), 16), :]
        v = lanes_of(v, ((lane & 63) >> 1) + ((z >> 3) & 3) * 32)
        v = jnp.where((z >= 0) & (z < SLABS), v, 0.0)
        f1[pl.ds(32 * j, 16, stride=2), :] = v
        f1[pl.ds(32 * j + 1, 16, stride=2), :] = v
    for j in range(5):
        below = y1[j - 1] if j > 0 else zero
        above = y1[j + 1] if j < 4 else zero
        xa[j] = block_sweep(y1[j], w1[j], below, above) + f1[pl.ds(32 * j, 32), :]
    xb[0] = zero
    xb[4] = zero
    for old, new in ((xa, xb), (xb, xa)):
        for j in (1, 2, 3):
            c = old[j]
            t = around_block(c, old[j - 1], old[j + 1])
            new[j] = 0.2 * c + y1[j] + 0.5 * w1[j] * t
    one, two, three = xa[1], xa[2], xa[3]
    half = iota((32, 128), 1) >> 1
    wide = (
        lanes_of(one, half + 64),
        lanes_of(two, half),
        lanes_of(two, half + 64),
        lanes_of(three, half),
    )
    for q, v in enumerate(wide):
        f0[pl.ds(64 * q, 32, stride=2), :] = v
        f0[pl.ds(64 * q + 1, 32, stride=2), :] = v
    for i in range(8):
        x0[i] = xs[i] + f0[pl.ds(64 * (i // 2), 64), :]
    for i in range(6):
        c = x0[i + 1]
        x9[i] = 0.2 * c + yx[i] + wx[i] * around_plane(c, x0[i], x0[i + 2])
    for p in range(DEPTH):
        c = x9[p + 1]
        out(p, 0.2 * c + yx[p + 1] + wx[p + 1] * around_plane(c, x9[p], x9[p + 2]))


def first_up_body(
    x2, lo2, pair, hi2, wx, yx, xs, w, cap, src, u_out, y, x, block, up, dn, w1, send, *work
):
    b_out, c1, rs, *work = work

    def out(p, u):
        u_out[0, p] = u
        b_out[p] = cap[p] * u + src[0, 1, p]

    fine_up(x2, lo2, pair, hi2, c1, wx, yx, xs, w1, work, out)
    own = local_down(lambda p: b_out[p], cap, w, y, x, rs, False)
    wide_share(own, y, x, wx, w1, c1, send, rs)
    block[...] = own
    fill_edges(up, dn, y, x)
    up[pl.ds(192, 32), :] = own
    dn[pl.ds(192, 32), :] = own


def next_up_body(x2, lo2, pair, hi2, wx, yx, xs, w1, u_out, *work):
    def out(p, u):
        u_out[0, p] = u

    fine_up(x2, lo2, pair, hi2, None, wx, yx, xs, w1, work, out)


LOW_WORK = [(64, 128)]
LOW_FLOPS = 1 << 31
WORK = [
    (160, 128),
    (5, 32, 128),
    (5, 32, 128),
    (5, 32, 128),
    (256, 128),
    (8, NY, NX),
    (6, NY, NX),
]
EDGE_SUMS = (256, 128)
PLANE = (NY, NX)
PLANE4 = (DEPTH, NY, NX)
MESSAGE = f32(SLABS, 16, 128)
WIDE_MESSAGE = f32(SLABS * 5, 4, 128)


def moved(x, spans, slabs):
    pairs = []
    for t in range(SPANS):
        for s in range(SLABS):
            pairs.append((t * SLABS + s, (t + spans) % SPANS * SLABS + (s + slabs) % SLABS))
    return lax.ppermute(x, ("tm", "space"), pairs)


def gathered(send):
    return lax.all_to_all(send, "space", 0, 0, tiled=True)


def both(up, dn, reach):
    lo = moved(up, 0, reach)
    hi = moved(dn, 0, -reach)
    return lo, hi


def near(pair):
    lo, hi = both(pair, pair, 2)
    return lo, pair, hi


def shards(u0, src, cap):
    slab = f32(*PLANE4)
    w, y, x, block, up, dn, cap_in = call(
        pack_body,
        (slab, slab, slab, f32(64, 128), f32(288, 128), f32(288, 128), slab),
        [PLANE4, PLANE4, EDGE_SUMS],
        *(pltpu.with_memory_space_constraint(v, pltpu.HBM) for v in (u0, src, cap)),
        space=pl.BlockSpec(memory_space=pltpu.HBM),
        sems=[pltpu.SemaphoreType.DMA((3,))],
    )
    lo, hi = both(up, dn, 1)
    wx, yx, xs, pair, send = call(
        first_down_body,
        (f32(6, *PLANE), f32(6, *PLANE), f32(8, *PLANE), f32(128, 128), MESSAGE),
        [EDGE_SUMS],
        *(w, y, x, block, lo, hi),
    )
    got = gathered(send)
    w2, d2, w3, x2 = call(
        first_low_body,
        (f32(128, 128), f32(128, 128), f32(16, 128), f32(128, 128)),
        LOW_WORK,
        got,
        flops=LOW_FLOPS,
    )
    fpoint, y, x, block, up, dn, w1, send = call(
        first_up_body,
        (
            f32(1, *PLANE4),
            slab,
            slab,
            f32(32, 128),
            f32(224, 128),
            f32(224, 128),
            f32(5, 32, 128),
            WIDE_MESSAGE,
        ),
        [PLANE4, (5, 32, 128), EDGE_SUMS, *WORK],
        *(x2, *near(pair), wx, yx, xs, w, cap_in, src),
    )
    got = gathered(send)
    lo, hi = both(up, dn, 1)
    yx, xs, pair = call(
        next_down_body,
        (f32(6, *PLANE), f32(8, *PLANE), f32(64, 128)),
        [EDGE_SUMS],
        *(y, x, block, lo, hi, w, wx),
    )
    (x2,) = call(
        next_low_body,
        (f32(128, 128),),
        [*LOW_WORK, (SLABS, 32, 128)],
        *(got, w2, d2, w3, pair),
        flops=LOW_FLOPS,
    )
    (u,) = call(next_up_body, (f32(1, *PLANE4),), WORK, *(x2, *near(pair), wx, yx, xs, w1))
    updated = jnp.where(lax.axis_index("tm") == 0, u0, moved(u, 1, 0))
    return fpoint, updated


def solution(mesh):
    in_specs = (
        P("tm", "space", None, None),
        P("tm", None, "space", None, None),
        P("space", None, None),
    )
    out_specs = (P("tm", "space", None, None), P("tm", "space", None, None))
    return jax.shard_map(shards, mesh=mesh, in_specs=in_specs, out_specs=out_specs, check_vma=False)
```

```python
import jax
import jax.numpy as jnp
from jax import lax
from jax.experimental import pallas as pl
from jax.experimental.pallas import tpu as pltpu
from jax.sharding import PartitionSpec as P


COARSE_SWEEPS = 24
NY, NX = 64, 128
SLABS = 32
SPANS = 8
DEPTH = 4
OMEGA = 0.8
F32 = jnp.float32
VMEM = pl.BlockSpec(memory_space=pltpu.VMEM)


def f32(*shape):
    return jax.ShapeDtypeStruct(shape, F32)


def call(body, outs, scratch, *args, space=VMEM, flops=None, sems=()):
    return pl.pallas_call(
        body,
        out_shape=outs,
        in_specs=[space] * len(args),
        out_specs=tuple(VMEM for _ in outs),
        scratch_shapes=[pltpu.VMEM(s, F32) for s in scratch] + list(sems),
        compiler_params=pltpu.CompilerParams(vmem_limit_bytes=16 << 20),
        cost_estimate=flops and pl.CostEstimate(flops=flops, transcendentals=0, bytes_accessed=0),
    )(*args)


def lanes_of(v, lane):
    return jnp.take_along_axis(v, lane, axis=1, mode="promise_in_bounds")


def iota(shape, axis):
    return lax.broadcasted_iota(jnp.int32, shape, axis)


def halves(low, high):
    lane = iota(low.shape, 1)
    at = (lane & 63) * 2
    low = lanes_of(low, at) + lanes_of(low, at + 1)
    high = lanes_of(high, at) + lanes_of(high, at + 1)
    return 0.125 * jnp.where(lane < 64, low, high)


def quarters(v):
    at = (iota(v.shape, 1) & 31) * 2
    low = lanes_of(v, at) + lanes_of(v, at + 1)
    return 0.125 * (low + (lanes_of(v, at + 64) + lanes_of(v, at + 65)))


def inside_plane(c):
    row, lane = iota(c.shape, 0), iota(c.shape, 1)
    total = jnp.where(lane > 0, pltpu.roll(c, 1, 1), 0.0)
    total = total + jnp.where(lane < NX - 1, pltpu.roll(c, NX - 1, 1), 0.0)
    total = total + jnp.where(row > 0, pltpu.roll(c, 1, 0), 0.0)
    return total + jnp.where(row < NY - 1, pltpu.roll(c, NY - 1, 0), 0.0)


def around_plane(c, below, above):
    return inside_plane(c) + (below + above)


def around_block(c, below, above):
    row, lane = iota(c.shape, 0), iota(c.shape, 1)
    col = lane & 63
    total = pltpu.roll(c + jnp.where(lane < 64, above, below), 64, 1)
    total = total + jnp.where(col > 0, pltpu.roll(c, 1, 1), 0.0)
    total = total + jnp.where(col < 63, pltpu.roll(c, 127, 1), 0.0)
    total = total + jnp.where(row > 0, pltpu.roll(c, 1, 0), 0.0)
    return total + jnp.where(row < 31, pltpu.roll(c, 31, 0), 0.0)


def around_low(v):
    row, lane = iota(v.shape, 0), iota(v.shape, 1)
    y, x = row & 15, lane & 31
    ends = iota((16, 128), 1)
    below = jnp.where(ends >= 32, pltpu.roll(v[112:], 32, 1), 0.0)
    above = jnp.where(ends < 96, pltpu.roll(v[:16], 96, 1), 0.0)
    total = jnp.concatenate([below, v[:112]], 0) + jnp.concatenate([v[16:], above], 0)
    total = total + jnp.where(x > 0, pltpu.roll(v, 1, 1), 0.0)
    total = total + jnp.where(x < 31, pltpu.roll(v, 127, 1), 0.0)
    total = total + jnp.where(y > 0, pltpu.roll(v, 1, 0), 0.0)
    return total + jnp.where(y < 15, pltpu.roll(v, 127, 0), 0.0)


def rolled(v, k, j):
    return pltpu.roll(v[k % 2], (j - 16 * (k // 2)) % 128, 1) if (k // 2 or j) else v[k]


def within(reach):
    return [
        (k, j)
        for k in range(-reach, 2 + reach)
        for j in range(-reach, reach + 1)
        if max(0, -k, k - 1) + abs(j) <= reach
    ]


def coarsest(b3, w3, most):
    lane, row = iota((8, 128), 1), iota((8, 128), 0)
    x = lane & 15
    base, own = [], []
    for k in range(2):
        w = w3[8 * k : 8 * k + 8]
        wh = 0.125 * w
        own.append(w * b3[8 * k : 8 * k + 8])
        base.append(
            (
                jnp.where(lane >= 16, wh, 0.0) if k == 0 else wh,
                jnp.where(lane < 112, wh, 0.0) if k == 1 else wh,
                jnp.where(x > 0, wh, 0.0),
                jnp.where(x < 15, wh, 0.0),
                jnp.where(row > 0, wh, 0.0),
                jnp.where(row < 7, wh, 0.0),
            )
        )
    terms = list(zip(*base))
    steps = {
        (k, j): (rolled(own, k, j), *(rolled(t, k, j) for t in terms)) for k, j in within(most - 1)
    }

    def sweep(v, k, j):
        wb, below, above, left, right, up, down = steps[k, j]
        c = v[k, j]
        t = (0.2 * c + wb) + (below * v[k - 1, j] + above * v[k + 1, j])
        s = up * pltpu.roll(c, 1, 0) + down * pltpu.roll(c, 7, 0)
        return (t + s) + (left * v[k, j + 1] + right * v[k, j - 1])

    v, remaining = own, COARSE_SWEEPS - 1
    while remaining:
        count = min(most, remaining)
        v = {(k, j): rolled(v, k, j) for k, j in within(count)}
        for reach in reversed(range(count)):
            v = {(k, j): sweep(v, k, j) for k, j in within(reach)}
        v = [v[k, 0] for k in range(2)]
        remaining -= count
    return jnp.concatenate(v, 0)


def row_pairs(ref, start, count):
    return ref[pl.ds(start, count, stride=2), :] + ref[pl.ds(start + 1, count, stride=2), :]


def block_sweep(y, w, below, above):
    return 1.2 * y + 0.5 * w * around_block(y, below, above)


def local_down(b, cap, w, y, x, rs, first):
    for p in range(DEPTH):
        y[p] = w[p] * b(p)
    zero = jnp.zeros((NY, NX), F32)
    for p in range(DEPTH):
        below = y[p - 1] if p > 0 else zero
        above = y[p + 1] if p < 3 else zero
        x[p] = 1.2 * y[p] + w[p] * around_plane(y[p], below, above)
    for half in range(2):
        total = None
        for p in (2 * half, 2 * half + 1):
            below = x[p - 1] if p > 0 else zero
            above = x[p + 1] if p < 3 else zero
            r = b(p) - (cap[p] + 6.0) * x[p] + around_plane(x[p], below, above)
            total = r if total is None else total + r
        rs[pl.ds(64 * half, 64), :] = total
        if first:
            rs[pl.ds(128 + 64 * half, 64), :] = cap[2 * half] + cap[2 * half + 1]
    low, high = row_pairs(rs, 0, 32), row_pairs(rs, 64, 32)
    if first:
        low = jnp.concatenate([low, row_pairs(rs, 128, 32)], 0)
        high = jnp.concatenate([high, row_pairs(rs, 192, 32)], 0)
    return halves(low, high)


def fill_edges(up, dn, y, x):
    for edge, p, q in ((up, 3, 2), (dn, 0, 1)):
        edge[pl.ds(0, 64), :] = y[p]
        edge[pl.ds(64, 64), :] = x[p]
        edge[pl.ds(128, 64), :] = x[q]


def pack_body(u, src, cap, w, y, x, block, up, dn, cap_out, u_in, src_in, rs, sems):
    copies = [
        pltpu.make_async_copy(cap, cap_out, sems.at[0]),
        pltpu.make_async_copy(u.at[0], u_in, sems.at[1]),
        pltpu.make_async_copy(src.at[0, 0], src_in, sems.at[2]),
    ]
    for copy in copies:
        copy.start()
    copies[0].wait()
    for p in range(DEPTH):
        w[p] = OMEGA / (cap_out[p] + 6.0)
    for copy in copies[1:]:
        copy.wait()
    for p in range(DEPTH):
        u_in[p] = cap_out[p] * u_in[p] + src_in[p]
    blocks = local_down(lambda p: u_in[p], cap_out, w, y, x, rs, True)
    block[...] = blocks
    fill_edges(up, dn, y, x)
    lane = iota((32, 128), 1)
    b1, c1 = blocks[:32], blocks[32:]
    up[pl.ds(192, 32), :] = jnp.where(lane < 64, pltpu.roll(b1, 64, 1), c1)
    dn[pl.ds(192, 32), :] = jnp.where(lane < 64, b1, pltpu.roll(c1, 64, 1))
    up[pl.ds(224, 64), :] = w[3]
    dn[pl.ds(224, 64), :] = w[0]


def finish_down(first, w, y, x, b1, c1, lo, hi, wx, yx, xs, pair, rs):
    s = lax.axis_index("space")
    lane = iota((32, 128), 1)

    def edge(ref, there):
        return [
            jnp.where(there, ref[pl.ds(start, 64), :], 0.0)
            for start in ((0, 64, 128, 224) if first else (0, 64, 128))
        ]

    sides = []
    for ref, there, i, p in ((lo, s > 0, 0, 0), (hi, s < SLABS - 1, 5, 3)):
        ye, xe, xs_far, *we = edge(ref, there)
        if first:
            wx[i] = we[0]
        yx[i] = ye
        near = w[p] * ye
        far = wx[i] * y[p]
        x_near, x_far = x[p] + near, xe + far
        j = 1 if p == 0 else 6
        xs[j] = x_far
        xs[0 if p == 0 else 7] = xs_far
        xs[p + 2] = x_near
        own = (near - OMEGA * ye) + inside_plane(near) + x_far
        beside = (far - OMEGA * y[p]) + inside_plane(far) + x_near
        sides.append((own, jnp.where(there, beside, 0.0)))
    for p in range(DEPTH):
        yx[p + 1] = y[p]
        if first:
            wx[p + 1] = w[p]
    xs[3] = x[1]
    xs[4] = x[2]
    for k, v in enumerate((sides[0][0], sides[1][1], sides[1][0], sides[0][1])):
        rs[pl.ds(64 * k, 64), :] = v
    low = jnp.concatenate([row_pairs(rs, 0, 32), row_pairs(rs, 64, 32)], 0)
    high = jnp.concatenate([row_pairs(rs, 128, 32), row_pairs(rs, 192, 32)], 0)
    terms = halves(low, high)
    lo_block, hi_block = lo[pl.ds(192, 32), :], hi[pl.ds(192, 32), :]
    if first:
        pair[pl.ds(64, 32), :] = c1
        pair[pl.ds(96, 32), :] = jnp.where(lane < 64, pltpu.roll(hi_block, 64, 1), lo_block)
        lo_block = pltpu.roll(lo_block, 64, 1)
    own = b1 + terms[:32]
    pair[pl.ds(0, 32), :] = own
    pair[pl.ds(32, 32), :] = jnp.where(lane < 64, hi_block, lo_block) + terms[32:]
    return own


def share(b1, c1, c_mix, send, rs):
    s = lax.axis_index("space")
    lane = iota((32, 128), 1)
    zero = jnp.zeros((32, 128), F32)
    own, beside = c1 + 3.0, c_mix + 3.0
    w_own, w_mix = OMEGA / own, OMEGA / beside
    y = w_own * b1
    x = [
        block_sweep(zero, jnp.where((lane >= 64) & (s > 0), w_mix, 0.0), zero, y),
        block_sweep(y, w_own, zero, zero),
        block_sweep(zero, jnp.where((lane < 64) & (s < SLABS - 1), w_mix, 0.0), y, zero),
    ]
    r = [
        0.5 * around_block(x[0], zero, x[1]) - beside * x[0],
        b1 - own * x[1] + 0.5 * around_block(x[1], x[0], x[2]),
        0.5 * around_block(x[2], x[1], zero) - beside * x[2],
        c1,
    ]
    for k in range(4):
        rs[pl.ds(32 * k, 32), :] = r[k]
    low = quarters(row_pairs(rs, 0, 64))
    group = iota((16, 128), 1) >> 5
    message = low[48:]
    for k in range(3):
        message = jnp.where(group == k, low[16 * k : 16 * k + 16], message)
    for peer in range(SLABS):
        send[peer] = message


def first_down_body(w, y, x, block, lo, hi, wx, yx, xs, pair, send, rs):
    b1, c1 = block[pl.ds(0, 32), :], block[pl.ds(32, 32), :]
    own = finish_down(True, w, y, x, b1, c1, lo, hi, wx, yx, xs, pair, rs)
    share(own, c1, pair[pl.ds(96, 32), :], send, rs)


def next_down_body(y, x, block, lo, hi, w, wx, yx, xs, pair, rs):
    finish_down(False, w, y, x, block[...], None, lo, hi, wx, yx, xs, pair, rs)


def wide_share_body(own, y, x, wx, w1, c1, send, rs):
    block = own[...]
    lane = iota((32, 128), 1)
    zero = jnp.zeros((32, 128), F32)
    for k, (i, p) in enumerate(((0, 0), (5, 3))):
        far = wx[i] * y[p]
        rs[pl.ds(64 * k, 64), :] = far
        rs[pl.ds(128 + 64 * k, 64), :] = (far - OMEGA * y[p]) + inside_plane(far) + x[p]
    low = jnp.concatenate([row_pairs(rs, 0, 32), row_pairs(rs, 192, 32)], 0)
    high = jnp.concatenate([row_pairs(rs, 64, 32), row_pairs(rs, 128, 32)], 0)
    terms = halves(low, high)
    mix = terms[32:]
    b = [jnp.where(lane >= 64, mix, 0.0), block + terms[:32], jnp.where(lane < 64, mix, 0.0)]
    v = [zero] + [w1[j + 1] * b[j] for j in range(3)] + [zero]
    v = [zero] + [block_sweep(v[j], w1[j], v[j - 1], v[j + 1]) for j in (1, 2, 3)] + [zero]
    r = [0.5 * around_block(zero, zero, v[1])]
    for j in (1, 2, 3):
        r.append(b[j - 1] - (c1[j] + 3.0) * v[j] + 0.5 * around_block(v[j], v[j - 1], v[j + 1]))
    r.append(0.5 * around_block(zero, v[3], zero))
    for k in range(5):
        rs[pl.ds(32 * k, 32), :] = r[k]
    low = quarters(row_pairs(rs, 0, 80))
    group = iota((16, 128), 1) >> 5
    message = low[:16]
    for k in (1, 2, 3):
        message = jnp.where(group == k, low[16 * k : 16 * k + 16], message)
    pieces = [message[4 * k : 4 * k + 4] for k in range(4)]
    last = low[64:68]
    for k in (1, 2, 3):
        last = jnp.where(group[:4] == k, low[64 + 4 * k : 68 + 4 * k], last)
    pieces.append(last)
    for peer in range(SLABS):
        for k in range(5):
            send[5 * peer + k] = pieces[k]


def spread(v):
    v = v + pltpu.roll(v, 64, 1)
    return v + pltpu.roll(v, 32, 1)


def to_coarsest(v, t3):
    for k in range(4):
        t3[pl.ds(16 * k, 16), :] = v[32 * k : 32 * k + 16] + v[32 * k + 16 : 32 * k + 32]
    v = row_pairs(t3, 0, 32)
    lane = iota(v.shape, 1)
    at = (lane & 96) + 2 * (lane & 15)
    v = 0.125 * (lanes_of(v, at) + lanes_of(v, at + 1))
    return jnp.where((lane[:16] & 16) == 0, v[:16], v[16:])


def from_coarsest(v, t3):
    lane = iota(v.shape, 1)
    at = (lane & 96) + ((lane & 31) >> 1)
    v = jnp.concatenate([lanes_of(v, at), lanes_of(v, at + 16)], 0)
    t3[pl.ds(0, 32, stride=2), :] = v
    t3[pl.ds(1, 32, stride=2), :] = v
    parts = []
    for k in range(4):
        block = t3[pl.ds(16 * k, 16), :]
        parts += [block, block]
    return jnp.concatenate(parts, 0)


def low_levels(first, got, w2, d2, w3, x2, t3, joined=None):
    group = iota((16, 128), 1) >> 5
    quarter = iota((16, 128), 0) >> 2
    if not first:
        for z in range(SLABS):
            for k in range(4):
                joined[z, pl.ds(4 * k, 4), :] = got[5 * z + k]
                joined[z, pl.ds(16 + 4 * k, 4), :] = got[5 * z + 4]
    rows = got if first else joined
    reach = 1 if first else 2
    parts, caps = [], []
    for zl in range(8):
        total, cap = None, None
        for zh in range(4):
            z = 8 * zh + zl
            v = jnp.zeros((16, 128), F32)
            for k in range(3 if first else 4):
                if 0 <= z + reach - k < SLABS:
                    v = jnp.where(group == k, rows[z + reach - k, pl.ds(0, 16), :], v)
            if not first and z >= 2:
                v = v + jnp.where(group == quarter, rows[z - 2, pl.ds(16, 16), :], 0.0)
            v = spread(v)
            total = v if total is None else jnp.where(group == zh, v, total)
            if first:
                v = spread(jnp.where(group == 3, got[z], 0.0))
                cap = v if cap is None else jnp.where(group == zh, v, cap)
        parts.append(total)
        caps.append(cap)
    b = jnp.concatenate(parts, 0)
    if first:
        c2 = jnp.concatenate(caps, 0)
        d2[...] = c2 + 1.5
        w2[...] = OMEGA / (c2 + 1.5)
        w3[...] = OMEGA / (to_coarsest(c2, t3) + 0.75)
    w, d = w2[...], d2[...]
    y = w * b
    x = 1.2 * y + 0.25 * w * around_low(y)
    r = b - d * x + 0.25 * around_low(x)
    x = x + from_coarsest(coarsest(to_coarsest(r, t3), w3[...], 2 if first else 3), t3)
    for _ in range(2):
        x = 0.2 * x + y + 0.25 * w * around_low(x)
    x2[...] = x


def first_low_body(got, w2, d2, w3, x2, t3):
    low_levels(True, got, w2, d2, w3, x2, t3)


def next_low_body(got, w2, d2, w3, after, x2, t3, joined):
    low_levels(False, got, w2, d2, w3, x2, t3, joined)


def fine_up(x2, lo2, pair, hi2, c1, wx, yx, xs, w1, work, out):
    f1, y1, xa, xb, f0, x0, x9 = work
    s = lax.axis_index("space")
    lane = iota((32, 128), 1)

    def blocks(start):
        mixed = [ref[pl.ds(start + 32, 32), :] for ref in (lo2, pair, hi2)]
        return (
            lo2[pl.ds(start, 32), :],
            jnp.where(lane < 64, mixed[0], mixed[1]),
            pair[pl.ds(start, 32), :],
            jnp.where(lane < 64, mixed[1], mixed[2]),
            hi2[pl.ds(start, 32), :],
        )

    if c1 is not None:
        for j, c in enumerate(blocks(64)):
            c1[j] = c
            z = s + (j - 2)
            w1[j] = jnp.where((z >= 0) & (z < SLABS), OMEGA / (c + 3.0), 0.0)
    for j, b in enumerate(blocks(0)):
        y1[j] = w1[j] * b
    zero = jnp.zeros((32, 128), F32)
    lane = iota((16, 128), 1)
    for j in range(5):
        z = s + (j - 2)
        v = x2[pl.ds(pl.multiple_of((z & 7) * 16, 16), 16), :]
        v = lanes_of(v, ((lane & 63) >> 1) + ((z >> 3) & 3) * 32)
        v = jnp.where((z >= 0) & (z < SLABS), v, 0.0)
        f1[pl.ds(32 * j, 16, stride=2), :] = v
        f1[pl.ds(32 * j + 1, 16, stride=2), :] = v
    for j in range(5):
        below = y1[j - 1] if j > 0 else zero
        above = y1[j + 1] if j < 4 else zero
        xa[j] = block_sweep(y1[j], w1[j], below, above) + f1[pl.ds(32 * j, 32), :]
    xb[0] = zero
    xb[4] = zero
    for old, new in ((xa, xb), (xb, xa)):
        for j in (1, 2, 3):
            c = old[j]
            t = around_block(c, old[j - 1], old[j + 1])
            new[j] = 0.2 * c + y1[j] + 0.5 * w1[j] * t
    one, two, three = xa[1], xa[2], xa[3]
    half = iota((32, 128), 1) >> 1
    wide = (
        lanes_of(one, half + 64),
        lanes_of(two, half),
        lanes_of(two, half + 64),
        lanes_of(three, half),
    )
    for q, v in enumerate(wide):
        f0[pl.ds(64 * q, 32, stride=2), :] = v
        f0[pl.ds(64 * q + 1, 32, stride=2), :] = v
    for i in range(8):
        x0[i] = xs[i] + f0[pl.ds(64 * (i // 2), 64), :]
    for i in range(6):
        c = x0[i + 1]
        x9[i] = 0.2 * c + yx[i] + wx[i] * around_plane(c, x0[i], x0[i + 2])
    for p in range(DEPTH):
        c = x9[p + 1]
        out(p, 0.2 * c + yx[p + 1] + wx[p + 1] * around_plane(c, x9[p], x9[p + 2]))


def first_up_body(
    x2, lo2, pair, hi2, wx, yx, xs, w, cap, src, u_out, y, x, block, up, dn, w1, c1, *work
):
    b_out, rs, *work = work

    def out(p, u):
        u_out[0, p] = u
        b_out[p] = cap[p] * u + src[0, 1, p]

    fine_up(x2, lo2, pair, hi2, c1, wx, yx, xs, w1, work, out)
    own = local_down(lambda p: b_out[p], cap, w, y, x, rs, False)
    block[...] = own
    fill_edges(up, dn, y, x)
    up[pl.ds(192, 32), :] = own
    dn[pl.ds(192, 32), :] = own


def next_up_body(x2, lo2, pair, hi2, wx, yx, xs, w1, u_out, *work):
    def out(p, u):
        u_out[0, p] = u

    fine_up(x2, lo2, pair, hi2, None, wx, yx, xs, w1, work, out)


LOW_WORK = [(64, 128)]
LOW_FLOPS = 1 << 31
WORK = [
    (160, 128),
    (5, 32, 128),
    (5, 32, 128),
    (5, 32, 128),
    (256, 128),
    (8, NY, NX),
    (6, NY, NX),
]
EDGE_SUMS = (256, 128)
PLANE = (NY, NX)
PLANE4 = (DEPTH, NY, NX)
MESSAGE = f32(SLABS, 16, 128)
WIDE_MESSAGE = f32(SLABS * 5, 4, 128)


def moved(x, spans, slabs):
    pairs = []
    for t in range(SPANS):
        for s in range(SLABS):
            pairs.append((t * SLABS + s, (t + spans) % SPANS * SLABS + (s + slabs) % SLABS))
    return lax.ppermute(x, ("tm", "space"), pairs)


def gathered(send):
    return lax.all_to_all(send, "space", 0, 0, tiled=True)


def both(up, dn, reach):
    lo = moved(up, 0, reach)
    hi = moved(dn, 0, -reach)
    return lo, hi


def near(pair):
    lo, hi = both(pair, pair, 2)
    return lo, pair, hi


def shards(u0, src, cap):
    slab = f32(*PLANE4)
    w, y, x, block, up, dn, cap_in = call(
        pack_body,
        (slab, slab, slab, f32(64, 128), f32(288, 128), f32(288, 128), slab),
        [PLANE4, PLANE4, EDGE_SUMS],
        *(pltpu.with_memory_space_constraint(v, pltpu.HBM) for v in (u0, src, cap)),
        space=pl.BlockSpec(memory_space=pltpu.HBM),
        sems=[pltpu.SemaphoreType.DMA((3,))],
    )
    lo, hi = both(up, dn, 1)
    wx, yx, xs, pair, send = call(
        first_down_body,
        (f32(6, *PLANE), f32(6, *PLANE), f32(8, *PLANE), f32(128, 128), MESSAGE),
        [EDGE_SUMS],
        *(w, y, x, block, lo, hi),
    )
    got = gathered(send)
    w2, d2, w3, x2 = call(
        first_low_body,
        (f32(128, 128), f32(128, 128), f32(16, 128), f32(128, 128)),
        LOW_WORK,
        got,
        flops=LOW_FLOPS,
    )
    fpoint, y, x, block, up, dn, w1, c1 = call(
        first_up_body,
        (
            f32(1, *PLANE4),
            slab,
            slab,
            f32(32, 128),
            f32(224, 128),
            f32(224, 128),
            f32(5, 32, 128),
            f32(5, 32, 128),
        ),
        [PLANE4, EDGE_SUMS, *WORK],
        *(x2, *near(pair), wx, yx, xs, w, cap_in, src),
    )
    (send,) = call(wide_share_body, (WIDE_MESSAGE,), [EDGE_SUMS], *(block, y, x, wx, w1, c1))
    got = gathered(send)
    lo, hi = both(up, dn, 1)
    yx, xs, pair = call(
        next_down_body,
        (f32(6, *PLANE), f32(8, *PLANE), f32(64, 128)),
        [EDGE_SUMS],
        *(y, x, block, lo, hi, w, wx),
    )
    (x2,) = call(
        next_low_body,
        (f32(128, 128),),
        [*LOW_WORK, (SLABS, 32, 128)],
        *(got, w2, d2, w3, pair),
        flops=LOW_FLOPS,
    )
    (u,) = call(next_up_body, (f32(1, *PLANE4),), WORK, *(x2, *near(pair), wx, yx, xs, w1))
    updated = jnp.where(lax.axis_index("tm") == 0, u0, moved(u, 1, 0))
    return fpoint, updated


def solution(mesh):
    in_specs = (
        P("tm", "space", None, None),
        P("tm", None, "space", None, None),
        P("space", None, None),
    )
    out_specs = (P("tm", "space", None, None), P("tm", "space", None, None))
    return jax.shard_map(shards, mesh=mesh, in_specs=in_specs, out_specs=out_specs, check_vma=False)
```
